32 devices in a mesh: dp: 8 (over z, x), tensor: 4 (over y, core).
Axes of the slice: x: 2, y: 2, z: 4, core: 2. Of those that a mesh axis runs over, the one named last changes fastest.
Arguments:
- latents: bfloat16 [32, 512, 1024], P(('dp', 'tensor')), may hold values from -6 to 6
- cotangent: bfloat16 [32, 512, 1024], P(('dp', 'tensor')), may hold values from -6 to 6
- counts: int32 [16], replicated, may hold values from 1 to 3, as said below
- assign: int32 [16], replicated, may hold values from 0 to 7, as said below
- pre_gain: float32 [1024], replicated, may hold values from 0.1 to 1.9
- pre_shift: float32 [1024], replicated, may hold values from -1.75 to 1.75
- w_query: bfloat16 [1024, 1024], P(None, 'tensor'), may hold values from -0.375 to 0.375
- b_query: float32 [1024], P('tensor'), may hold values from -3 to 3
- w_key: bfloat16 [1024, 1024], P(None, 'tensor'), may hold values from -0.1875 to 0.1875
- w_value: bfloat16 [1024, 1024], P(None, 'tensor'), may hold values from -0.1875 to 0.1875
- b_value: float32 [1024], P('tensor'), may hold values from -1.75 to 1.75
- w_out: bfloat16 [1024, 1024], P('tensor'), may hold values from -0.75 to 0.75
- b_out: float32 [1024], replicated, may hold values from -1.75 to 1.75
- mid_gain: float32 [1024], replicated, may hold values from 0.1 to 1.9
- mid_shift: float32 [1024], replicated, may hold values from -1.75 to 1.75
- w_up: bfloat16 [1024, 1024], P(None, 'tensor'), may hold values from -0.1875 to 0.1875
- b_up: float32 [1024], P('tensor'), may hold values from -1.75 to 1.75
- w_down: bfloat16 [1024, 1024], P('tensor'), may hold values from -0.25 to 0.25
- b_down: float32 [1024], replicated, may hold values from -1.75 to 1.75
Outputs:
- latents_out: bfloat16 [32, 512, 1024], P(('dp', 'tensor'))
- latents_grad: float32 [32, 512, 1024], P(('dp', 'tensor'))
- pregain_grad: float32 [1024], replicated
- preshift_grad: float32 [1024], replicated
- wquery_grad: float32 [1024, 1024], P(None, 'tensor')
- bquery_grad: float32 [1024], P('tensor')
- wkey_grad: float32 [1024, 1024], P(None, 'tensor')
- wvalue_grad: float32 [1024, 1024], P(None, 'tensor')
- bvalue_grad: float32 [1024], P('tensor')
- wout_grad: float32 [1024, 1024], P('tensor')
- bout_grad: float32 [1024], replicated
- midgain_grad: float32 [1024], replicated
- midshift_grad: float32 [1024], replicated
- wup_grad: float32 [1024, 1024], P(None, 'tensor')
- bup_grad: float32 [1024], P('tensor')
- wdown_grad: float32 [1024, 1024], P('tensor')
- bdown_grad: float32 [1024], replicated
The draws below stay inside these ranges and needn't reach their ends.
Inputs may be any that keep to these rules, and one draw needn't show every extreme that they name: The counts of the 2 images of one data index add up to at most 4, and to exactly 4 on at least one data index. `assign`: each data index holds exactly 2 images.
All inputs are finite; a program needn't handle non-finite values.
Results may differ from the reference program's by a relative error of at most 0.017.
Values may be sent and summed in bfloat16 or wider, within the bound.
A program may use at most 128 MiB of HBM per device.

```python
import math
import jax
import jax.numpy as jnp
from jax import lax

D = 1024
HEADS = 8
FF = 1024
LAT = 512
SLOTS = 4
HEAD = 128
CROPS = 32
IMAGES = 16
N_DP = 8


def crop_plan(key):
    folded = jax.random.fold_in(key, 101)
    order_key, first_key, second_key, forced_key = jax.random.split(folded, 4)
    groups = IMAGES // 2
    order = jax.random.permutation(order_key, IMAGES)
    first = jax.random.randint(first_key, (groups,), 1, SLOTS)
    forced = jax.random.randint(forced_key, (), 0, groups)
    first = jnp.where(jnp.arange(groups) == forced, SLOTS - 1, first)
    second = jax.random.randint(second_key, (groups,), 1, SLOTS + 1 - first)
    holder = order // 2
    amounts = jnp.where(order % 2 == 0, first[holder], second[holder])
    return (amounts.astype(jnp.int32), holder.astype(jnp.int32))


def draw_counts(key, part):
    return crop_plan(key)[0]


def draw_assign(key, part):
    return crop_plan(key)[1]


def block_scale(stream_key, extent, pieces, least, high):
    level = 1.0
    for position, blocks in pieces:
        steps = jax.random.uniform(jax.random.fold_in(jax.random.fold_in(stream_key, 6), position), (blocks,), jnp.float32, least / len(pieces), high / len(pieces))
        level = level * jnp.repeat(jnp.exp(steps), extent[position] // blocks).reshape((-1,) + (1,) * (len(extent) - 1 - position))
    return level


def normal_values(stream_key, extent, width, limit, pieces=(), kind=jnp.bfloat16):
    values = jax.random.normal(stream_key, extent, jnp.float32) * width
    if len(pieces) > 0:
        values = block_scale(stream_key, extent, pieces, -0.22, 0.18) * values
    return jnp.clip(values, min=-limit, max=limit).astype(kind)


def setup_inputs(seed: int = 0) -> dict:
    key_of = jax.random.split(jax.random.key(seed), 20)
    return {
        "latents": normal_values(key_of[0], (CROPS, LAT, D), 1.0, 6.0, ((0, 32),)),
        "cotangent": normal_values(key_of[1], (CROPS, LAT, D), 1.0, 6.0, ((0, 32),)),
        "counts": draw_counts(jax.random.fold_in(key_of[19], 71), 0),
        "assign": draw_assign(jax.random.fold_in(key_of[19], 71), 0),
        "pre_gain": jnp.clip(1.0 + 0.18 * jax.random.normal(key_of[4], (D,), jnp.float32), 0.1, 1.9),
        "pre_shift": normal_values(key_of[5], (D,), 0.3, 1.75, (), jnp.float32),
        "w_query": normal_values(key_of[6], (D, D), (D // 4) ** -0.5, 0.375, ((1, 4),)),
        "b_query": normal_values(key_of[7], (D,), 0.5, 3.0, ((0, 4),), jnp.float32),
        "w_key": normal_values(key_of[8], (D, D), D ** -0.5, 0.1875, ((1, 4),)),
        "w_value": normal_values(key_of[9], (D, D), D ** -0.5, 0.1875, ((1, 4),)),
        "b_value": normal_values(key_of[10], (D,), 0.3, 1.75, ((0, 4),), jnp.float32),
        "w_out": normal_values(key_of[11], (D, D), (D // 16) ** -0.5, 0.75, ((0, 4),)),
        "b_out": normal_values(key_of[12], (D,), 0.3, 1.75, (), jnp.float32),
        "mid_gain": jnp.clip(1.0 + 0.18 * jax.random.normal(key_of[13], (D,), jnp.float32), 0.1, 1.9),
        "mid_shift": normal_values(key_of[14], (D,), 0.3, 1.75, (), jnp.float32),
        "w_up": normal_values(key_of[15], (D, FF), D ** -0.5, 0.1875, ((1, 4),)),
        "b_up": normal_values(key_of[16], (FF,), 0.3, 1.75, ((0, 4),), jnp.float32),
        "w_down": normal_values(key_of[17], (FF, D), (FF // 2) ** -0.5, 0.25, ((0, 4),)),
        "b_down": normal_values(key_of[18], (D,), 0.3, 1.75, (), jnp.float32),
    }


@jax.custom_vjp
def low(v):
    return lax.optimization_barrier(v.astype(jnp.bfloat16)).astype(jnp.float32)

@jax.custom_vjp
def low_back(v):
    return v

def low_keep(v):
    return (low(v), None)

def low_pass(kept, grad):
    return (grad,)

def back_keep(v):
    return (v, None)

def back_low(kept, grad):
    return (low(grad),)
low.defvjp(low_keep, low_pass)
low_back.defvjp(back_keep, back_low)
highest = lax.Precision.HIGHEST
epsilon = 1e-05

def normalize(inputs, norm_gain, norm_shift):
    center = lax.optimization_barrier(jnp.mean(inputs, axis=-1, keepdims=True))
    centered = inputs - center
    inverse = lax.rsqrt(lax.optimization_barrier(jnp.mean(centered * centered, axis=-1, keepdims=True)) + epsilon)
    return centered * inverse * norm_gain + norm_shift

def project(inputs, matrix):
    return jnp.einsum('cqi,ij->cqj', inputs, matrix, precision=highest, preferred_element_type=jnp.float32)

def one_crop(operands):
    queries, key_rows, values = operands
    scores = jnp.einsum('qhd,khd->hqk', queries, key_rows, precision=highest, preferred_element_type=jnp.float32)
    scores = low_back(scores / math.sqrt(HEAD))
    attn_probs = low(jax.nn.softmax(scores, axis=-1))
    return jnp.einsum('hqk,khd->qhd', attn_probs, values, precision=highest, preferred_element_type=jnp.float32)

def forward(params, crop_rows, live_mask):
    pre_gain, pre_shift, w_query, b_query, w_key, w_value, b_value, w_out, b_out, mid_gain, mid_shift, w_up, b_up, w_down, b_down = params
    crop_count = crop_rows.shape[0]
    normed_pre = low(normalize(crop_rows, pre_gain, pre_shift))
    queries = low(low_back(project(normed_pre, w_query) + b_query))
    key_rows = low(low_back(project(normed_pre, w_key)))
    values = low(low_back(project(normed_pre, w_value) + b_value))
    head_shape = (crop_count, LAT, HEADS, HEAD)
    mixed = lax.map(jax.checkpoint(one_crop), (queries.reshape(head_shape), key_rows.reshape(head_shape), values.reshape(head_shape)))
    mixed = low(low_back(mixed.reshape(crop_count, LAT, D)))
    hidden = crop_rows + low_back(project(mixed, w_out) + b_out)
    normed_mid = low(normalize(hidden, mid_gain, mid_shift))
    upward = low_back(project(normed_mid, w_up) + b_up)
    activated = low(jax.nn.gelu(upward, approximate=True))
    result = hidden + (project(activated, w_down) + b_down)
    return result * live_mask[:, None, None]

def reference(latents, cotangent, counts, assign, pre_gain, pre_shift, w_query, b_query, w_key, w_value, b_value, w_out, b_out, mid_gain, mid_shift, w_up, b_up, w_down, b_down):
    params = tuple((member.astype(jnp.float32) for member in (pre_gain, pre_shift, w_query, b_query, w_key, w_value, b_value, w_out, b_out, mid_gain, mid_shift, w_up, b_up, w_down, b_down)))
    group_ids = jnp.arange(N_DP, dtype=jnp.int32)
    group_totals = lax.optimization_barrier(jnp.sum(jnp.where(assign[None, :] == group_ids[:, None], counts[None, :], 0), axis=1))
    live_table = (jnp.arange(SLOTS, dtype=jnp.int32)[None, :] < group_totals[:, None]).astype(jnp.float32)
    crop_rows = latents.astype(jnp.float32).reshape(N_DP, SLOTS, LAT, D)
    crop_cots = cotangent.astype(jnp.float32).reshape(N_DP, SLOTS, LAT, D)

    def group_step(running, operands):
        group_rows, group_cot, group_live = operands

        def applied(weights, inputs):
            return forward(weights, inputs, group_live)
        outputs, pullback = jax.vjp(applied, params, group_rows)
        weight_grads, input_grad = pullback(group_cot)
        running = tuple((summed + addend for summed, addend in zip(running, weight_grads)))
        return (running, (outputs.astype(jnp.bfloat16), input_grad))
    initial = tuple((jnp.zeros_like(member) for member in params))
    weight_sums, (outputs, input_grads) = lax.scan(group_step, initial, (crop_rows, crop_cots, live_table))
    latents_out = outputs.reshape(CROPS, LAT, D)
    latents_grad = input_grads.reshape(CROPS, LAT, D)
    return (latents_out, latents_grad, weight_sums[0], weight_sums[1], weight_sums[2], weight_sums[3], weight_sums[4], weight_sums[5], weight_sums[6], weight_sums[7], weight_sums[8], weight_sums[9], weight_sums[10], weight_sums[11], weight_sums[12], weight_sums[13], weight_sums[14])
```

```python
from functools import partial
import math

import jax
import jax.numpy as jnp
from jax import lax
from jax.sharding import PartitionSpec as P

HEAD = 128


epsilon = 1e-05


def normalize(inputs, norm_gain, norm_shift):
    center = jnp.mean(inputs, axis=-1, keepdims=True)
    centered = inputs - center
    inverse = lax.rsqrt(jnp.mean(centered * centered, axis=-1, keepdims=True) + epsilon)
    scaled = centered * inverse
    return (scaled * norm_gain + norm_shift, scaled, inverse)


def norm_backward(upstream, scaled, inverse, norm_gain):
    weighted = upstream * norm_gain
    first_mean = jnp.mean(weighted, axis=-1, keepdims=True)
    second_mean = jnp.mean(weighted * scaled, axis=-1, keepdims=True)
    return inverse * (weighted - first_mean - scaled * second_mean)


def shards(
    latents,
    cotangent,
    counts,
    assign,
    pre_gain,
    pre_shift,
    w_query,
    b_query,
    w_key,
    w_value,
    b_value,
    w_out,
    b_out,
    mid_gain,
    mid_shift,
    w_up,
    b_up,
    w_down,
    b_down,
):
    f32, bf16 = jnp.float32, jnp.bfloat16
    crops, length, width = latents.shape
    tensor = lax.axis_size("tensor")
    heads = width // HEAD
    group_total = jnp.sum(jnp.where(assign == lax.axis_index("dp"), counts, 0))
    slot_ids = lax.axis_index("tensor") * crops + jnp.arange(crops, dtype=jnp.int32)
    live = jnp.repeat((slot_ids < group_total).astype(f32), length)[:, None]
    scaling = 1.0 / math.sqrt(HEAD)

    def dot(left, right, dims):
        return lax.dot_general(left, right, (dims, ((), ())), preferred_element_type=f32)

    columns = jnp.concatenate([w_query.T, w_key.T, w_value.T, w_out, w_up.T, w_down], axis=0)
    per = w_query.shape[1]
    gathered = lax.all_gather(columns, "tensor", axis=0, tiled=False).reshape(tensor, 6, per, width)
    wq, wk, wv, wo, wu, wd = [gathered[:, i].reshape(tensor * per, width) for i in range(6)]
    bias = lax.all_gather(jnp.stack([b_query, b_value, b_up]), "tensor", axis=1, tiled=True)

    rows = latents.astype(f32).reshape(crops * length, width)
    normed, scaled, inverse = normalize(rows, pre_gain, pre_shift)
    normed = normed.astype(bf16)
    q = (dot(normed, wq, ((1,), (1,))) + bias[0]).astype(bf16)
    k = dot(normed, wk, ((1,), (1,))).astype(bf16)
    v = (dot(normed, wv, ((1,), (1,))) + bias[1]).astype(bf16)
    split = lambda a: a.reshape(crops, length, heads, HEAD)
    q4, k4, v4 = split(q), split(k), split(v)
    ein = partial(jnp.einsum, preferred_element_type=f32)
    probs = jax.nn.softmax(ein("cqhd,ckhd->chqk", q4, k4) * scaling, axis=-1)
    low = probs.astype(bf16)
    mixed = ein("chqk,ckhd->cqhd", low, v4).astype(bf16).reshape(crops * length, width)
    hidden = rows + (dot(mixed, wo, ((1,), (0,))) + b_out)
    normed2, scaled2, inverse2 = normalize(hidden, mid_gain, mid_shift)
    normed2 = normed2.astype(bf16)
    upward = dot(normed2, wu, ((1,), (1,))) + bias[2]
    act32, gelu_pull = jax.vjp(partial(jax.nn.gelu, approximate=True), upward)
    act = act32.astype(bf16)
    result = hidden + (dot(act, wd, ((1,), (0,))) + b_down)
    latents_out = (result * live).astype(bf16).reshape(latents.shape)
    gy = cotangent.reshape(crops * length, width) * live.astype(bf16)
    g_wd = dot(act, gy, ((0,), (0,)))
    gu = gelu_pull(dot(gy, wd, ((1,), (1,))))[0].astype(bf16)
    g_wu = dot(gu, normed2, ((0,), (0,)))
    gn2 = dot(gu, wu, ((1,), (0,)))
    gh = gy.astype(f32) + norm_backward(gn2, scaled2, inverse2, mid_gain)
    ga = gh.astype(bf16)
    g_wo = dot(mixed, ga, ((0,), (0,)))
    go = split(dot(ga, wo, ((1,), (1,))).astype(bf16))
    gp = ein("cqhd,ckhd->chqk", go, v4)
    gs = (probs * (gp - jnp.sum(probs * gp, axis=-1, keepdims=True))).astype(bf16)
    flat = lambda a: a.astype(bf16).reshape(crops * length, width)
    gq = flat(ein("chqk,ckhd->cqhd", gs, k4) * scaling)
    gk = flat(ein("chqk,cqhd->ckhd", gs, q4) * scaling)
    gv = flat(ein("chqk,cqhd->ckhd", low, go))
    g_wq, g_wk, g_wv = [dot(a, normed, ((0,), (0,))) for a in (gq, gk, gv)]
    gn1 = dot(gq, wq, ((1,), (0,))) + dot(gk, wk, ((1,), (0,))) + dot(gv, wv, ((1,), (0,)))
    latents_grad = (gh + norm_backward(gn1, scaled, inverse, pre_gain)).reshape(latents.shape)

    def total(parts):
        stacked = jnp.stack([p.astype(bf16).reshape(tensor, per, width) for p in parts], axis=1)
        part = lax.psum_scatter(stacked, "tensor", scatter_dimension=0, tiled=True)
        return lax.psum(part, "dp")[0].astype(f32)

    s_wd, s_wu, s_wo = total((g_wd, g_wu, g_wo))
    s_wq, s_wk, s_wv = total((g_wq, g_wk, g_wv))
    col = lambda a: jnp.sum(a, axis=0, dtype=f32)
    sums = lax.psum(
        jnp.stack(
            [
                col(gn1 * scaled),
                col(gn1),
                col(ga),
                col(gn2 * scaled2),
                col(gn2),
                col(gy),
                col(gq),
                col(gv),
                col(gu),
            ]
        ),
        ("dp", "tensor"),
    )
    mine = lax.dynamic_slice_in_dim(sums[6:], lax.axis_index("tensor") * per, per, axis=1)
    return (
        latents_out,
        latents_grad,
        sums[0],
        sums[1],
        s_wq.T,
        mine[0],
        s_wk.T,
        s_wv.T,
        mine[1],
        s_wo,
        sums[2],
        sums[3],
        sums[4],
        s_wu.T,
        mine[2],
        s_wd,
        sums[5],
    )


def solution(mesh):
    return jax.shard_map(
        shards,
        mesh=mesh,
        in_specs=(
            P(("dp", "tensor"), None, None),
            P(("dp", "tensor"), None, None),
            P(),
            P(),
            P(),
            P(),
            P(None, "tensor"),
            P("tensor"),
            P(None, "tensor"),
            P(None, "tensor"),
            P("tensor"),
            P("tensor", None),
            P(),
            P(),
            P(),
            P(None, "tensor"),
            P("tensor"),
            P("tensor", None),
            P(),
        ),
        out_specs=(
            P(("dp", "tensor"), None, None),
            P(("dp", "tensor"), None, None),
            P(),
            P(),
            P(None, "tensor"),
            P("tensor"),
            P(None, "tensor"),
            P(None, "tensor"),
            P("tensor"),
            P("tensor", None),
            P(),
            P(),
            P(),
            P(None, "tensor"),
            P("tensor"),
            P("tensor", None),
            P(),
        ),
        check_vma=False,
    )
```

```python
from functools import partial
import math

import jax
import jax.numpy as jnp
from jax import lax
from jax.experimental import pallas as pl
from jax.experimental.pallas import tpu as pltpu
from jax.sharding import PartitionSpec as P

HEAD = 128
EPS = 1e-05
CHUNKS = 12
BLOCK = 128
ROWS = 128
F32 = jnp.float32
BF16 = jnp.bfloat16
MESH = pl.DeviceIdType.MESH


def dot(left, right):
    return lax.dot_general(left, right, (((1,), (0,)), ((), ())), preferred_element_type=F32)


def dot_nt(left, right):
    return lax.dot_general(left, right, (((1,), (1,)), ((), ())), preferred_element_type=F32)


def dot_tn(left, right):
    return lax.dot_general(left, right, (((0,), (0,)), ((), ())), preferred_element_type=F32)


def aligned(start, size):
    return pl.ds(pl.multiple_of(start, size), size)


def row_stats(values):
    center = jnp.mean(values, axis=-1, keepdims=True)
    centered = values - center
    inverse = lax.rsqrt(jnp.mean(centered * centered, axis=-1, keepdims=True) + EPS)
    return centered * inverse, inverse


def norm_pull(upstream, scaled, inverse, gain):
    weighted = upstream * gain
    first = jnp.mean(weighted, axis=-1, keepdims=True)
    second = jnp.mean(weighted * scaled, axis=-1, keepdims=True)
    return inverse * (weighted - first - scaled * second)


def step_kernel(
    lines,
    lat, cot, counts, assign, pre_gain, pre_shift, b_out, mid_gain, mid_shift, b_down, bias_in,
    w_query, w_key, w_value, w_out, w_up, w_down,
    y_out, gx_out, grads_out, vec_out,
    wc, wr, bias, xb, dy, n1, n2, lhs, rhs, fa, fb, vec,
    csend, crecv, ysend, yrecv, xsend, xrecv, zsend, zrecv, gathered, vrecv, vz,
    load_sem, own_sem, out_sem,
    gc_s, gc_r, gy_s, gy_r, gx_s, gx_r, ga_s, ga_r, gb_s, gb_r, bias_s, bias_r,
    c_s, c_r, y_s, y_r, x_s, x_r, z_s, z_r, az_s, az_r, ax_s, ax_r, v_s, v_r,
):
    length, width = xb.shape
    per = wc.shape[3]
    half = width // 2
    piece = half // lines
    scaling = 1.0 / math.sqrt(HEAD)
    dp = lax.axis_index("dp")
    me = lax.axis_index("tensor")
    px, rz = lax.rem(dp, 2), lax.div(dp, 2)
    core, yy = lax.rem(me, 2), lax.div(me, 2)
    t_core, t_y, t_diag = me + 1 - 2 * core, me + 2 - 4 * yy, 3 - me
    to_core, to_y, to_diag = {"tensor": t_core}, {"tensor": t_y}, {"tensor": t_diag}
    to_x = {"dp": dp + 1 - 2 * px}

    def to_z(offset):
        return {"dp": lax.rem(rz + offset, lines) * 2 + px}

    def remote(src, dst, send, recv, target):
        return pltpu.make_async_remote_copy(
            src_ref=src, dst_ref=dst, send_sem=send, recv_sem=recv, device_id=target, device_id_type=MESH
        )

    loads = [
        pltpu.make_async_copy(lat, xb, load_sem.at[0]),
        pltpu.make_async_copy(cot, dy, load_sem.at[1]),
        pltpu.make_async_copy(bias_in, bias.at[me], load_sem.at[2]),
    ]
    for copy in loads:
        copy.start()
    barrier = pltpu.get_barrier_semaphore()
    for target in [to_core, to_y, to_diag, to_x] + [to_z(i) for i in range(1, lines)]:
        pl.semaphore_signal(barrier, inc=1, device_id=target, device_id_type=MESH)
    pl.semaphore_wait(barrier, 3 + lines)

    shards = [
        (w_query, wc.at[0]), (w_key, wc.at[1]), (w_value, wc.at[2]),
        (w_out, wr.at[0]), (w_up, wc.at[3]), (w_down, wr.at[1]),
    ]

    def part(ref, index):
        size = ref.shape[0] // 2
        return ref.at[aligned(index * size, size)]

    def own_copy(w):
        return pltpu.make_async_copy(shards[w][0], shards[w][1].at[me], own_sem.at[w])

    def core_copy(w, who):
        return remote(shards[w][0], shards[w][1].at[who], gc_s.at[w], gc_r.at[w], to_core)

    def y_copy(w, who):
        return remote(part(shards[w][0], px), part(shards[w][1].at[who], px), gy_s.at[w], gy_r.at[w], to_y)

    def x_copy(w, which):
        ref = part(shards[w][1].at[t_y], which)
        return remote(ref, ref, gx_s.at[w], gx_r.at[w], to_x)

    def a_copy(w, who):
        ref = part(shards[w][1].at[who], px)
        return remote(ref, ref, ga_s.at[w], ga_r.at[w], to_core)

    def b_copy(w, who):
        ref = part(shards[w][1].at[who], 1 - px)
        return remote(ref, ref, gb_s.at[w], gb_r.at[w], to_core)

    for w in range(6):
        y_copy(w, me).start()
        core_copy(w, me).start()
        own_copy(w).start()
    loads[2].wait()
    for i, target in enumerate((to_core, to_y, to_diag)):
        remote(bias.at[me], bias.at[me], bias_s.at[i], bias_r.at[i], target).start()

    def gather_first(w):
        y_copy(w, t_y).wait_recv()
        x_copy(w, px).start()
        a_copy(w, t_y).start()

    def gather_second(w):
        x_copy(w, 1 - px).wait_recv()
        b_copy(w, t_y).start()

    def gather_near(w):
        own_copy(w).wait()
        core_copy(w, t_core).wait_recv()

    def gather_far(w):
        a_copy(w, t_diag).wait_recv()
        b_copy(w, t_diag).wait_recv()

    loads[0].wait()
    loads[1].wait()
    total = jnp.sum(jnp.where(assign[...] == dp, counts[...], 0).astype(F32), axis=-1, keepdims=True)
    live = (me.astype(F32) < total).astype(F32)
    vec[...] = jnp.zeros_like(vec)

    def add_vec(row, values):
        vec[row : row + 1, :] += jnp.sum(values, axis=0, keepdims=True)

    @pl.loop(0, length // ROWS)
    def _(i):
        rows = aligned(i * ROWS, ROWS)
        scaled, _ = row_stats(xb[rows, :].astype(F32))
        normed = scaled * pre_gain[...] + pre_shift[...]
        n1[rows, :] = normed.astype(BF16)
        lhs[3, :, rows] = normed.T.astype(BF16)
        grad = dy[rows, :].astype(F32) * live
        dy[rows, :] = grad.astype(BF16)
        lhs[0, :, rows] = grad.T.astype(BF16)
        add_vec(5, grad)

    for i, who in enumerate((t_core, t_y, t_diag)):
        remote(bias.at[who], bias.at[who], bias_s.at[i], bias_r.at[i], to_core).wait_recv()

    def project(who):
        columns = aligned(who * per, per)

        @pl.loop(0, 3)
        def _(i):
            value = dot(n1[...], wc[i, who]) + bias[who, pl.ds(i, 1), :]
            rhs[3 + i, :, columns] = value.astype(BF16)

    def probabilities(rows, columns):
        scores = dot_nt(rhs[3, rows, columns], rhs[4, :, columns]) * scaling
        exponent = jnp.exp(scores - jnp.max(scores, axis=-1, keepdims=True))
        return exponent / jnp.sum(exponent, axis=-1, keepdims=True)

    QROWS = length // 2

    def attend(head):
        columns = aligned(head * HEAD, HEAD)

        @pl.loop(0, 2)
        def _(i):
            rows = aligned(i * QROWS, QROWS)
            probs = probabilities(rows, columns).astype(BF16)
            rhs[2, rows, columns] = dot(probs, rhs[5, :, columns]).astype(BF16)

    for w in range(3):
        gather_near(w)
    for who in (me, t_core):
        project(who)
    gather_first(0)
    for i, who in enumerate((me, t_core)):
        attend(2 * who)
        attend(2 * who + 1)
        gather_first(i + 1)
        gather_second(i)
    gather_first(3)
    gather_second(2)
    for w in range(3):
        gather_far(w)
    for who in (t_y, t_diag):
        project(who)
    gather_first(4)
    gather_second(3)
    for who in (t_y, t_diag):
        attend(2 * who)
        attend(2 * who + 1)

    gather_near(3)
    gather_far(3)

    @pl.loop(0, 4)
    def _(i):
        columns = aligned(i * per, per)
        value = dot(rhs[2], wr[0, :, :, columns].reshape(width, per))
        fa[:, columns] = xb[:, columns].astype(F32) + (value + b_out[:, columns])

    gather_first(5)
    gather_second(4)

    @pl.loop(0, length // ROWS)
    def _(i):
        rows = aligned(i * ROWS, ROWS)
        scaled, _ = row_stats(fa[rows, :])
        normed = scaled * mid_gain[...] + mid_shift[...]
        n2[rows, :] = normed.astype(BF16)
        lhs[1, :, rows] = normed.T.astype(BF16)

    gather_near(4)
    gather_far(4)

    @pl.loop(0, 4)
    def _(i):
        columns = aligned(i * per, per)
        up = dot(n2[...], wc[3, i]) + bias[i, 3:4, :]
        root = math.sqrt(2.0 / math.pi)
        square = up * up
        curve = jnp.tanh(root * up * (1.0 + 0.044715 * square))
        outer = 0.5 * (1.0 + curve)
        rhs[0, :, columns] = (up * outer).astype(BF16)
        slope = root * (1.0 + 3 * 0.044715 * square)
        fb[:, columns] = outer + 0.5 * up * (1.0 - curve * curve) * slope

    def place(k):
        early = k < 6
        late = k - 6
        which = jnp.where(early, lax.div(k, 2), 3 + lax.rem(late + 6, 3))
        side = jnp.where(early, lax.rem(k, 2), jnp.where(late >= 3, 1, 0))
        return which, side, jnp.minimum(which, 3)

    def block_of(which, side, who):
        return rhs[which, :, aligned(who * per + side * BLOCK, BLOCK)]

    def c_copy(k):
        return remote(csend.at[k], crecv.at[k], c_s.at[k], c_r.at[k], to_core)

    def yg_copy(k):
        return remote(ysend.at[k], yrecv.at[k], y_s.at[k], y_r.at[k], to_y)

    def xg_copy(k):
        return remote(xsend.at[k], xrecv.at[k], x_s.at[k], x_r.at[k], to_x)

    def z_copy(k, offset):
        peer = lax.rem(rz + offset, lines)
        return remote(
            zsend.at[k, aligned(peer * piece, piece)], zrecv.at[k, offset - 1], z_s.at[k], z_r.at[k], to_z(offset)
        )

    def z_all(k):
        return remote(zrecv.at[k], zrecv.at[k], z_s.at[k], z_r.at[k], to_x)

    def az_copy(k, offset):
        ref = gathered.at[k, aligned(px * half + rz * piece, piece)]
        return remote(ref, ref, az_s.at[k], az_r.at[k], to_z(offset))

    def az_all(k):
        return remote(zrecv.at[k], zrecv.at[k], az_s.at[k], az_r.at[k], to_x)

    def ax_copy(k, which):
        ref = gathered.at[k, aligned(which * half, half)]
        return remote(ref, ref, ax_s.at[k], ax_r.at[k], to_x)

    def out_copy(k):
        return pltpu.make_async_copy(gathered.at[k], grads_out.at[k], out_sem.at[k])

    def stage0(k):
        which, side, left = place(k)
        pair = jnp.concatenate(
            [block_of(which, side, 1 - core), block_of(which, side, 3 - core)], axis=1
        )

        @pl.loop(0, 2)
        def _(i):
            rows = aligned(i * half, half)
            value = dot(lhs[left, rows, :], pair).astype(BF16)
            csend[k, 0, rows, :] = value[:, :BLOCK]
            csend[k, 1, rows, :] = value[:, BLOCK:]

        c_copy(k).start()

    def stage1(k):
        which, side, left = place(k)
        c_copy(k).wait_recv()
        value = dot(lhs[left], block_of(which, side, t_y))
        ysend[k] = (value + crecv[k, 1 - yy].astype(F32)).astype(BF16)
        yg_copy(k).start()

    def stage2(k):
        which, side, left = place(k)
        yg_copy(k).wait_recv()
        rows = aligned((1 - px) * half, half)
        value = dot(lhs[left, rows, :], block_of(which, side, me))
        value = value + crecv[k, yy, rows, :].astype(F32) + yrecv[k, rows, :].astype(F32)
        xsend[k] = value.astype(BF16)
        xg_copy(k).start()

    def stage3(k):
        which, side, left = place(k)
        rows = aligned(px * half, half)
        value = dot(lhs[left, rows, :], block_of(which, side, me))
        value = value + crecv[k, yy, rows, :].astype(F32) + yrecv[k, rows, :].astype(F32)
        xg_copy(k).wait_recv()
        zsend[k] = (value + xrecv[k].astype(F32)).astype(BF16)
        for offset in range(1, lines):
            z_copy(k, offset).start()

    def stage4(k):
        z_all(k).wait_recv()
        value = zsend[k, aligned(rz * piece, piece), :].astype(F32)
        for offset in range(1, lines):
            value = value + zrecv[k, offset - 1].astype(F32)
        gathered[k, aligned(px * half + rz * piece, piece), :] = value.astype(BF16)
        for offset in range(1, lines):
            az_copy(k, offset).start()

    def stage5(k):
        az_all(k).wait_recv()
        ax_copy(k, px).start()

    def stage6(k):
        ax_copy(k, 1 - px).wait_recv()
        out_copy(k).start()

    def v_copy(i, target):
        return remote(vec.at[pl.ds(16 * i, 16)], vrecv.at[i], v_s.at[i], v_r.at[i], target)

    def vz_copy(offset):
        ref = vz.at[rz]
        return remote(ref, ref, v_s.at[3], v_r.at[3], to_z(offset))

    def vz_all():
        ref = vz.at[pl.ds(0, lines - 1)]
        return remote(ref, ref, v_s.at[3], v_r.at[3], to_x)

    def piece_out():
        @pl.loop(0, 4)
        def _(i):
            columns = aligned(i * per, per)
            value = dot(rhs[0], wr[1, :, :, columns].reshape(width, per))
            value = fa[:, columns] + (value + b_down[:, columns])
            n1[:, columns] = (value * live).astype(BF16)

        pltpu.make_async_copy(n1, y_out, load_sem.at[3]).start()

        @pl.loop(0, 4)
        def _(i):
            columns = aligned(i * per, per)
            value = (dot_nt(dy[...], wr[1, i]) * fb[:, columns]).astype(BF16)
            rhs[1, :, columns] = value
            vec[8:9, columns] = jnp.sum(value.astype(F32), axis=0, keepdims=True)

    def piece_mid():
        @pl.loop(0, 4)
        def _(i):
            rows = aligned(i * per, per)
            value = dot_nt(rhs[1, :, :per], wc[3, 0, rows, :])
            for who in range(1, 4):
                value = value + dot_nt(rhs[1, :, who * per : (who + 1) * per], wc[3, who, rows, :])
            fb[:, rows] = value

        @pl.loop(0, length // ROWS)
        def _(i):
            rows = aligned(i * ROWS, ROWS)
            scaled, inverse = row_stats(fa[rows, :])
            up = fb[rows, :]
            add_vec(3, up * scaled)
            add_vec(4, up)
            value = dy[rows, :].astype(F32) + norm_pull(up, scaled, inverse, mid_gain[...])
            fb[rows, :] = value
            low = value.astype(BF16)
            n2[rows, :] = low
            lhs[2, :, rows] = value.T.astype(BF16)
            add_vec(2, low.astype(F32))

    def piece_mixed():
        pltpu.make_async_copy(n1, y_out, load_sem.at[3]).wait()

        @pl.loop(0, 4)
        def _(i):
            columns = aligned(i * per, per)
            n1[:, columns] = dot_nt(n2[...], wr[0, i]).astype(BF16)

    def piece_head(head):
        columns = aligned(head * HEAD, HEAD)
        queries, keys, values = rhs[3, :, columns], rhs[4, :, columns], rhs[5, :, columns]
        grad_queries = []
        grad_keys = jnp.zeros((length, HEAD), F32)
        grad_values = jnp.zeros((length, HEAD), F32)
        for i in range(2):
            rows = slice(i * QROWS, (i + 1) * QROWS)
            probs = probabilities(rows, columns)
            upstream = n1[rows, columns]
            grad_values = grad_values + dot_tn(probs.astype(BF16), upstream)
            grad_probs = dot_nt(upstream, values)
            inner = jnp.sum(probs * grad_probs, axis=-1, keepdims=True)
            grad_scores = (probs * (grad_probs - inner)).astype(BF16)
            grad_keys = grad_keys + dot_tn(grad_scores, rhs[3, rows, columns])
            grad_queries.append((dot(grad_scores, keys) * scaling).astype(BF16))
        grad_queries = jnp.concatenate(grad_queries, axis=0)
        grad_values = grad_values.astype(BF16)
        rhs[3, :, columns] = grad_queries
        rhs[4, :, columns] = (grad_keys * scaling).astype(BF16)
        rhs[5, :, columns] = grad_values
        vec[6:7, columns] = jnp.sum(grad_queries.astype(F32), axis=0, keepdims=True)
        vec[7:8, columns] = jnp.sum(grad_values.astype(F32), axis=0, keepdims=True)

    def piece_input():
        @pl.loop(0, 4)
        def _(i):
            rows = aligned(i * per, per)
            fa[:, rows] = jnp.zeros((length, per), F32)

            @pl.loop(0, 3)
            def _(m):
                value = fa[:, rows]
                for who in range(4):
                    value = value + dot_nt(rhs[3 + m, :, who * per : (who + 1) * per], wc[m, who, rows, :])
                fa[:, rows] = value

    def piece_last():
        @pl.loop(0, length // ROWS)
        def _(i):
            rows = aligned(i * ROWS, ROWS)
            scaled, inverse = row_stats(xb[rows, :].astype(F32))
            up = fa[rows, :]
            add_vec(0, up * scaled)
            add_vec(1, up)
            fa[rows, :] = fb[rows, :] + norm_pull(up, scaled, inverse, pre_gain[...])

        pltpu.make_async_copy(fa, gx_out, load_sem.at[4]).start()
        v_copy(0, to_core).start()

    stages = [stage0, stage1, stage2, stage3, stage4, stage5, stage6]

    @pl.loop(0, CHUNKS + len(stages) - 1)
    def _(tick):
        @pl.when(tick == 0)
        def _():
            gather_second(5)
            gather_near(5)
            gather_far(5)
            piece_out()

        pl.when(tick == 1)(piece_mid)
        pl.when(tick == 2)(piece_mixed)

        @pl.when((tick >= 2) & (tick < 10))
        def _():
            order = tick - 2
            piece_head(2 * lax.rem(order, 4) + lax.div(order, 4))

        pl.when(tick == 10)(piece_input)
        pl.when(tick == 11)(piece_last)
        for number, stage in enumerate(stages):
            k = tick - number

            @pl.when((k >= 0) & (k < CHUNKS))
            def _():
                stage(jnp.clip(k, 0, CHUNKS - 1))

        for i, target in ((0, to_y), (1, to_x)):
            @pl.when(tick == 12 + i)
            def _():
                v_copy(i, to_core).wait_recv()
                vec[16 * (i + 1) : 16 * (i + 2), :] = vec[16 * i : 16 * (i + 1), :] + vrecv[i]
                v_copy(i + 1, target).start()

        @pl.when(tick == 14)
        def _():
            v_copy(2, to_x).wait_recv()
            vz[rz] = vec[32:48, :] + vrecv[2]
            for offset in range(1, lines):
                vz_copy(offset).start()

        @pl.when(tick == 16)
        def _():
            vz_all().wait_recv()
            value = vz[0]
            for i in range(1, lines):
                value = value + vz[i]
            vec_out[...] = value

    for w in range(6):
        y_copy(w, me).wait_send()
        core_copy(w, me).wait_send()
        x_copy(w, px).wait_send()
        a_copy(w, t_y).wait_send()
        b_copy(w, t_y).wait_send()
    for i in range(3):
        remote(bias.at[me], bias.at[me], bias_s.at[i], bias_r.at[i], to_core).wait_send()
        v_copy(i, to_core).wait_send()
    vz_all().wait_send()

    @pl.loop(0, CHUNKS)
    def _(k):
        c_copy(k).wait_send()
        yg_copy(k).wait_send()
        xg_copy(k).wait_send()
        z_all(k).wait_send()
        az_all(k).wait_send()
        ax_copy(k, px).wait_send()
        out_copy(k).wait()

    pltpu.make_async_copy(fa, gx_out, load_sem.at[4]).wait()


def shards_of(
    lines,
    latents, cotangent, counts, assign, pre_gain, pre_shift, w_query, b_query, w_key, w_value, b_value,
    w_out, b_out, mid_gain, mid_shift, w_up, b_up, w_down, b_down,
):
    _, length, width = latents.shape
    per = w_query.shape[1]
    half = width // 2
    line = lambda a: a.reshape(1, -1)
    zero = jnp.zeros_like(b_query)
    bias_in = jnp.stack([b_query, zero, b_value, b_up, zero, zero, zero, zero])
    anywhere = pl.BlockSpec(memory_space=pl.ANY)
    inside = pl.BlockSpec(memory_space=pltpu.VMEM)
    dma = pltpu.SemaphoreType.DMA
    y_out, gx_out, grads, sums = pl.pallas_call(
        partial(step_kernel, lines),
        out_shape=(
            jax.ShapeDtypeStruct((length, width), BF16),
            jax.ShapeDtypeStruct((length, width), F32),
            jax.ShapeDtypeStruct((CHUNKS, width, BLOCK), BF16),
            jax.ShapeDtypeStruct((16, width), F32),
        ),
        in_specs=[anywhere] * 2 + [inside] * 8 + [anywhere] * 7,
        out_specs=(anywhere, anywhere, anywhere, inside),
        scratch_shapes=[
            pltpu.VMEM((4, 4, width, per), BF16),
            pltpu.VMEM((2, 4, per, width), BF16),
            pltpu.VMEM((4, 8, per), F32),
            pltpu.VMEM((length, width), BF16),
            pltpu.VMEM((length, width), BF16),
            pltpu.VMEM((length, width), BF16),
            pltpu.VMEM((length, width), BF16),
            pltpu.VMEM((4, width, length), BF16),
            pltpu.VMEM((6, length, width), BF16),
            pltpu.VMEM((length, width), F32),
            pltpu.VMEM((length, width), F32),
            pltpu.VMEM((48, width), F32),
            pltpu.VMEM((CHUNKS, 2, width, BLOCK), BF16),
            pltpu.VMEM((CHUNKS, 2, width, BLOCK), BF16),
            pltpu.VMEM((CHUNKS, width, BLOCK), BF16),
            pltpu.VMEM((CHUNKS, width, BLOCK), BF16),
            pltpu.VMEM((CHUNKS, half, BLOCK), BF16),
            pltpu.VMEM((CHUNKS, half, BLOCK), BF16),
            pltpu.VMEM((CHUNKS, half, BLOCK), BF16),
            pltpu.VMEM((CHUNKS, lines - 1, half // lines, BLOCK), BF16),
            pltpu.VMEM((CHUNKS, width, BLOCK), BF16),
            pltpu.VMEM((3, 16, width), F32),
            pltpu.VMEM((lines, 16, width), F32),
            dma((5,)), dma((6,)), dma((CHUNKS,)),
        ]
        + [dma((6,))] * 10
        + [dma((3,))] * 2
        + [dma((CHUNKS,))] * 12
        + [dma((4,))] * 2,
        compiler_params=pltpu.CompilerParams(
            collective_id=0, has_side_effects=True, vmem_limit_bytes=67043328
        ),
    )(
        latents.reshape(length, width), cotangent.reshape(length, width), line(counts), line(assign),
        line(pre_gain), line(pre_shift), line(b_out), line(mid_gain), line(mid_shift), line(b_down), bias_in,
        w_query, w_key, w_value, w_out, w_up, w_down,
    )

    def pick(first, second):
        return jnp.concatenate([grads[first], grads[second]], axis=1).astype(F32)

    mine = lax.dynamic_slice_in_dim(sums[6:9], lax.axis_index("tensor") * per, per, axis=1)
    return (
        y_out.reshape(latents.shape),
        gx_out.reshape(latents.shape),
        sums[0], sums[1],
        pick(6, 9), mine[0], pick(7, 10), pick(8, 11), mine[1],
        pick(4, 5).T, sums[2], sums[3], sums[4],
        pick(2, 3), mine[2], pick(0, 1).T, sums[5],
    )


def solution(mesh):
    assert mesh.shape["tensor"] == 4
    return jax.shard_map(
        partial(shards_of, mesh.shape["dp"] // 2),
        mesh=mesh,
        in_specs=(
            P(("dp", "tensor"), None, None),
            P(("dp", "tensor"), None, None),
            P(),
            P(),
            P(),
            P(),
            P(None, "tensor"),
            P("tensor"),
            P(None, "tensor"),
            P(None, "tensor"),
            P("tensor"),
            P("tensor", None),
            P(),
            P(),
            P(),
            P(None, "tensor"),
            P("tensor"),
            P("tensor", None),
            P(),
        ),
        out_specs=(
            P(("dp", "tensor"), None, None),
            P(("dp", "tensor"), None, None),
            P(),
            P(),
            P(None, "tensor"),
            P("tensor"),
            P(None, "tensor"),
            P(None, "tensor"),
            P("tensor"),
            P("tensor", None),
            P(),
            P(),
            P(),
            P(None, "tensor"),
            P("tensor"),
            P("tensor", None),
            P(),
        ),
        check_vma=False,
    )
```

```python
from functools import partial
import math

import jax
import jax.numpy as jnp
from jax import lax
from jax.experimental import pallas as pl
from jax.experimental.pallas import tpu as pltpu
from jax.sharding import PartitionSpec as P

HEAD = 128
EPS = 1e-05
CHUNKS = 12
BLOCK = 128
ROWS = 128
F32 = jnp.float32
BF16 = jnp.bfloat16
MESH = pl.DeviceIdType.MESH


def dot(left, right):
    return lax.dot_general(left, right, (((1,), (0,)), ((), ())), preferred_element_type=F32)


def dot_nt(left, right):
    return lax.dot_general(left, right, (((1,), (1,)), ((), ())), preferred_element_type=F32)


def dot_tn(left, right):
    return lax.dot_general(left, right, (((0,), (0,)), ((), ())), preferred_element_type=F32)


def aligned(start, size):
    return pl.ds(pl.multiple_of(start, size), size)


def row_stats(values):
    center = jnp.mean(values, axis=-1, keepdims=True)
    centered = values - center
    inverse = lax.rsqrt(jnp.mean(centered * centered, axis=-1, keepdims=True) + EPS)
    return centered * inverse, inverse


def norm_pull(upstream, scaled, inverse, gain):
    weighted = upstream * gain
    first = jnp.mean(weighted, axis=-1, keepdims=True)
    second = jnp.mean(weighted * scaled, axis=-1, keepdims=True)
    return inverse * (weighted - first - scaled * second)


def step_kernel(
    lines,
    lat, cot, counts, assign, pre_gain, pre_shift, b_out, mid_gain, mid_shift, b_down, b_query, b_value, b_up,
    w_query, w_key, w_value, w_out, w_up, w_down,
    y_out, gx_out, grads_out, vec_out,
    wc, wr, bias, xb, dy, n1, n2, lhs, rhs, fa, fb, vec,
    csend, crecv, ysend, yrecv, xsend, xrecv, zsend, zrecv, gathered, vrecv, vz,
    load_sem, own_sem, out_sem,
    gc_s, gc_r, gy_s, gy_r, gx_s, gx_r, ga_s, ga_r, gb_s, gb_r, bias_s, bias_r,
    c_s, c_r, y_s, y_r, x_s, x_r, z_s, z_r, az_s, az_r, ax_s, ax_r, v_s, v_r,
):
    length, width = xb.shape
    per = wc.shape[3]
    half = width // 2
    piece = half // lines
    scaling = 1.0 / math.sqrt(HEAD)
    dp = lax.axis_index("dp")
    me = lax.axis_index("tensor")
    px, rz = lax.rem(dp, 2), lax.div(dp, 2)
    core, yy = lax.rem(me, 2), lax.div(me, 2)
    t_core, t_y, t_diag = me + 1 - 2 * core, me + 2 - 4 * yy, 3 - me
    to_core, to_y, to_diag = {"tensor": t_core}, {"tensor": t_y}, {"tensor": t_diag}
    to_x = {"dp": dp + 1 - 2 * px}

    def to_z(offset):
        return {"dp": lax.rem(rz + offset, lines) * 2 + px}

    def remote(src, dst, send, recv, target):
        return pltpu.make_async_remote_copy(
            src_ref=src, dst_ref=dst, send_sem=send, recv_sem=recv, device_id=target, device_id_type=MESH
        )

    loads = [
        pltpu.make_async_copy(lat, xb, load_sem.at[0]),
        pltpu.make_async_copy(cot, dy, load_sem.at[1]),
        pltpu.make_async_copy(b_query, bias.at[me, 0:1], load_sem.at[2]),
        pltpu.make_async_copy(b_value, bias.at[me, 1:2], load_sem.at[5]),
        pltpu.make_async_copy(b_up, bias.at[me, 2:3], load_sem.at[6]),
    ]
    for copy in loads:
        copy.start()
    barrier = pltpu.get_barrier_semaphore()
    for target in [to_core, to_y, to_diag, to_x] + [to_z(i) for i in range(1, lines)]:
        pl.semaphore_signal(barrier, inc=1, device_id=target, device_id_type=MESH)
    pl.semaphore_wait(barrier, 3 + lines)

    shards = [
        (w_query, wc.at[0]), (w_key, wc.at[1]), (w_value, wc.at[2]),
        (w_out, wr.at[0]), (w_up, wc.at[3]), (w_down, wr.at[1]),
    ]

    def part(ref, index):
        size = ref.shape[0] // 2
        return ref.at[aligned(index * size, size)]

    def own_copy(w):
        return pltpu.make_async_copy(shards[w][0], shards[w][1].at[me], own_sem.at[w])

    def core_copy(w, who):
        return remote(shards[w][0], shards[w][1].at[who], gc_s.at[w], gc_r.at[w], to_core)

    def y_copy(w, who):
        return remote(part(shards[w][0], px), part(shards[w][1].at[who], px), gy_s.at[w], gy_r.at[w], to_y)

    def x_copy(w, which):
        ref = part(shards[w][1].at[t_y], which)
        return remote(ref, ref, gx_s.at[w], gx_r.at[w], to_x)

    def a_copy(w, who):
        ref = part(shards[w][1].at[who], px)
        return remote(ref, ref, ga_s.at[w], ga_r.at[w], to_core)

    def b_copy(w, who):
        ref = part(shards[w][1].at[who], 1 - px)
        return remote(ref, ref, gb_s.at[w], gb_r.at[w], to_core)

    def bias_copy(i, who, target):
        ref = bias.at[who, 0:3]
        return remote(ref, ref, bias_s.at[i], bias_r.at[i], target)

    y_copy(0, me).start()
    for w in range(6):
        core_copy(w, me).start()
        own_copy(w).start()
    for copy in loads[2:]:
        copy.wait()
    for i, target in enumerate((to_core, to_y, to_diag)):
        bias_copy(i, me, target).start()

    def gather_first(w):
        y_copy(w, t_y).wait_recv()
        if w + 2 < 6:
            y_copy(w + 2, me).start()
        x_copy(w, px).start()
        a_copy(w, t_y).start()

    def gather_second(w):
        x_copy(w, 1 - px).wait_recv()
        b_copy(w, t_y).start()

    def gather_near(w):
        own_copy(w).wait()
        core_copy(w, t_core).wait_recv()

    def gather_far(w):
        a_copy(w, t_diag).wait_recv()
        b_copy(w, t_diag).wait_recv()

    loads[0].wait()
    loads[1].wait()
    total = jnp.sum(jnp.where(assign[...] == dp, counts[...], 0).astype(F32), axis=-1, keepdims=True)
    live = (me.astype(F32) < total).astype(F32)
    vec[...] = jnp.zeros_like(vec)
    for who in range(4):
        bias[who, 3:4, :] = jnp.zeros((1, per), F32)

    def add_vec(row, values):
        vec[row : row + 1, :] += jnp.sum(values, axis=0, keepdims=True)

    @pl.loop(0, length // ROWS)
    def _(i):
        rows = aligned(i * ROWS, ROWS)
        scaled, _ = row_stats(xb[rows, :].astype(F32))
        normed = scaled * pre_gain[...] + pre_shift[...]
        n1[rows, :] = normed.astype(BF16)
        lhs[3, :, rows] = normed.T.astype(BF16)
        grad = dy[rows, :].astype(F32) * live
        dy[rows, :] = grad.astype(BF16)
        lhs[0, :, rows] = grad.T.astype(BF16)
        add_vec(5, grad)

        @pl.when(i == 1)
        def _():
            y_copy(1, me).start()

    for i, who in enumerate((t_core, t_y, t_diag)):
        bias_copy(i, who, to_core).wait_recv()

    def project(who):
        columns = aligned(who * per, per)

        @pl.loop(0, 3)
        def _(i):
            value = dot(n1[...], wc[i, who]) + bias[who, pl.ds(jnp.where(i == 1, 3, lax.div(i, 2)), 1), :]
            rhs[3 + i, :, columns] = value.astype(BF16)

    def probabilities(rows, columns):
        scores = dot_nt(rhs[3, rows, columns], rhs[4, :, columns]) * scaling
        exponent = jnp.exp(scores - jnp.max(scores, axis=-1, keepdims=True))
        return exponent / jnp.sum(exponent, axis=-1, keepdims=True)

    QROWS = length // 2

    def attend(head):
        columns = aligned(head * HEAD, HEAD)

        @pl.loop(0, 2)
        def _(i):
            rows = aligned(i * QROWS, QROWS)
            probs = probabilities(rows, columns).astype(BF16)
            rhs[2, rows, columns] = dot(probs, rhs[5, :, columns]).astype(BF16)

    for w in range(3):
        gather_near(w)
    for who in (me, t_core):
        project(who)
    gather_first(0)
    for i, who in enumerate((me, t_core)):
        attend(2 * who)
        attend(2 * who + 1)
        gather_first(i + 1)
        gather_second(i)
    gather_first(3)
    gather_second(2)
    for w in range(3):
        gather_far(w)
    for who in (t_y, t_diag):
        project(who)
    gather_first(4)
    gather_second(3)
    for who in (t_y, t_diag):
        attend(2 * who)
        attend(2 * who + 1)

    gather_near(3)
    gather_far(3)

    @pl.loop(0, 4)
    def _(i):
        columns = aligned(i * per, per)
        value = dot(rhs[2], wr[0, :, :, columns].reshape(width, per))
        fa[:, columns] = xb[:, columns].astype(F32) + (value + b_out[:, columns])

    gather_first(5)
    gather_second(4)

    @pl.loop(0, length // ROWS)
    def _(i):
        rows = aligned(i * ROWS, ROWS)
        scaled, _ = row_stats(fa[rows, :])
        normed = scaled * mid_gain[...] + mid_shift[...]
        n2[rows, :] = normed.astype(BF16)
        lhs[1, :, rows] = normed.T.astype(BF16)

    gather_near(4)
    gather_far(4)

    @pl.loop(0, 4)
    def _(i):
        columns = aligned(i * per, per)
        up = dot(n2[...], wc[3, i]) + bias[i, 2:3, :]
        root = math.sqrt(2.0 / math.pi)
        square = up * up
        curve = jnp.tanh(root * up * (1.0 + 0.044715 * square))
        outer = 0.5 * (1.0 + curve)
        rhs[0, :, columns] = (up * outer).astype(BF16)
        slope = root * (1.0 + 3 * 0.044715 * square)
        fb[:, columns] = outer + 0.5 * up * (1.0 - curve * curve) * slope

    def place(k):
        early = k < 6
        late = k - 6
        which = jnp.where(early, lax.div(k, 2), 3 + lax.rem(late + 6, 3))
        side = jnp.where(early, lax.rem(k, 2), jnp.where(late >= 3, 1, 0))
        return which, side, jnp.minimum(which, 3)

    def block_of(which, side, who):
        return rhs[which, :, aligned(who * per + side * BLOCK, BLOCK)]

    def c_copy(k):
        return remote(csend.at[k], crecv.at[k], c_s.at[k], c_r.at[k], to_core)

    def yg_copy(k):
        return remote(ysend.at[k], yrecv.at[k], y_s.at[k], y_r.at[k], to_y)

    def xg_copy(k):
        return remote(xsend.at[k], xrecv.at[k], x_s.at[k], x_r.at[k], to_x)

    def z_copy(k, offset):
        peer = lax.rem(rz + offset, lines)
        return remote(
            zsend.at[k, aligned(peer * piece, piece)], zrecv.at[k, offset - 1], z_s.at[k], z_r.at[k], to_z(offset)
        )

    def z_all(k):
        return remote(zrecv.at[k], zrecv.at[k], z_s.at[k], z_r.at[k], to_x)

    def az_copy(k, offset):
        ref = gathered.at[k, aligned(px * half + rz * piece, piece)]
        return remote(ref, ref, az_s.at[k], az_r.at[k], to_z(offset))

    def az_all(k):
        return remote(zrecv.at[k], zrecv.at[k], az_s.at[k], az_r.at[k], to_x)

    def ax_copy(k, which):
        ref = gathered.at[k, aligned(which * half, half)]
        return remote(ref, ref, ax_s.at[k], ax_r.at[k], to_x)

    def out_copy(k):
        return pltpu.make_async_copy(gathered.at[k], grads_out.at[k], out_sem.at[k])

    def stage0(k):
        which, side, left = place(k)
        pair = jnp.concatenate(
            [block_of(which, side, 1 - core), block_of(which, side, 3 - core)], axis=1
        )

        @pl.loop(0, 2)
        def _(i):
            rows = aligned(i * half, half)
            value = dot(lhs[left, rows, :], pair).astype(BF16)
            csend[k, 0, rows, :] = value[:, :BLOCK]
            csend[k, 1, rows, :] = value[:, BLOCK:]

        c_copy(k).start()

    def stage1(k):
        which, side, left = place(k)
        c_copy(k).wait_recv()
        value = dot(lhs[left], block_of(which, side, t_y))
        ysend[k] = (value + crecv[k, 1 - yy].astype(F32)).astype(BF16)
        yg_copy(k).start()

    def stage2(k):
        which, side, left = place(k)
        yg_copy(k).wait_recv()
        rows = aligned((1 - px) * half, half)
        value = dot(lhs[left, rows, :], block_of(which, side, me))
        value = value + crecv[k, yy, rows, :].astype(F32) + yrecv[k, rows, :].astype(F32)
        xsend[k] = value.astype(BF16)
        xg_copy(k).start()

    def stage3(k):
        which, side, left = place(k)
        rows = aligned(px * half, half)
        value = dot(lhs[left, rows, :], block_of(which, side, me))
        value = value + crecv[k, yy, rows, :].astype(F32) + yrecv[k, rows, :].astype(F32)
        xg_copy(k).wait_recv()
        zsend[k] = (value + xrecv[k].astype(F32)).astype(BF16)
        for offset in range(1, lines):
            z_copy(k, offset).start()

    def stage4(k):
        z_all(k).wait_recv()
        value = zsend[k, aligned(rz * piece, piece), :].astype(F32)
        for offset in range(1, lines):
            value = value + zrecv[k, offset - 1].astype(F32)
        gathered[k, aligned(px * half + rz * piece, piece), :] = value.astype(BF16)
        for offset in range(1, lines):
            az_copy(k, offset).start()

    def stage5(k):
        az_all(k).wait_recv()
        ax_copy(k, px).start()

    def stage6(k):
        ax_copy(k, 1 - px).wait_recv()
        out_copy(k).start()

    def v_copy(i, target):
        return remote(vec.at[pl.ds(16 * i, 16)], vrecv.at[i], v_s.at[i], v_r.at[i], target)

    def vz_copy(offset):
        ref = vz.at[rz]
        return remote(ref, ref, v_s.at[3], v_r.at[3], to_z(offset))

    def vz_all():
        ref = vz.at[pl.ds(0, lines - 1)]
        return remote(ref, ref, v_s.at[3], v_r.at[3], to_x)

    def piece_out():
        @pl.loop(0, 4)
        def _(i):
            columns = aligned(i * per, per)
            value = dot(rhs[0], wr[1, :, :, columns].reshape(width, per))
            value = fa[:, columns] + (value + b_down[:, columns])
            n1[:, columns] = (value * live).astype(BF16)

        pltpu.make_async_copy(n1, y_out, load_sem.at[3]).start()

        @pl.loop(0, 4)
        def _(i):
            columns = aligned(i * per, per)
            value = (dot_nt(dy[...], wr[1, i]) * fb[:, columns]).astype(BF16)
            rhs[1, :, columns] = value
            vec[8:9, columns] = jnp.sum(value.astype(F32), axis=0, keepdims=True)

    def piece_mid():
        @pl.loop(0, 4)
        def _(i):
            rows = aligned(i * per, per)
            value = dot_nt(rhs[1, :, :per], wc[3, 0, rows, :])
            for who in range(1, 4):
                value = value + dot_nt(rhs[1, :, who * per : (who + 1) * per], wc[3, who, rows, :])
            fb[:, rows] = value

        @pl.loop(0, length // ROWS)
        def _(i):
            rows = aligned(i * ROWS, ROWS)
            scaled, inverse = row_stats(fa[rows, :])
            up = fb[rows, :]
            add_vec(3, up * scaled)
            add_vec(4, up)
            value = dy[rows, :].astype(F32) + norm_pull(up, scaled, inverse, mid_gain[...])
            fb[rows, :] = value
            low = value.astype(BF16)
            n2[rows, :] = low
            lhs[2, :, rows] = value.T.astype(BF16)
            add_vec(2, low.astype(F32))

    def piece_mixed():
        pltpu.make_async_copy(n1, y_out, load_sem.at[3]).wait()

        @pl.loop(0, 4)
        def _(i):
            columns = aligned(i * per, per)
            n1[:, columns] = dot_nt(n2[...], wr[0, i]).astype(BF16)

    def piece_head(head):
        columns = aligned(head * HEAD, HEAD)
        queries, keys, values = rhs[3, :, columns], rhs[4, :, columns], rhs[5, :, columns]
        grad_queries = []
        grad_keys = jnp.zeros((length, HEAD), F32)
        grad_values = jnp.zeros((length, HEAD), F32)
        for i in range(2):
            rows = slice(i * QROWS, (i + 1) * QROWS)
            probs = probabilities(rows, columns)
            upstream = n1[rows, columns]
            grad_values = grad_values + dot_tn(probs.astype(BF16), upstream)
            grad_probs = dot_nt(upstream, values)
            inner = jnp.sum(probs * grad_probs, axis=-1, keepdims=True)
            grad_scores = (probs * (grad_probs - inner)).astype(BF16)
            grad_keys = grad_keys + dot_tn(grad_scores, rhs[3, rows, columns])
            grad_queries.append((dot(grad_scores, keys) * scaling).astype(BF16))
        grad_queries = jnp.concatenate(grad_queries, axis=0)
        grad_values = grad_values.astype(BF16)
        rhs[3, :, columns] = grad_queries
        rhs[4, :, columns] = (grad_keys * scaling).astype(BF16)
        rhs[5, :, columns] = grad_values
        vec[6:7, columns] = jnp.sum(grad_queries.astype(F32), axis=0, keepdims=True)
        vec[7:8, columns] = jnp.sum(grad_values.astype(F32), axis=0, keepdims=True)

    def piece_input():
        @pl.loop(0, 4)
        def _(i):
            rows = aligned(i * per, per)
            fa[:, rows] = jnp.zeros((length, per), F32)

            @pl.loop(0, 3)
            def _(m):
                value = fa[:, rows]
                for who in range(4):
                    value = value + dot_nt(rhs[3 + m, :, who * per : (who + 1) * per], wc[m, who, rows, :])
                fa[:, rows] = value

    def piece_last():
        @pl.loop(0, length // ROWS)
        def _(i):
            rows = aligned(i * ROWS, ROWS)
            scaled, inverse = row_stats(xb[rows, :].astype(F32))
            up = fa[rows, :]
            add_vec(0, up * scaled)
            add_vec(1, up)
            fa[rows, :] = fb[rows, :] + norm_pull(up, scaled, inverse, pre_gain[...])

        pltpu.make_async_copy(fa, gx_out, load_sem.at[4]).start()
        v_copy(0, to_core).start()

    stages = [stage0, stage1, stage2, stage3, stage4, stage5, stage6]

    lags = [0, 1, 3, 4, 5, 6, 7]

    @pl.loop(0, CHUNKS + lags[-1])
    def _(tick):
        @pl.when(tick == 0)
        def _():
            gather_second(5)
            gather_near(5)
            gather_far(5)
            piece_out()

        pl.when(tick == 1)(piece_mid)
        pl.when(tick == 2)(piece_mixed)

        @pl.when((tick >= 2) & (tick < 10))
        def _():
            order = tick - 2
            piece_head(2 * lax.rem(order, 4) + lax.div(order, 4))

        pl.when(tick == 10)(piece_input)
        pl.when(tick == 11)(piece_last)
        for lag, stage in zip(lags, stages):
            k = tick - lag

            @pl.when((k >= 0) & (k < CHUNKS))
            def _():
                stage(jnp.clip(k, 0, CHUNKS - 1))

        for i, target in ((0, to_y), (1, to_x)):
            @pl.when(tick == 12 + i)
            def _():
                v_copy(i, to_core).wait_recv()
                vec[16 * (i + 1) : 16 * (i + 2), :] = vec[16 * i : 16 * (i + 1), :] + vrecv[i]
                v_copy(i + 1, target).start()

        @pl.when(tick == 14)
        def _():
            v_copy(2, to_x).wait_recv()
            vz[rz] = vec[32:48, :] + vrecv[2]
            for offset in range(1, lines):
                vz_copy(offset).start()

        @pl.when(tick == 16)
        def _():
            vz_all().wait_recv()
            value = vz[0]
            for i in range(1, lines):
                value = value + vz[i]
            vec_out[...] = value

    for w in range(6):
        y_copy(w, me).wait_send()
        core_copy(w, me).wait_send()
        x_copy(w, px).wait_send()
        a_copy(w, t_y).wait_send()
        b_copy(w, t_y).wait_send()
    for i in range(3):
        bias_copy(i, me, to_core).wait_send()
        v_copy(i, to_core).wait_send()
    vz_all().wait_send()

    @pl.loop(0, CHUNKS)
    def _(k):
        c_copy(k).wait_send()
        yg_copy(k).wait_send()
        xg_copy(k).wait_send()
        z_all(k).wait_send()
        az_all(k).wait_send()
        ax_copy(k, px).wait_send()
        out_copy(k).wait()

    pltpu.make_async_copy(fa, gx_out, load_sem.at[4]).wait()


PAIRS = ((6, 9), (7, 10), (8, 11), (2, 3), (4, 5), (0, 1))


def finish_kernel(
    grads, y_in, gx_in, sums,
    y_out, gx_out, g_query, g_key, g_value, g_up, g_out, g_down,
    v0, v1, v2, v3, v4, v5, b0, b1, b2,
    low, high, tall, yb, gb, in_sem, out_sem,
):
    per = high.shape[2]
    me = lax.axis_index("tensor")
    loads = [
        pltpu.make_async_copy(grads.at[k], low.at[m, i], in_sem.at[2 * m + i])
        for m, pair in enumerate(PAIRS)
        for i, k in enumerate(pair)
    ]
    loads += [pltpu.make_async_copy(y_in, yb, in_sem.at[12]), pltpu.make_async_copy(gx_in, gb, in_sem.at[13])]
    stores = [
        pltpu.make_async_copy(high.at[m], out, out_sem.at[m])
        for m, out in enumerate((g_query, g_key, g_value, g_up))
    ]
    stores += [pltpu.make_async_copy(tall.at[m], out, out_sem.at[4 + m]) for m, out in enumerate((g_out, g_down))]
    stores += [pltpu.make_async_copy(yb, y_out, out_sem.at[6]), pltpu.make_async_copy(gb, gx_out, out_sem.at[7])]
    for copy in loads[12:]:
        copy.start()
    for copy in loads[:12]:
        copy.start()
    for out, row in ((v0, 0), (v1, 1), (v2, 2), (v3, 3), (v4, 4), (v5, 5)):
        out[...] = sums[row : row + 1, :]
    for out, row in ((b0, 6), (b1, 7), (b2, 8)):
        out[...] = sums[row : row + 1, aligned(me * per, per)]
    for i in range(2):
        loads[12 + i].wait()
        stores[6 + i].start()
    for m in range(6):
        loads[2 * m].wait()
        loads[2 * m + 1].wait()
        for i in range(2):
            if m < 4:
                high[m, :, i * BLOCK : (i + 1) * BLOCK] = low[m, i].astype(F32)
            else:
                tall[m - 4, i * BLOCK : (i + 1) * BLOCK, :] = low[m, i].astype(F32).T
        stores[m].start()
    for copy in stores:
        copy.wait()


def shards_of(
    lines,
    latents, cotangent, counts, assign, pre_gain, pre_shift, w_query, b_query, w_key, w_value, b_value,
    w_out, b_out, mid_gain, mid_shift, w_up, b_up, w_down, b_down,
):
    _, length, width = latents.shape
    per = w_query.shape[1]
    half = width // 2
    line = lambda a: a.reshape(1, -1)
    anywhere = pl.BlockSpec(memory_space=pl.ANY)
    inside = pl.BlockSpec(memory_space=pltpu.VMEM)
    dma = pltpu.SemaphoreType.DMA
    y_out, gx_out, grads, sums = pl.pallas_call(
        partial(step_kernel, lines),
        out_shape=(
            jax.ShapeDtypeStruct((length, width), BF16),
            jax.ShapeDtypeStruct((length, width), F32),
            jax.ShapeDtypeStruct((CHUNKS, width, BLOCK), BF16),
            jax.ShapeDtypeStruct((16, width), F32),
        ),
        in_specs=[anywhere] * 2 + [inside] * 8 + [anywhere] * 9,
        out_specs=(anywhere, anywhere, anywhere, inside),
        scratch_shapes=[
            pltpu.VMEM((4, 4, width, per), BF16),
            pltpu.VMEM((2, 4, per, width), BF16),
            pltpu.VMEM((4, 8, per), F32),
            pltpu.VMEM((length, width), BF16),
            pltpu.VMEM((length, width), BF16),
            pltpu.VMEM((length, width), BF16),
            pltpu.VMEM((length, width), BF16),
            pltpu.VMEM((4, width, length), BF16),
            pltpu.VMEM((6, length, width), BF16),
            pltpu.VMEM((length, width), F32),
            pltpu.VMEM((length, width), F32),
            pltpu.VMEM((48, width), F32),
            pltpu.VMEM((CHUNKS, 2, width, BLOCK), BF16),
            pltpu.VMEM((CHUNKS, 2, width, BLOCK), BF16),
            pltpu.VMEM((CHUNKS, width, BLOCK), BF16),
            pltpu.VMEM((CHUNKS, width, BLOCK), BF16),
            pltpu.VMEM((CHUNKS, half, BLOCK), BF16),
            pltpu.VMEM((CHUNKS, half, BLOCK), BF16),
            pltpu.VMEM((CHUNKS, half, BLOCK), BF16),
            pltpu.VMEM((CHUNKS, lines - 1, half // lines, BLOCK), BF16),
            pltpu.VMEM((CHUNKS, width, BLOCK), BF16),
            pltpu.VMEM((3, 16, width), F32),
            pltpu.VMEM((lines, 16, width), F32),
            dma((7,)), dma((6,)), dma((CHUNKS,)),
        ]
        + [dma((6,))] * 10
        + [dma((3,))] * 2
        + [dma((CHUNKS,))] * 12
        + [dma((4,))] * 2,
        compiler_params=pltpu.CompilerParams(
            collective_id=0, has_side_effects=True, vmem_limit_bytes=67043328
        ),
    )(
        latents.reshape(length, width), cotangent.reshape(length, width), line(counts), line(assign),
        line(pre_gain), line(pre_shift), line(b_out), line(mid_gain), line(mid_shift), line(b_down),
        line(b_query), line(b_value), line(b_up),
        w_query, w_key, w_value, w_out, w_up, w_down,
    )

    full = jax.ShapeDtypeStruct((1, width), F32)
    own = jax.ShapeDtypeStruct((1, per), F32)
    wide = jax.ShapeDtypeStruct((width, per), F32)
    flat = jax.ShapeDtypeStruct((per, width), F32)
    results = pl.pallas_call(
        finish_kernel,
        out_shape=(
            jax.ShapeDtypeStruct((length, width), BF16),
            jax.ShapeDtypeStruct((length, width), F32),
            *[wide] * 4, *[flat] * 2, *[full] * 6, *[own] * 3,
        ),
        in_specs=[anywhere] * 3 + [inside],
        out_specs=(*[anywhere] * 8, *[inside] * 9),
        scratch_shapes=[
            pltpu.VMEM((6, 2, width, BLOCK), BF16),
            pltpu.VMEM((4, width, per), F32),
            pltpu.VMEM((2, per, width), F32),
            pltpu.VMEM((length, width), BF16),
            pltpu.VMEM((length, width), F32),
            dma((14,)), dma((8,)),
        ],
        compiler_params=pltpu.CompilerParams(vmem_limit_bytes=67043328),
    )(grads, y_out, gx_out, sums)
    y_out, gx_out, g_query, g_key, g_value, g_up, g_out, g_down = results[:8]
    v0, v1, v2, v3, v4, v5, b0, b1, b2 = [a.reshape(-1) for a in results[8:]]
    return (
        y_out.reshape(latents.shape), gx_out.reshape(latents.shape),
        v0, v1, g_query, b0, g_key, g_value, b1, g_out, v2, v3, v4, g_up, b2, g_down, v5,
    )


def solution(mesh):
    assert mesh.shape["tensor"] == 4
    return jax.shard_map(
        partial(shards_of, mesh.shape["dp"] // 2),
        mesh=mesh,
        in_specs=(
            P(("dp", "tensor"), None, None),
            P(("dp", "tensor"), None, None),
            P(),
            P(),
            P(),
            P(),
            P(None, "tensor"),
            P("tensor"),
            P(None, "tensor"),
            P(None, "tensor"),
            P("tensor"),
            P("tensor", None),
            P(),
            P(),
            P(),
            P(None, "tensor"),
            P("tensor"),
            P("tensor", None),
            P(),
        ),
        out_specs=(
            P(("dp", "tensor"), None, None),
            P(("dp", "tensor"), None, None),
            P(),
            P(),
            P(None, "tensor"),
            P("tensor"),
            P(None, "tensor"),
            P(None, "tensor"),
            P("tensor"),
            P("tensor", None),
            P(),
            P(),
            P(),
            P(None, "tensor"),
            P("tensor"),
            P("tensor", None),
            P(),
        ),
        check_vma=False,
    )
```

```python
from functools import partial
import math

import jax
import jax.numpy as jnp
from jax import lax
from jax.experimental import pallas as pl
from jax.experimental.pallas import tpu as pltpu
from jax.sharding import PartitionSpec as P

HEAD = 128
EPS = 1e-05
CHUNKS = 12
BLOCK = 128
ROWS = 128
LAGS = (0, 1, 3, 5, 7, 9, 11)
WEAVE = dict(up=1, down=3, mid=5, mixed=7, even=8, odd=12, out=16, input=18, last=22)
F32 = jnp.float32
BF16 = jnp.bfloat16
MESH = pl.DeviceIdType.MESH


def dot(left, right):
    return lax.dot_general(left, right, (((1,), (0,)), ((), ())), preferred_element_type=F32)


def dot_nt(left, right):
    return lax.dot_general(left, right, (((1,), (1,)), ((), ())), preferred_element_type=F32)


def dot_tn(left, right):
    return lax.dot_general(left, right, (((0,), (0,)), ((), ())), preferred_element_type=F32)


def aligned(start, size):
    return pl.ds(pl.multiple_of(start, size), size)


def row_stats(values):
    center = jnp.mean(values, axis=-1, keepdims=True)
    centered = values - center
    inverse = lax.rsqrt(jnp.mean(centered * centered, axis=-1, keepdims=True) + EPS)
    return centered * inverse, inverse


def norm_pull(upstream, scaled, inverse, gain):
    weighted = upstream * gain
    first = jnp.mean(weighted, axis=-1, keepdims=True)
    second = jnp.mean(weighted * scaled, axis=-1, keepdims=True)
    return inverse * (weighted - first - scaled * second)


def step_kernel(
    lines, split, lags, weave,
    lat, cot, counts, assign, pre_gain, pre_shift, b_out, mid_gain, mid_shift, b_down, b_query, b_value, b_up,
    w_query, w_key, w_value, w_out, w_up, w_down,
    y_out, gx_out, grads_out, vec_out,
    wc, wr, bias, xb, dy, n1, n2, lhs, rhs, fa, fb, vec,
    csend, crecv, ysend, yrecv, xsend, xrecv, zsend, zrecv, gathered, vrecv, vz,
    load_sem, own_sem, out_sem,
    gc_s, gc_r, gy_s, gy_r, gx_s, gx_r, ga_s, ga_r, gb_s, gb_r, bias_s, bias_r,
    c_s, c_r, y_s, y_r, x_s, x_r, z_s, z_r, az_s, az_r, ax_s, ax_r, v_s, v_r,
):
    length, width = xb.shape
    per = wc.shape[3]
    chunks = CHUNKS * split
    tall = width // split
    half = tall // 2
    piece = half // lines
    scaling = 1.0 / math.sqrt(HEAD)
    dp = lax.axis_index("dp")
    me = lax.axis_index("tensor")
    px, rz = lax.rem(dp, 2), lax.div(dp, 2)
    core, yy = lax.rem(me, 2), lax.div(me, 2)
    t_core, t_y, t_diag = me + 1 - 2 * core, me + 2 - 4 * yy, 3 - me
    to_core, to_y, to_diag = {"tensor": t_core}, {"tensor": t_y}, {"tensor": t_diag}
    to_x = {"dp": dp + 1 - 2 * px}

    def to_z(offset):
        return {"dp": lax.rem(rz + offset, lines) * 2 + px}

    def remote(src, dst, send, recv, target):
        return pltpu.make_async_remote_copy(
            src_ref=src, dst_ref=dst, send_sem=send, recv_sem=recv, device_id=target, device_id_type=MESH
        )

    loads = [
        pltpu.make_async_copy(lat, xb, load_sem.at[0]),
        pltpu.make_async_copy(cot, dy, load_sem.at[1]),
        pltpu.make_async_copy(b_query, bias.at[me, 0:1], load_sem.at[2]),
        pltpu.make_async_copy(b_value, bias.at[me, 1:2], load_sem.at[5]),
        pltpu.make_async_copy(b_up, bias.at[me, 2:3], load_sem.at[6]),
    ]
    for copy in loads:
        copy.start()
    barrier = pltpu.get_barrier_semaphore()
    for target in [to_core, to_y, to_diag, to_x] + [to_z(i) for i in range(1, lines)]:
        pl.semaphore_signal(barrier, inc=1, device_id=target, device_id_type=MESH)
    pl.semaphore_wait(barrier, 3 + lines)

    shards = [
        (w_query, wc.at[0]), (w_key, wc.at[1]), (w_value, wc.at[2]),
        (w_out, wr.at[0]), (w_up, wc.at[3]), (w_down, wr.at[1]),
    ]

    def part(ref, index):
        size = ref.shape[0] // 2
        return ref.at[aligned(index * size, size)]

    def own_copy(w):
        return pltpu.make_async_copy(shards[w][0], shards[w][1].at[me], own_sem.at[w])

    def core_copy(w, who):
        return remote(shards[w][0], shards[w][1].at[who], gc_s.at[w], gc_r.at[w], to_core)

    def y_copy(w, who):
        return remote(part(shards[w][0], px), part(shards[w][1].at[who], px), gy_s.at[w], gy_r.at[w], to_y)

    def x_copy(w, which):
        ref = part(shards[w][1].at[t_y], which)
        return remote(ref, ref, gx_s.at[w], gx_r.at[w], to_x)

    def a_copy(w, who):
        ref = part(shards[w][1].at[who], px)
        return remote(ref, ref, ga_s.at[w], ga_r.at[w], to_core)

    def b_copy(w, who):
        ref = part(shards[w][1].at[who], 1 - px)
        return remote(ref, ref, gb_s.at[w], gb_r.at[w], to_core)

    def bias_copy(i, who, target):
        ref = bias.at[who, 0:3]
        return remote(ref, ref, bias_s.at[i], bias_r.at[i], target)

    y_copy(0, me).start()
    for w in range(6):
        core_copy(w, me).start()
        own_copy(w).start()
    for copy in loads[2:]:
        copy.wait()
    for i, target in enumerate((to_core, to_y, to_diag)):
        bias_copy(i, me, target).start()

    def gather_first(w):
        y_copy(w, t_y).wait_recv()
        if w + 2 < 6:
            y_copy(w + 2, me).start()
        x_copy(w, px).start()
        a_copy(w, t_y).start()

    def gather_second(w):
        x_copy(w, 1 - px).wait_recv()
        b_copy(w, t_y).start()

    def gather_near(w):
        own_copy(w).wait()
        core_copy(w, t_core).wait_recv()

    def gather_far(w):
        a_copy(w, t_diag).wait_recv()
        b_copy(w, t_diag).wait_recv()

    loads[0].wait()
    loads[1].wait()
    total = jnp.sum(jnp.where(assign[...] == dp, counts[...], 0).astype(F32), axis=-1, keepdims=True)
    live = (me.astype(F32) < total).astype(F32)
    vec[...] = jnp.zeros_like(vec)
    for who in range(4):
        bias[who, 3:4, :] = jnp.zeros((1, per), F32)

    def add_vec(row, values):
        vec[row : row + 1, :] += jnp.sum(values, axis=0, keepdims=True)

    @pl.loop(0, length // ROWS)
    def _(i):
        rows = aligned(i * ROWS, ROWS)
        scaled, _ = row_stats(xb[rows, :].astype(F32))
        normed = scaled * pre_gain[...] + pre_shift[...]
        n1[rows, :] = normed.astype(BF16)
        lhs[3, :, rows] = normed.T.astype(BF16)
        grad = dy[rows, :].astype(F32) * live
        dy[rows, :] = grad.astype(BF16)
        lhs[0, :, rows] = grad.T.astype(BF16)
        add_vec(5, grad)

        @pl.when(i == 1)
        def _():
            y_copy(1, me).start()

    for i, who in enumerate((t_core, t_y, t_diag)):
        bias_copy(i, who, to_core).wait_recv()

    def project(who):
        columns = aligned(who * per, per)

        @pl.loop(0, 3)
        def _(i):
            value = dot(n1[...], wc[i, who]) + bias[who, pl.ds(jnp.where(i == 1, 3, lax.div(i, 2)), 1), :]
            rhs[3 + i, :, columns] = value.astype(BF16)

    def probabilities(rows, columns):
        scores = dot_nt(rhs[3, rows, columns], rhs[4, :, columns]) * scaling
        exponent = jnp.exp(scores - jnp.max(scores, axis=-1, keepdims=True))
        return exponent / jnp.sum(exponent, axis=-1, keepdims=True)

    QROWS = length // 2

    def attend(head):
        columns = aligned(head * HEAD, HEAD)

        @pl.loop(0, 2)
        def _(i):
            rows = aligned(i * QROWS, QROWS)
            probs = probabilities(rows, columns).astype(BF16)
            rhs[2, rows, columns] = dot(probs, rhs[5, :, columns]).astype(BF16)

    for w in range(3):
        gather_near(w)
    for who in (me, t_core):
        project(who)
    gather_first(0)
    for i, who in enumerate((me, t_core)):
        attend(2 * who)
        attend(2 * who + 1)
        gather_first(i + 1)
        gather_second(i)
    gather_first(3)
    gather_second(2)
    for w in range(3):
        gather_far(w)
    for who in (t_y, t_diag):
        project(who)
    gather_first(4)
    gather_second(3)
    for who in (t_y, t_diag):
        attend(2 * who)
        attend(2 * who + 1)

    gather_near(3)
    gather_far(3)

    @pl.loop(0, 4)
    def _(i):
        columns = aligned(i * per, per)
        value = dot(rhs[2], wr[0, :, :, columns].reshape(width, per))
        fa[:, columns] = xb[:, columns].astype(F32) + (value + b_out[:, columns])

    gather_first(5)
    gather_second(4)

    @pl.loop(0, length // ROWS)
    def _(i):
        rows = aligned(i * ROWS, ROWS)
        scaled, _ = row_stats(fa[rows, :])
        normed = scaled * mid_gain[...] + mid_shift[...]
        n2[rows, :] = normed.astype(BF16)
        lhs[1, :, rows] = normed.T.astype(BF16)

    gather_near(4)
    gather_far(4)

    @pl.loop(0, 4)
    def _(i):
        columns = aligned(i * per, per)
        up = dot(n2[...], wc[3, i]) + bias[i, 2:3, :]
        root = math.sqrt(2.0 / math.pi)
        square = up * up
        curve = jnp.tanh(root * up * (1.0 + 0.044715 * square))
        outer = 0.5 * (1.0 + curve)
        rhs[0, :, columns] = (up * outer).astype(BF16)
        slope = root * (1.0 + 3 * 0.044715 * square)
        fb[:, columns] = outer + 0.5 * up * (1.0 - curve * curve) * slope

    def place(k):
        base = lax.div(k, split)
        late = base - 6
        early = late < 0
        which = jnp.where(early, lax.div(base, 2), 3 + lax.rem(late + 6, 3))
        side = jnp.where(early, lax.rem(base, 2), jnp.where(late >= 3, 1, 0))
        return which, side, jnp.minimum(which, 3), lax.rem(k, split) * tall

    def block_of(which, side, who):
        return rhs[which, :, aligned(who * per + side * BLOCK, BLOCK)]

    def c_copy(k):
        return remote(csend.at[k], crecv.at[k], c_s.at[k], c_r.at[k], to_core)

    def yg_copy(k):
        return remote(ysend.at[k], yrecv.at[k], y_s.at[k], y_r.at[k], to_y)

    def xg_copy(k):
        return remote(xsend.at[k], xrecv.at[k], x_s.at[k], x_r.at[k], to_x)

    def z_copy(k, offset):
        peer = lax.rem(rz + offset, lines)
        return remote(
            zsend.at[k, aligned(peer * piece, piece)], zrecv.at[k, offset - 1], z_s.at[k], z_r.at[k], to_z(offset)
        )

    def z_all(k):
        return remote(zrecv.at[k], zrecv.at[k], z_s.at[k], z_r.at[k], to_x)

    def az_copy(k, offset):
        ref = gathered.at[k, aligned(px * half + rz * piece, piece)]
        return remote(ref, ref, az_s.at[k], az_r.at[k], to_z(offset))

    def az_all(k):
        return remote(zrecv.at[k], zrecv.at[k], az_s.at[k], az_r.at[k], to_x)

    def ax_copy(k, which):
        ref = gathered.at[k, aligned(which * half, half)]
        return remote(ref, ref, ax_s.at[k], ax_r.at[k], to_x)

    def out_copy(k):
        target = grads_out.at[lax.div(k, split), aligned(lax.rem(k, split) * tall, tall)]
        return pltpu.make_async_copy(gathered.at[k], target, out_sem.at[k])

    def stage0(k):
        which, side, left, start = place(k)
        pair = jnp.concatenate(
            [block_of(which, side, 1 - core), block_of(which, side, 3 - core)], axis=1
        )
        size = tall // (2 // split)

        @pl.loop(0, 2 // split)
        def _(i):
            value = dot(lhs[left, aligned(start + i * size, size), :], pair).astype(BF16)
            rows = aligned(i * size, size)
            csend[k, 0, rows, :] = value[:, :BLOCK]
            csend[k, 1, rows, :] = value[:, BLOCK:]

        c_copy(k).start()

    def stage1(k):
        which, side, left, start = place(k)
        c_copy(k).wait_recv()
        value = dot(lhs[left, aligned(start, tall), :], block_of(which, side, t_y))
        ysend[k] = (value + crecv[k, 1 - yy].astype(F32)).astype(BF16)
        yg_copy(k).start()

    def near_sum(k, index):
        which, side, left, start = place(k)
        rows = aligned(index * half, half)
        value = dot(lhs[left, aligned(start + index * half, half), :], block_of(which, side, me))
        return value + crecv[k, yy, rows, :].astype(F32) + yrecv[k, rows, :].astype(F32)

    def stage2(k):
        yg_copy(k).wait_recv()
        xsend[k] = near_sum(k, 1 - px).astype(BF16)
        xg_copy(k).start()

    def stage3(k):
        value = near_sum(k, px)
        xg_copy(k).wait_recv()
        zsend[k] = (value + xrecv[k].astype(F32)).astype(BF16)
        for offset in range(1, lines):
            z_copy(k, offset).start()

    def stage4(k):
        z_all(k).wait_recv()
        value = zsend[k, aligned(rz * piece, piece), :].astype(F32)
        for offset in range(1, lines):
            value = value + zrecv[k, offset - 1].astype(F32)
        gathered[k, aligned(px * half + rz * piece, piece), :] = value.astype(BF16)
        for offset in range(1, lines):
            az_copy(k, offset).start()

    def stage5(k):
        az_all(k).wait_recv()
        ax_copy(k, px).start()

    def stage6(k):
        ax_copy(k, 1 - px).wait_recv()
        out_copy(k).start()

    def v_copy(i, target):
        return remote(vec.at[pl.ds(16 * i, 16)], vrecv.at[i], v_s.at[i], v_r.at[i], target)

    def vz_copy(offset):
        ref = vz.at[rz]
        return remote(ref, ref, v_s.at[3], v_r.at[3], to_z(offset))

    def vz_all():
        ref = vz.at[pl.ds(0, lines - 1)]
        return remote(ref, ref, v_s.at[3], v_r.at[3], to_x)

    def piece_out(i):
        columns = aligned(i * per, per)
        value = dot(rhs[0], wr[1, :, :, columns].reshape(width, per))
        value = fa[:, columns] + (value + b_down[:, columns])
        low = (value * live).astype(BF16)
        n2[:, columns] = low

    def piece_up(i):
        columns = aligned(i * per, per)
        value = (dot_nt(dy[...], wr[1, i]) * fb[:, columns]).astype(BF16)
        rhs[1, :, columns] = value
        vec[8:9, columns] = jnp.sum(value.astype(F32), axis=0, keepdims=True)

    def piece_down(i):
        rows = aligned(i * per, per)
        value = dot_nt(rhs[1, :, :per], wc[3, 0, rows, :])
        for who in range(1, 4):
            value = value + dot_nt(rhs[1, :, who * per : (who + 1) * per], wc[3, who, rows, :])
        fb[:, rows] = value

    def piece_mid(i):
        rows = aligned(i * ROWS, ROWS)
        scaled, inverse = row_stats(fa[rows, :])
        up = fb[rows, :]
        add_vec(3, up * scaled)
        add_vec(4, up)
        value = dy[rows, :].astype(F32) + norm_pull(up, scaled, inverse, mid_gain[...])
        fb[rows, :] = value
        low = value.astype(BF16)
        n2[rows, :] = low
        lhs[2, :, rows] = value.T.astype(BF16)
        add_vec(2, low.astype(F32))

    def piece_mixed(i):
        columns = aligned(i * per, per)
        n1[:, columns] = dot_nt(n2[...], wr[0, i]).astype(BF16)

    def piece_head(head):
        columns = aligned(head * HEAD, HEAD)
        queries, keys, values = rhs[3, :, columns], rhs[4, :, columns], rhs[5, :, columns]
        grad_queries = []
        grad_keys = jnp.zeros((length, HEAD), F32)
        grad_values = jnp.zeros((length, HEAD), F32)
        for i in range(2):
            rows = slice(i * QROWS, (i + 1) * QROWS)
            probs = probabilities(rows, columns)
            upstream = n1[rows, columns]
            grad_values = grad_values + dot_tn(probs.astype(BF16), upstream)
            grad_probs = dot_nt(upstream, values)
            inner = jnp.sum(probs * grad_probs, axis=-1, keepdims=True)
            grad_scores = (probs * (grad_probs - inner)).astype(BF16)
            grad_keys = grad_keys + dot_tn(grad_scores, rhs[3, rows, columns])
            grad_queries.append((dot(grad_scores, keys) * scaling).astype(BF16))
        grad_queries = jnp.concatenate(grad_queries, axis=0)
        grad_values = grad_values.astype(BF16)
        rhs[3, :, columns] = grad_queries
        rhs[4, :, columns] = (grad_keys * scaling).astype(BF16)
        rhs[5, :, columns] = grad_values
        vec[6:7, columns] = jnp.sum(grad_queries.astype(F32), axis=0, keepdims=True)
        vec[7:8, columns] = jnp.sum(grad_values.astype(F32), axis=0, keepdims=True)

    def piece_input(i):
        rows = aligned(i * per, per)
        n1_part = jnp.zeros((length, per), F32)
        for m in range(3):
            for who in range(4):
                n1_part = n1_part + dot_nt(rhs[3 + m, :, who * per : (who + 1) * per], wc[m, who, rows, :])
        fa[:, rows] = n1_part

    def piece_last(i):
        rows = aligned(i * ROWS, ROWS)
        scaled, inverse = row_stats(xb[rows, :].astype(F32))
        up = fa[rows, :]
        add_vec(0, up * scaled)
        add_vec(1, up)
        fa[rows, :] = fb[rows, :] + norm_pull(up, scaled, inverse, pre_gain[...])

    def y_store():
        return pltpu.make_async_copy(n2, y_out, load_sem.at[3])

    def gx_store():
        return pltpu.make_async_copy(fa, gx_out, load_sem.at[4])

    def compute(step):
        def during(first, count, size, run):
            @pl.when((step >= first) & (step < first + count))
            def _():
                @pl.loop(0, size)
                def _(i):
                    run((step - first) * size + i)

        @pl.when(step == weave["up"])
        def _():
            gather_second(5)
            gather_near(5)
            gather_far(5)

        during(weave["up"], 2, 2, piece_up)
        during(weave["down"], 2, 2, piece_down)
        during(weave["mid"], 2, length // ROWS // 2, piece_mid)
        during(weave["mixed"], 1, 4, piece_mixed)
        during(weave["even"], 4, 1, lambda i: piece_head(2 * i))
        during(weave["odd"], 4, 1, lambda i: piece_head(2 * i + 1))
        during(weave["out"], 2, 2, piece_out)
        pl.when(step == weave["out"] + 1)(lambda: y_store().start())
        during(weave["input"], 4, 1, piece_input)
        during(weave["last"], 2, length // ROWS // 2, piece_last)

        @pl.when(step == weave["last"] + 1)
        def _():
            gx_store().start()
            v_copy(0, to_core).start()

    stages = [stage0, stage1, stage2, stage3, stage4, stage5, stage6]

    fine = 2 // split
    after = (weave["last"] + 1) // fine + 1

    @pl.loop(0, chunks + lags[-1])
    def _(tick):
        for lag, stage in zip(lags, stages):
            k = tick - lag

            @pl.when((k >= 0) & (k < chunks))
            def _():
                stage(jnp.clip(k, 0, chunks - 1))

        @pl.loop(0, fine)
        def _(i):
            compute(tick * fine + i)

        for i, target in ((0, to_y), (1, to_x)):
            @pl.when(tick == after + i)
            def _():
                v_copy(i, to_core).wait_recv()
                vec[16 * (i + 1) : 16 * (i + 2), :] = vec[16 * i : 16 * (i + 1), :] + vrecv[i]
                v_copy(i + 1, target).start()

        @pl.when(tick == after + 2)
        def _():
            v_copy(2, to_x).wait_recv()
            vz[rz] = vec[32:48, :] + vrecv[2]
            for offset in range(1, lines):
                vz_copy(offset).start()

        @pl.when(tick == after + 4)
        def _():
            vz_all().wait_recv()
            value = vz[0]
            for i in range(1, lines):
                value = value + vz[i]
            vec_out[...] = value

    for w in range(6):
        y_copy(w, me).wait_send()
        core_copy(w, me).wait_send()
        x_copy(w, px).wait_send()
        a_copy(w, t_y).wait_send()
        b_copy(w, t_y).wait_send()
    for i in range(3):
        bias_copy(i, me, to_core).wait_send()
        v_copy(i, to_core).wait_send()
    vz_all().wait_send()

    @pl.loop(0, chunks)
    def _(k):
        c_copy(k).wait_send()
        yg_copy(k).wait_send()
        xg_copy(k).wait_send()
        z_all(k).wait_send()
        az_all(k).wait_send()
        ax_copy(k, px).wait_send()
        out_copy(k).wait()

    y_store().wait()
    gx_store().wait()


PAIRS = ((6, 9), (7, 10), (8, 11), (2, 3), (4, 5), (0, 1))


def finish_kernel(
    grads, y_in, gx_in, sums,
    y_out, gx_out, g_query, g_key, g_value, g_up, g_out, g_down,
    v0, v1, v2, v3, v4, v5, b0, b1, b2,
    low, high, tall, yb, gb, in_sem, out_sem,
):
    per = high.shape[2]
    me = lax.axis_index("tensor")
    loads = [
        pltpu.make_async_copy(grads.at[k], low.at[m, i], in_sem.at[2 * m + i])
        for m, pair in enumerate(PAIRS)
        for i, k in enumerate(pair)
    ]
    loads += [pltpu.make_async_copy(y_in, yb, in_sem.at[12]), pltpu.make_async_copy(gx_in, gb, in_sem.at[13])]
    stores = [
        pltpu.make_async_copy(high.at[m], out, out_sem.at[m])
        for m, out in enumerate((g_query, g_key, g_value, g_up))
    ]
    stores += [pltpu.make_async_copy(tall.at[m], out, out_sem.at[4 + m]) for m, out in enumerate((g_out, g_down))]
    stores += [pltpu.make_async_copy(yb, y_out, out_sem.at[6]), pltpu.make_async_copy(gb, gx_out, out_sem.at[7])]
    for copy in loads[12:]:
        copy.start()
    for copy in loads[:12]:
        copy.start()
    for out, row in ((v0, 0), (v1, 1), (v2, 2), (v3, 3), (v4, 4), (v5, 5)):
        out[...] = sums[row : row + 1, :]
    for out, row in ((b0, 6), (b1, 7), (b2, 8)):
        out[...] = sums[row : row + 1, aligned(me * per, per)]
    for i in range(2):
        loads[12 + i].wait()
        stores[6 + i].start()
    for m in range(6):
        loads[2 * m].wait()
        loads[2 * m + 1].wait()
        for i in range(2):
            if m < 4:
                high[m, :, i * BLOCK : (i + 1) * BLOCK] = low[m, i].astype(F32)
            else:
                tall[m - 4, i * BLOCK : (i + 1) * BLOCK, :] = low[m, i].astype(F32).T
        stores[m].start()
    for copy in stores:
        copy.wait()


def shards_of(
    lines,
    latents, cotangent, counts, assign, pre_gain, pre_shift, w_query, b_query, w_key, w_value, b_value,
    w_out, b_out, mid_gain, mid_shift, w_up, b_up, w_down, b_down,
):
    _, length, width = latents.shape
    per = w_query.shape[1]
    split = 2 if lines <= 16 else 1
    chunks = CHUNKS * split
    tall = width // split
    half = tall // 2
    line = lambda a: a.reshape(1, -1)
    anywhere = pl.BlockSpec(memory_space=pl.ANY)
    inside = pl.BlockSpec(memory_space=pltpu.VMEM)
    dma = pltpu.SemaphoreType.DMA
    y_out, gx_out, grads, sums = pl.pallas_call(
        partial(step_kernel, lines, split, LAGS, WEAVE),
        out_shape=(
            jax.ShapeDtypeStruct((length, width), BF16),
            jax.ShapeDtypeStruct((length, width), F32),
            jax.ShapeDtypeStruct((CHUNKS, width, BLOCK), BF16),
            jax.ShapeDtypeStruct((16, width), F32),
        ),
        in_specs=[anywhere] * 2 + [inside] * 8 + [anywhere] * 9,
        out_specs=(anywhere, anywhere, anywhere, inside),
        scratch_shapes=[
            pltpu.VMEM((4, 4, width, per), BF16),
            pltpu.VMEM((2, 4, per, width), BF16),
            pltpu.VMEM((4, 8, per), F32),
            pltpu.VMEM((length, width), BF16),
            pltpu.VMEM((length, width), BF16),
            pltpu.VMEM((length, width), BF16),
            pltpu.VMEM((length, width), BF16),
            pltpu.VMEM((4, width, length), BF16),
            pltpu.VMEM((6, length, width), BF16),
            pltpu.VMEM((length, width), F32),
            pltpu.VMEM((length, width), F32),
            pltpu.VMEM((48, width), F32),
            pltpu.VMEM((chunks, 2, tall, BLOCK), BF16),
            pltpu.VMEM((chunks, 2, tall, BLOCK), BF16),
            pltpu.VMEM((chunks, tall, BLOCK), BF16),
            pltpu.VMEM((chunks, tall, BLOCK), BF16),
            pltpu.VMEM((chunks, half, BLOCK), BF16),
            pltpu.VMEM((chunks, half, BLOCK), BF16),
            pltpu.VMEM((chunks, half, BLOCK), BF16),
            pltpu.VMEM((chunks, lines - 1, half // lines, BLOCK), BF16),
            pltpu.VMEM((chunks, tall, BLOCK), BF16),
            pltpu.VMEM((3, 16, width), F32),
            pltpu.VMEM((lines, 16, width), F32),
            dma((7,)), dma((6,)), dma((chunks,)),
        ]
        + [dma((6,))] * 10
        + [dma((3,))] * 2
        + [dma((chunks,))] * 12
        + [dma((4,))] * 2,
        compiler_params=pltpu.CompilerParams(
            collective_id=0, has_side_effects=True, vmem_limit_bytes=67043328
        ),
    )(
        latents.reshape(length, width), cotangent.reshape(length, width), line(counts), line(assign),
        line(pre_gain), line(pre_shift), line(b_out), line(mid_gain), line(mid_shift), line(b_down),
        line(b_query), line(b_value), line(b_up),
        w_query, w_key, w_value, w_out, w_up, w_down,
    )

    full = jax.ShapeDtypeStruct((1, width), F32)
    own = jax.ShapeDtypeStruct((1, per), F32)
    wide = jax.ShapeDtypeStruct((width, per), F32)
    flat = jax.ShapeDtypeStruct((per, width), F32)
    results = pl.pallas_call(
        finish_kernel,
        out_shape=(
            jax.ShapeDtypeStruct((length, width), BF16),
            jax.ShapeDtypeStruct((length, width), F32),
            *[wide] * 4, *[flat] * 2, *[full] * 6, *[own] * 3,
        ),
        in_specs=[anywhere] * 3 + [inside],
        out_specs=(*[anywhere] * 8, *[inside] * 9),
        scratch_shapes=[
            pltpu.VMEM((6, 2, width, BLOCK), BF16),
            pltpu.VMEM((4, width, per), F32),
            pltpu.VMEM((2, per, width), F32),
            pltpu.VMEM((length, width), BF16),
            pltpu.VMEM((length, width), F32),
            dma((14,)), dma((8,)),
        ],
        compiler_params=pltpu.CompilerParams(vmem_limit_bytes=67043328),
    )(grads, y_out, gx_out, sums)
    y_out, gx_out, g_query, g_key, g_value, g_up, g_out, g_down = results[:8]
    v0, v1, v2, v3, v4, v5, b0, b1, b2 = [a.reshape(-1) for a in results[8:]]
    return (
        y_out.reshape(latents.shape), gx_out.reshape(latents.shape),
        v0, v1, g_query, b0, g_key, g_value, b1, g_out, v2, v3, v4, g_up, b2, g_down, v5,
    )


def solution(mesh):
    assert mesh.shape["tensor"] == 4
    return jax.shard_map(
        partial(shards_of, mesh.shape["dp"] // 2),
        mesh=mesh,
        in_specs=(
            P(("dp", "tensor"), None, None),
            P(("dp", "tensor"), None, None),
            P(),
            P(),
            P(),
            P(),
            P(None, "tensor"),
            P("tensor"),
            P(None, "tensor"),
            P(None, "tensor"),
            P("tensor"),
            P("tensor", None),
            P(),
            P(),
            P(),
            P(None, "tensor"),
            P("tensor"),
            P("tensor", None),
            P(),
        ),
        out_specs=(
            P(("dp", "tensor"), None, None),
            P(("dp", "tensor"), None, None),
            P(),
            P(),
            P(None, "tensor"),
            P("tensor"),
            P(None, "tensor"),
            P(None, "tensor"),
            P("tensor"),
            P("tensor", None),
            P(),
            P(),
            P(),
            P(None, "tensor"),
            P("tensor"),
            P("tensor", None),
            P(),
        ),
        check_vma=False,
    )
```

```python
from functools import partial
import math

import jax
import jax.numpy as jnp
from jax import lax
from jax.experimental import pallas as pl
from jax.experimental.pallas import tpu as pltpu
from jax.sharding import PartitionSpec as P

HEAD = 128
EPS = 1e-05
CHUNKS = 12
BLOCK = 128
ROWS = 128
RING = 8
LAGS = {1: (0, 1, 2, 3, 4, 5, 6, 7), 2: (0, 1, 3, 5, 7, 9, 11, 13)}
WEAVE = dict(up=1, down=3, mid=5, mixed=7, even=8, odd=12, out=16, input=18, last=22)
F32 = jnp.float32
BF16 = jnp.bfloat16
MESH = pl.DeviceIdType.MESH


def dot(left, right):
    return lax.dot_general(left, right, (((1,), (0,)), ((), ())), preferred_element_type=F32)


def dot_nt(left, right):
    return lax.dot_general(left, right, (((1,), (1,)), ((), ())), preferred_element_type=F32)


def dot_tn(left, right):
    return lax.dot_general(left, right, (((0,), (0,)), ((), ())), preferred_element_type=F32)


def aligned(start, size):
    return pl.ds(pl.multiple_of(start, size), size)


def row_stats(values):
    center = jnp.mean(values, axis=-1, keepdims=True)
    centered = values - center
    inverse = lax.rsqrt(jnp.mean(centered * centered, axis=-1, keepdims=True) + EPS)
    return centered * inverse, inverse


def norm_pull(upstream, scaled, inverse, gain):
    weighted = upstream * gain
    first = jnp.mean(weighted, axis=-1, keepdims=True)
    second = jnp.mean(weighted * scaled, axis=-1, keepdims=True)
    return inverse * (weighted - first - scaled * second)


def step_kernel(
    lines, split, lags, weave,
    lat, cot, counts, assign, pre_gain, pre_shift, b_out, mid_gain, mid_shift, b_down, b_query, b_value, b_up,
    w_query, w_key, w_value, w_out, w_up, w_down,
    y_out, gx_out, grads_out, vec_out,
    wc, wr, bias, xb, dy, n1, n2, lhs, rhs, fa, fb, vec,
    near, csend, crecv, ysend, yrecv, xsend, xrecv, zsend, zrecv, gathered, vrecv, vz,
    load_sem, own_sem, out_sem,
    gc_s, gc_r, gy_s, gy_r, gx_s, gx_r, gp_s, gp_r, gxx_s, gxx_r, gpp_s, gpp_r, ga_s, ga_r, bias_s, bias_r,
    c_s, c_r, y_s, y_r, x_s, x_r, z_s, z_r, az_s, az_r, bz_s, bz_r, ax_s, ax_r, v_s, v_r,
):
    length, width = xb.shape
    per = wc.shape[3]
    chunks = CHUNKS * split
    tall = width // split
    half = tall // 2
    piece = half // lines
    scaling = 1.0 / math.sqrt(HEAD)
    dp = lax.axis_index("dp")
    me = lax.axis_index("tensor")
    px, rz = lax.rem(dp, 2), lax.div(dp, 2)
    core, yy = lax.rem(me, 2), lax.div(me, 2)
    t_core, t_y, t_diag = me + 1 - 2 * core, me + 2 - 4 * yy, 3 - me
    to_core, to_y, to_diag = {"tensor": t_core}, {"tensor": t_y}, {"tensor": t_diag}
    to_x = {"dp": dp + 1 - 2 * px}
    qz = lax.rem(rz, 2)
    to_pair = {"dp": (rz + 1 - 2 * qz) * 2 + px}

    def to_z(offset):
        return {"dp": lax.rem(rz + offset, lines) * 2 + px}

    def remote(src, dst, send, recv, target):
        return pltpu.make_async_remote_copy(
            src_ref=src, dst_ref=dst, send_sem=send, recv_sem=recv, device_id=target, device_id_type=MESH
        )

    loads = [
        pltpu.make_async_copy(lat, xb, load_sem.at[0]),
        pltpu.make_async_copy(cot, dy, load_sem.at[1]),
        pltpu.make_async_copy(b_query, bias.at[me, 0:1], load_sem.at[2]),
        pltpu.make_async_copy(b_value, bias.at[me, 1:2], load_sem.at[5]),
        pltpu.make_async_copy(b_up, bias.at[me, 2:3], load_sem.at[6]),
    ]
    for copy in loads:
        copy.start()
    barrier = pltpu.get_barrier_semaphore()
    for target in [to_core, to_y, to_diag, to_x] + [to_z(i) for i in range(1, lines)]:
        pl.semaphore_signal(barrier, inc=1, device_id=target, device_id_type=MESH)
    pl.semaphore_wait(barrier, 3 + lines)

    shards = [
        (w_query, wc.at[0]), (w_key, wc.at[1]), (w_value, wc.at[2]),
        (w_out, wr.at[0]), (w_up, wc.at[3]), (w_down, wr.at[1]),
    ]

    def part(ref, index, count):
        size = ref.shape[0] // count
        return ref.at[aligned(index * size, size)]

    def own_copy(w):
        return pltpu.make_async_copy(shards[w][0], shards[w][1].at[me], own_sem.at[w])

    def core_copy(w, who):
        return remote(shards[w][0], shards[w][1].at[who], gc_s.at[0], gc_r.at[w], to_core)

    def y_copy(w, who):
        mine = 2 * px + qz
        return remote(part(shards[w][0], mine, 4), part(shards[w][1].at[who], mine, 4), gy_s.at[0], gy_r.at[w], to_y)

    def x_copy(w, which):
        ref = part(shards[w][1].at[t_y], 2 * which + qz, 4)
        return remote(ref, ref, gx_s.at[0], gx_r.at[w], to_x)

    def p_copy(w, which):
        ref = part(shards[w][1].at[t_y], 2 * px + which, 4)
        return remote(ref, ref, gp_s.at[0], gp_r.at[w], to_pair)

    def xx_copy(w, x_part, z_part):
        ref = part(shards[w][1].at[t_y], 2 * (2 * x_part + z_part), 8)
        return remote(ref, ref, gxx_s.at[0], gxx_r.at[w], to_x)

    def pp_copy(w, x_part, z_part):
        ref = part(shards[w][1].at[t_y], 2 * (2 * x_part + z_part) + 1, 8)
        return remote(ref, ref, gpp_s.at[0], gpp_r.at[w], to_pair)

    def far_copy(w, who):
        ref = shards[w][1].at[who]
        return remote(ref, ref, ga_s.at[0], ga_r.at[w], to_core)

    def bias_copy(i, who, target):
        ref = bias.at[who, 0:3]
        return remote(ref, ref, bias_s.at[i], bias_r.at[i], target)

    y_copy(0, me).start()
    for w in range(6):
        core_copy(w, me).start()
        own_copy(w).start()
    for copy in loads[2:]:
        copy.wait()
    for i, target in enumerate((to_core, to_y, to_diag)):
        bias_copy(i, me, target).start()

    def gather_first(w):
        y_copy(w, t_y).wait_recv()
        if w + 2 < 6:
            y_copy(w + 2, me).start()
        x_copy(w, px).start()
        p_copy(w, qz).start()

    def gather_second(w):
        x_copy(w, 1 - px).wait_recv()
        pp_copy(w, 1 - px, qz).start()
        p_copy(w, 1 - qz).wait_recv()
        xx_copy(w, px, 1 - qz).start()

    def gather_third(w):
        xx_copy(w, 1 - px, 1 - qz).wait_recv()
        pp_copy(w, 1 - px, 1 - qz).wait_recv()
        far_copy(w, t_y).start()

    def gather_near(w):
        own_copy(w).wait()
        core_copy(w, t_core).wait_recv()

    def gather_far(w):
        far_copy(w, t_diag).wait_recv()

    loads[0].wait()
    loads[1].wait()
    total = jnp.sum(jnp.where(assign[...] == dp, counts[...], 0).astype(F32), axis=-1, keepdims=True)
    live = (me.astype(F32) < total).astype(F32)
    vec[...] = jnp.zeros_like(vec)
    for who in range(4):
        bias[who, 3:4, :] = jnp.zeros((1, per), F32)

    def add_vec(row, values):
        vec[row : row + 1, :] += jnp.sum(values, axis=0, keepdims=True)

    @pl.loop(0, length // ROWS)
    def _(i):
        rows = aligned(i * ROWS, ROWS)
        scaled, _ = row_stats(xb[rows, :].astype(F32))
        n1[rows, :] = (scaled * pre_gain[...] + pre_shift[...]).astype(BF16)

    y_copy(1, me).start()

    def prepare(first, count):
        @pl.loop(first, first + count)
        def _(i):
            rows = aligned(i * ROWS, ROWS)
            lhs[3, :, rows] = n1[rows, :].astype(F32).T.astype(BF16)
            grad = dy[rows, :].astype(F32) * live
            dy[rows, :] = grad.astype(BF16)
            lhs[0, :, rows] = grad.T.astype(BF16)
            add_vec(5, grad)

    for i, who in enumerate((t_core, t_y, t_diag)):
        bias_copy(i, who, to_core).wait_recv()

    def project(who):
        columns = aligned(who * per, per)

        @pl.loop(0, 3)
        def _(i):
            value = dot(n1[...], wc[i, who]) + bias[who, pl.ds(jnp.where(i == 1, 3, lax.div(i, 2)), 1), :]
            rhs[3 + i, :, columns] = value.astype(BF16)

    def probabilities(rows, columns):
        scores = dot_nt(rhs[3, rows, columns], rhs[4, :, columns]) * (scaling * math.log2(math.e))
        exponent = jnp.exp2(scores - jnp.max(scores, axis=-1, keepdims=True))
        return exponent * (1.0 / jnp.sum(exponent, axis=-1, keepdims=True))

    QROWS = length // 2

    def attend(head):
        columns = aligned(head * HEAD, HEAD)

        @pl.loop(0, 2)
        def _(i):
            rows = aligned(i * QROWS, QROWS)
            probs = probabilities(rows, columns).astype(BF16)
            rhs[2, rows, columns] = dot(probs, rhs[5, :, columns]).astype(BF16)

    tiles = length // ROWS
    for w in range(3):
        gather_near(w)
    project(me)
    gather_first(0)
    project(t_core)
    gather_first(1)
    prepare(0, tiles // 2)
    gather_second(0)
    attend(2 * me)
    gather_first(2)
    attend(2 * me + 1)
    gather_third(0)
    gather_second(1)
    attend(2 * t_core)
    gather_first(3)
    attend(2 * t_core + 1)
    gather_third(1)
    gather_second(2)
    prepare(tiles // 2, tiles // 4)
    gather_first(4)
    prepare(tiles // 2 + tiles // 4, tiles // 4)
    gather_third(2)
    gather_second(3)
    for w in range(3):
        gather_far(w)
    project(t_y)
    gather_first(5)
    gather_third(3)
    project(t_diag)
    gather_second(4)
    attend(2 * t_y)
    attend(2 * t_y + 1)
    gather_third(4)
    gather_second(5)
    attend(2 * t_diag)
    attend(2 * t_diag + 1)
    gather_third(5)

    gather_near(3)
    gather_far(3)

    @pl.loop(0, 4)
    def _(i):
        columns = aligned(i * per, per)
        value = dot(rhs[2], wr[0, :, :, columns].reshape(width, per))
        fa[:, columns] = xb[:, columns].astype(F32) + (value + b_out[:, columns])

    @pl.loop(0, length // ROWS)
    def _(i):
        rows = aligned(i * ROWS, ROWS)
        scaled, _ = row_stats(fa[rows, :])
        normed = scaled * mid_gain[...] + mid_shift[...]
        n2[rows, :] = normed.astype(BF16)
        lhs[1, :, rows] = normed.T.astype(BF16)

    gather_near(4)
    gather_far(4)

    @pl.loop(0, 4)
    def _(i):
        columns = aligned(i * per, per)
        up = dot(n2[...], wc[3, i]) + bias[i, 2:3, :]
        root = math.sqrt(2.0 / math.pi)
        square = up * up
        curve = jnp.tanh(root * up * (1.0 + 0.044715 * square))
        outer = 0.5 * (1.0 + curve)
        rhs[0, :, columns] = (up * outer).astype(BF16)
        slope = root * (1.0 + 3 * 0.044715 * square)
        fb[:, columns] = outer + 0.5 * up * (1.0 - curve * curve) * slope

    def place(k):
        base = lax.div(k, split)
        late = base - 6
        early = late < 0
        which = jnp.where(early, lax.div(base, 2), 3 + lax.rem(late + 6, 3))
        side = jnp.where(early, lax.rem(base, 2), jnp.where(late >= 3, 1, 0))
        return which, side, jnp.minimum(which, 3), lax.rem(k, split) * tall

    def block_of(which, side, who):
        return rhs[which, :, aligned(who * per + side * BLOCK, BLOCK)]

    def c_copy(k):
        return remote(csend.at[k], crecv.at[k], c_s.at[0], c_r.at[lax.rem(k, RING)], to_core)

    def yg_copy(k):
        return remote(ysend.at[k], yrecv.at[k], y_s.at[0], y_r.at[lax.rem(k, RING)], to_y)

    def xg_copy(k):
        return remote(xsend.at[k], xrecv.at[k], x_s.at[0], x_r.at[lax.rem(k, RING)], to_x)

    def z_copy(k, offset):
        peer = lax.rem(rz + offset, lines)
        return remote(
            zsend.at[k, aligned(slot(peer) * piece, piece)], zrecv.at[k, offset - 1], z_s.at[0], z_r.at[lax.rem(k, RING)], to_z(offset)
        )

    def slot(line):
        return lax.rem(line, 2) * (lines // 2) + lax.div(line, 2)

    def z_all(k):
        return remote(zrecv.at[k], zrecv.at[k], z_s.at[0], z_r.at[lax.rem(k, RING)], to_x)

    def az_copy(k, offset):
        peer = lax.rem(lax.div(rz, 2) + offset, lines // 2) * 2 + lax.rem(rz, 2)
        ref = gathered.at[k, aligned(px * half + slot(rz) * piece, piece)]
        return remote(ref, ref, az_s.at[0], az_r.at[lax.rem(k, RING)], {"dp": peer * 2 + px})

    def az_all(k):
        ref = zrecv.at[k, pl.ds(0, lines // 2 - 1)]
        return remote(ref, ref, az_s.at[0], az_r.at[lax.rem(k, RING)], to_x)

    def bz_copy(k, parity):
        ref = gathered.at[k, aligned(px * half + parity * (half // 2), half // 2)]
        return remote(ref, ref, bz_s.at[0], bz_r.at[lax.rem(k, RING)], to_pair)

    def ax_copy(k, which):
        ref = gathered.at[k, aligned(which * half, half)]
        return remote(ref, ref, ax_s.at[0], ax_r.at[lax.rem(k, RING)], to_x)

    def out_copy(k):
        target = grads_out.at[lax.div(k, split), aligned(lax.rem(k, split) * tall, tall)]
        return pltpu.make_async_copy(gathered.at[k], target, out_sem.at[0])

    def stage0(k):
        which, side, left, start = place(k)
        kept = lax.rem(k, lags[3] + 1)
        size = tall // (2 // split)

        @pl.loop(0, 2 // split)
        def _(i):
            rows = aligned(i * size, size)
            block = lhs[left, aligned(start + i * size, size), :]
            for target, first, second in (
                (csend.at[k], 1 - core, 3 - core), (near.at[kept], core, core + 2),
            ):
                pair = jnp.concatenate([block_of(which, side, first), block_of(which, side, second)], axis=1)
                value = dot(block, pair).astype(BF16)
                target[0, rows, :] = value[:, :BLOCK]
                target[1, rows, :] = value[:, BLOCK:]

        c_copy(k).start()

    def stage1(k):
        c_copy(k).wait_recv()
        value = near[lax.rem(k, lags[3] + 1), 1 - yy].astype(F32) + crecv[k, 1 - yy].astype(F32)
        ysend[k] = value.astype(BF16)
        yg_copy(k).start()

    def near_sum(k, index):
        rows = aligned(index * half, half)
        value = near[lax.rem(k, lags[3] + 1), yy, rows, :].astype(F32) + crecv[k, yy, rows, :].astype(F32)
        return value + yrecv[k, rows, :].astype(F32)

    def stage2(k):
        yg_copy(k).wait_recv()
        xsend[k] = near_sum(k, 1 - px).astype(BF16)
        xg_copy(k).start()

    def stage3(k):
        value = near_sum(k, px)
        xg_copy(k).wait_recv()
        zsend[k] = (value + xrecv[k].astype(F32)).astype(BF16)
        for offset in range(1, lines):
            z_copy(k, offset).start()

    def stage4(k):
        z_all(k).wait_recv()
        value = zsend[k, aligned(slot(rz) * piece, piece), :].astype(F32)
        for offset in range(1, lines):
            value = value + zrecv[k, offset - 1].astype(F32)
        gathered[k, aligned(px * half + slot(rz) * piece, piece), :] = value.astype(BF16)
        for offset in range(1, lines // 2):
            az_copy(k, offset).start()

    def stage5(k):
        az_all(k).wait_recv()
        bz_copy(k, lax.rem(rz, 2)).start()

    def stage6(k):
        bz_copy(k, 1 - lax.rem(rz, 2)).wait_recv()
        ax_copy(k, px).start()

    def stage7(k):
        ax_copy(k, 1 - px).wait_recv()
        out_copy(k).start()

    def v_copy(i, target):
        return remote(vec.at[pl.ds(16 * i, 16)], vrecv.at[i], v_s.at[i], v_r.at[i], target)

    def vz_copy(offset):
        ref = vz.at[rz]
        return remote(ref, ref, v_s.at[3], v_r.at[3], to_z(offset))

    def vz_all():
        ref = vz.at[pl.ds(0, lines - 1)]
        return remote(ref, ref, v_s.at[3], v_r.at[3], to_x)

    def piece_out(i):
        columns = aligned(i * per, per)
        value = dot(rhs[0], wr[1, :, :, columns].reshape(width, per))
        value = fa[:, columns] + (value + b_down[:, columns])
        low = (value * live).astype(BF16)
        n2[:, columns] = low

    def piece_up(i):
        columns = aligned(i * per, per)
        value = (dot_nt(dy[...], wr[1, i]) * fb[:, columns]).astype(BF16)
        rhs[1, :, columns] = value
        vec[8:9, columns] = jnp.sum(value.astype(F32), axis=0, keepdims=True)

    def piece_down(i):
        rows = aligned(i * per, per)
        value = dot_nt(rhs[1, :, :per], wc[3, 0, rows, :])
        for who in range(1, 4):
            value = value + dot_nt(rhs[1, :, who * per : (who + 1) * per], wc[3, who, rows, :])
        fb[:, rows] = value

    def piece_mid(i):
        rows = aligned(i * ROWS, ROWS)
        scaled, inverse = row_stats(fa[rows, :])
        up = fb[rows, :]
        add_vec(3, up * scaled)
        add_vec(4, up)
        value = dy[rows, :].astype(F32) + norm_pull(up, scaled, inverse, mid_gain[...])
        fb[rows, :] = value
        low = value.astype(BF16)
        n2[rows, :] = low
        lhs[2, :, rows] = value.T.astype(BF16)
        add_vec(2, low.astype(F32))

    def piece_mixed(i):
        columns = aligned(i * per, per)
        n1[:, columns] = dot_nt(n2[...], wr[0, i]).astype(BF16)

    def piece_head(head):
        columns = aligned(head * HEAD, HEAD)
        queries, keys, values = rhs[3, :, columns], rhs[4, :, columns], rhs[5, :, columns]
        grad_queries = []
        grad_keys = jnp.zeros((length, HEAD), F32)
        grad_values = jnp.zeros((length, HEAD), F32)
        for i in range(2):
            rows = slice(i * QROWS, (i + 1) * QROWS)
            probs = probabilities(rows, columns)
            upstream = n1[rows, columns]
            grad_values = grad_values + dot_tn(probs.astype(BF16), upstream)
            grad_probs = dot_nt(upstream, values)
            inner = jnp.sum(probs * grad_probs, axis=-1, keepdims=True)
            grad_scores = (probs * (grad_probs - inner)).astype(BF16)
            grad_keys = grad_keys + dot_tn(grad_scores, rhs[3, rows, columns])
            grad_queries.append((dot(grad_scores, keys) * scaling).astype(BF16))
        grad_queries = jnp.concatenate(grad_queries, axis=0)
        grad_values = grad_values.astype(BF16)
        rhs[3, :, columns] = grad_queries
        rhs[4, :, columns] = (grad_keys * scaling).astype(BF16)
        rhs[5, :, columns] = grad_values
        vec[6:7, columns] = jnp.sum(grad_queries.astype(F32), axis=0, keepdims=True)
        vec[7:8, columns] = jnp.sum(grad_values.astype(F32), axis=0, keepdims=True)

    def piece_input(i):
        rows = aligned(i * per, per)
        n1_part = jnp.zeros((length, per), F32)
        for m in range(3):
            for who in range(4):
                n1_part = n1_part + dot_nt(rhs[3 + m, :, who * per : (who + 1) * per], wc[m, who, rows, :])
        fa[:, rows] = n1_part

    def piece_last(i):
        rows = aligned(i * ROWS, ROWS)
        scaled, inverse = row_stats(xb[rows, :].astype(F32))
        up = fa[rows, :]
        add_vec(0, up * scaled)
        add_vec(1, up)
        fa[rows, :] = fb[rows, :] + norm_pull(up, scaled, inverse, pre_gain[...])

    def y_store():
        return pltpu.make_async_copy(n2, y_out, load_sem.at[3])

    def gx_store():
        return pltpu.make_async_copy(fa, gx_out, load_sem.at[4])

    def compute(step):
        def during(first, count, size, run):
            @pl.when((step >= first) & (step < first + count))
            def _():
                @pl.loop(0, size)
                def _(i):
                    run((step - first) * size + i)

        @pl.when(step == weave["up"])
        def _():
            gather_near(5)
            gather_far(5)

        during(weave["up"], 2, 2, piece_up)
        during(weave["down"], 2, 2, piece_down)
        during(weave["mid"], 2, length // ROWS // 2, piece_mid)
        during(weave["mixed"], 1, 4, piece_mixed)
        during(weave["even"], 4, 1, lambda i: piece_head(2 * i))
        during(weave["odd"], 4, 1, lambda i: piece_head(2 * i + 1))
        during(weave["out"], 2, 2, piece_out)
        pl.when(step == weave["out"] + 1)(lambda: y_store().start())
        during(weave["input"], 4, 1, piece_input)
        during(weave["last"], 2, length // ROWS // 2, piece_last)

        @pl.when(step == weave["last"] + 1)
        def _():
            gx_store().start()
            v_copy(0, to_core).start()

    stages = [stage0, stage1, stage2, stage3, stage4, stage5, stage6, stage7]

    fine = 2 // split
    after = (weave["last"] + 1) // fine + 1

    @pl.loop(0, chunks + lags[-1])
    def _(tick):
        for lag, stage in zip(lags, stages):
            k = tick - lag

            @pl.when((k >= 0) & (k < chunks))
            def _():
                stage(jnp.clip(k, 0, chunks - 1))

        @pl.loop(0, fine)
        def _(i):
            compute(tick * fine + i)

        for i, target in ((0, to_y), (1, to_x)):
            @pl.when(tick == after + i)
            def _():
                v_copy(i, to_core).wait_recv()
                vec[16 * (i + 1) : 16 * (i + 2), :] = vec[16 * i : 16 * (i + 1), :] + vrecv[i]
                v_copy(i + 1, target).start()

        @pl.when(tick == after + 2)
        def _():
            v_copy(2, to_x).wait_recv()
            vz[rz] = vec[32:48, :] + vrecv[2]
            for offset in range(1, lines):
                vz_copy(offset).start()

        @pl.when(tick == after + 4)
        def _():
            vz_all().wait_recv()
            value = vz[0]
            for i in range(1, lines):
                value = value + vz[i]
            vec_out[...] = value

    for i in range(3):
        bias_copy(i, me, to_core).wait_send()
        v_copy(i, to_core).wait_send()
    vz_all().wait_send()

    def sent(ref, send, recv):
        remote(ref, ref, send.at[0], recv.at[0], to_core).wait_send()

    some = wc.at[0, pl.ds(0, 3)]
    every = wc.at[pl.ds(0, 3), pl.ds(0, 2)]
    for ref, send, recv in (
        (every, gc_s, gc_r), (every, ga_s, ga_r),
        (some.at[:, pl.ds(0, width // 2)], gy_s, gy_r),
        (some.at[:, pl.ds(0, width // 2)], gx_s, gx_r),
        (some.at[:, pl.ds(0, width // 2)], gp_s, gp_r),
        (some.at[:, pl.ds(0, width // 4)], gxx_s, gxx_r),
        (some.at[:, pl.ds(0, width // 4)], gpp_s, gpp_r),
    ):
        sent(ref, send, recv)
    sent(csend, c_s, c_r)
    sent(ysend, y_s, y_r)
    sent(xsend, x_s, x_r)
    sent(zrecv, z_s, z_r)
    sent(zrecv.at[:, pl.ds(0, lines // 2 - 1)], az_s, az_r)
    sent(xsend.at[:, pl.ds(0, half // 2)], bz_s, bz_r)
    sent(xsend, ax_s, ax_r)
    pltpu.make_async_copy(gathered, gathered, out_sem.at[0]).wait()
    y_store().wait()
    gx_store().wait()


PAIRS = ((6, 9), (7, 10), (8, 11), (2, 3), (4, 5), (0, 1))


def finish_kernel(
    grads, y_in, gx_in, sums,
    y_out, gx_out, g_query, g_key, g_value, g_up, g_out, g_down,
    v0, v1, v2, v3, v4, v5, b0, b1, b2,
    low, high, tall, yb, gb, in_sem, out_sem,
):
    per = high.shape[2]
    me = lax.axis_index("tensor")
    loads = [
        pltpu.make_async_copy(grads.at[k], low.at[m, i], in_sem.at[2 * m + i])
        for m, pair in enumerate(PAIRS)
        for i, k in enumerate(pair)
    ]
    loads += [pltpu.make_async_copy(y_in, yb, in_sem.at[12]), pltpu.make_async_copy(gx_in, gb, in_sem.at[13])]
    stores = [
        pltpu.make_async_copy(high.at[m], out, out_sem.at[m])
        for m, out in enumerate((g_query, g_key, g_value, g_up))
    ]
    stores += [pltpu.make_async_copy(tall.at[m], out, out_sem.at[4 + m]) for m, out in enumerate((g_out, g_down))]
    stores += [pltpu.make_async_copy(yb, y_out, out_sem.at[6]), pltpu.make_async_copy(gb, gx_out, out_sem.at[7])]
    for copy in loads[12:]:
        copy.start()
    for copy in loads[:12]:
        copy.start()
    for out, row in ((v0, 0), (v1, 1), (v2, 2), (v3, 3), (v4, 4), (v5, 5)):
        out[...] = sums[row : row + 1, :]
    for out, row in ((b0, 6), (b1, 7), (b2, 8)):
        out[...] = sums[row : row + 1, aligned(me * per, per)]
    for i in range(2):
        loads[12 + i].wait()
        stores[6 + i].start()
    for m in range(6):
        loads[2 * m].wait()
        loads[2 * m + 1].wait()
        for i in range(2):
            if m < 4:
                high[m, :, i * BLOCK : (i + 1) * BLOCK] = low[m, i].astype(F32)
            else:
                tall[m - 4, i * BLOCK : (i + 1) * BLOCK, :] = low[m, i].astype(F32).T
        stores[m].start()
    for copy in stores:
        copy.wait()


def shards_of(
    lines,
    latents, cotangent, counts, assign, pre_gain, pre_shift, w_query, b_query, w_key, w_value, b_value,
    w_out, b_out, mid_gain, mid_shift, w_up, b_up, w_down, b_down,
):
    _, length, width = latents.shape
    per = w_query.shape[1]
    split = 2 if lines <= 16 else 1
    chunks = CHUNKS * split
    tall = width // split
    half = tall // 2
    line = lambda a: a.reshape(1, -1)
    anywhere = pl.BlockSpec(memory_space=pl.ANY)
    inside = pl.BlockSpec(memory_space=pltpu.VMEM)
    dma = pltpu.SemaphoreType.DMA
    y_out, gx_out, grads, sums = pl.pallas_call(
        partial(step_kernel, lines, split, LAGS[split], WEAVE),
        out_shape=(
            jax.ShapeDtypeStruct((length, width), BF16),
            jax.ShapeDtypeStruct((length, width), F32),
            jax.ShapeDtypeStruct((CHUNKS, width, BLOCK), BF16),
            jax.ShapeDtypeStruct((16, width), F32),
        ),
        in_specs=[anywhere] * 2 + [inside] * 8 + [anywhere] * 9,
        out_specs=(anywhere, anywhere, anywhere, inside),
        scratch_shapes=[
            pltpu.VMEM((4, 4, width, per), BF16),
            pltpu.VMEM((2, 4, per, width), BF16),
            pltpu.VMEM((4, 8, per), F32),
            pltpu.VMEM((length, width), BF16),
            pltpu.VMEM((length, width), BF16),
            pltpu.VMEM((length, width), BF16),
            pltpu.VMEM((length, width), BF16),
            pltpu.VMEM((4, width, length), BF16),
            pltpu.VMEM((6, length, width), BF16),
            pltpu.VMEM((length, width), F32),
            pltpu.VMEM((length, width), F32),
            pltpu.VMEM((48, width), F32),
            pltpu.VMEM((LAGS[split][3] + 1, 2, tall, BLOCK), BF16),
            pltpu.VMEM((chunks, 2, tall, BLOCK), BF16),
            pltpu.VMEM((chunks, 2, tall, BLOCK), BF16),
            pltpu.VMEM((chunks, tall, BLOCK), BF16),
            pltpu.VMEM((chunks, tall, BLOCK), BF16),
            pltpu.VMEM((chunks, half, BLOCK), BF16),
            pltpu.VMEM((chunks, half, BLOCK), BF16),
            pltpu.VMEM((chunks, half, BLOCK), BF16),
            pltpu.VMEM((chunks, lines - 1, half // lines, BLOCK), BF16),
            pltpu.VMEM((chunks, tall, BLOCK), BF16),
            pltpu.VMEM((3, 16, width), F32),
            pltpu.VMEM((lines, 16, width), F32),
            dma((7,)), dma((6,)), dma((1,)),
        ]
        + [dma((1,)), dma((6,))] * 7
        + [dma((3,))] * 2
        + [dma((1,)), dma((RING,))] * 7
        + [dma((4,))] * 2,
        compiler_params=pltpu.CompilerParams(
            collective_id=0, has_side_effects=True, vmem_limit_bytes=67043328
        ),
    )(
        latents.reshape(length, width), cotangent.reshape(length, width), line(counts), line(assign),
        line(pre_gain), line(pre_shift), line(b_out), line(mid_gain), line(mid_shift), line(b_down),
        line(b_query), line(b_value), line(b_up),
        w_query, w_key, w_value, w_out, w_up, w_down,
    )

    full = jax.ShapeDtypeStruct((1, width), F32)
    own = jax.ShapeDtypeStruct((1, per), F32)
    wide = jax.ShapeDtypeStruct((width, per), F32)
    flat = jax.ShapeDtypeStruct((per, width), F32)
    results = pl.pallas_call(
        finish_kernel,
        out_shape=(
            jax.ShapeDtypeStruct((length, width), BF16),
            jax.ShapeDtypeStruct((length, width), F32),
            *[wide] * 4, *[flat] * 2, *[full] * 6, *[own] * 3,
        ),
        in_specs=[anywhere] * 3 + [inside],
        out_specs=(*[anywhere] * 8, *[inside] * 9),
        scratch_shapes=[
            pltpu.VMEM((6, 2, width, BLOCK), BF16),
            pltpu.VMEM((4, width, per), F32),
            pltpu.VMEM((2, per, width), F32),
            pltpu.VMEM((length, width), BF16),
            pltpu.VMEM((length, width), F32),
            dma((14,)), dma((8,)),
        ],
        compiler_params=pltpu.CompilerParams(vmem_limit_bytes=67043328),
    )(grads, y_out, gx_out, sums)
    y_out, gx_out, g_query, g_key, g_value, g_up, g_out, g_down = results[:8]
    v0, v1, v2, v3, v4, v5, b0, b1, b2 = [a.reshape(-1) for a in results[8:]]
    return (
        y_out.reshape(latents.shape), gx_out.reshape(latents.shape),
        v0, v1, g_query, b0, g_key, g_value, b1, g_out, v2, v3, v4, g_up, b2, g_down, v5,
    )


def solution(mesh):
    assert mesh.shape["tensor"] == 4
    return jax.shard_map(
        partial(shards_of, mesh.shape["dp"] // 2),
        mesh=mesh,
        in_specs=(
            P(("dp", "tensor"), None, None),
            P(("dp", "tensor"), None, None),
            P(),
            P(),
            P(),
            P(),
            P(None, "tensor"),
            P("tensor"),
            P(None, "tensor"),
            P(None, "tensor"),
            P("tensor"),
            P("tensor", None),
            P(),
            P(),
            P(),
            P(None, "tensor"),
            P("tensor"),
            P("tensor", None),
            P(),
        ),
        out_specs=(
            P(("dp", "tensor"), None, None),
            P(("dp", "tensor"), None, None),
            P(),
            P(),
            P(None, "tensor"),
            P("tensor"),
            P(None, "tensor"),
            P(None, "tensor"),
            P("tensor"),
            P("tensor", None),
            P(),
            P(),
            P(),
            P(None, "tensor"),
            P("tensor"),
            P("tensor", None),
            P(),
        ),
        check_vma=False,
    )
```

```python
from functools import partial
import math

import jax
import jax.numpy as jnp
from jax import lax
from jax.experimental import pallas as pl
from jax.experimental.pallas import tpu as pltpu
from jax.sharding import PartitionSpec as P

HEAD = 128
EPS = 1e-05
CHUNKS = 12
BLOCK = 128
ROWS = 128
RING = 8
DIRECT = (2, 3, 4)
LAGS = {1: (0, 1, 2, 3, 4, 5, 6, 7), 2: (0, 1, 3, 5, 7, 9, 11, 13)}
WEAVE = dict(up=1, down=3, mid=5, mixed=7, even=8, odd=12, out=10, input=16, last=20)
F32 = jnp.float32
BF16 = jnp.bfloat16
MESH = pl.DeviceIdType.MESH


def dot(left, right):
    return lax.dot_general(left, right, (((1,), (0,)), ((), ())), preferred_element_type=F32)


def dot_nt(left, right):
    return lax.dot_general(left, right, (((1,), (1,)), ((), ())), preferred_element_type=F32)


def dot_tn(left, right):
    return lax.dot_general(left, right, (((0,), (0,)), ((), ())), preferred_element_type=F32)


def aligned(start, size):
    return pl.ds(pl.multiple_of(start, size), size)


def row_stats(values):
    center = jnp.mean(values, axis=-1, keepdims=True)
    centered = values - center
    inverse = lax.rsqrt(jnp.mean(centered * centered, axis=-1, keepdims=True) + EPS)
    return centered * inverse, inverse


def norm_pull(upstream, scaled, inverse, gain):
    weighted = upstream * gain
    first = jnp.mean(weighted, axis=-1, keepdims=True)
    second = jnp.mean(weighted * scaled, axis=-1, keepdims=True)
    return inverse * (weighted - first - scaled * second)


def step_kernel(
    lines, split, lags, weave,
    lat, cot, counts, assign, pre_gain, pre_shift, b_out, mid_gain, mid_shift, b_down, b_query, b_value, b_up,
    w_query, w_key, w_value, w_out, w_up, w_down,
    y_out, gx_out, grads_out, vec_out,
    wc, wr, bias, xb, dy, n1, n2, lhs, rhs, fa, fb, vec,
    near, csend, crecv, ysend, yrecv, xsend, xrecv, zsend, zrecv, gathered, vrecv, vz,
    load_sem, own_sem, out_sem,
    gc_s, gc_r, gy_s, gy_r, gyd_s, gyd_r, gx_s, gx_r, gp_s, gp_r, gxx_s, gxx_r, gpp_s, gpp_r, ga_s, ga_r, bias_s, bias_r,
    c_s, c_r, y_s, y_r, x_s, x_r, z_s, z_r, az_s, az_r, bz_s, bz_r, ax_s, ax_r, v_s, v_r,
):
    length, width = xb.shape
    per = wc.shape[3]
    chunks = CHUNKS * split
    tall = width // split
    half = tall // 2
    piece = half // lines
    scaling = 1.0 / math.sqrt(HEAD)
    dp = lax.axis_index("dp")
    me = lax.axis_index("tensor")
    px, rz = lax.rem(dp, 2), lax.div(dp, 2)
    core, yy = lax.rem(me, 2), lax.div(me, 2)
    t_core, t_y, t_diag = me + 1 - 2 * core, me + 2 - 4 * yy, 3 - me
    to_core, to_y, to_diag = {"tensor": t_core}, {"tensor": t_y}, {"tensor": t_diag}
    to_x = {"dp": dp + 1 - 2 * px}
    qz = lax.rem(rz, 2)
    to_pair = {"dp": (rz + 1 - 2 * qz) * 2 + px}

    def to_z(offset):
        return {"dp": lax.rem(rz + offset, lines) * 2 + px}

    def remote(src, dst, send, recv, target):
        return pltpu.make_async_remote_copy(
            src_ref=src, dst_ref=dst, send_sem=send, recv_sem=recv, device_id=target, device_id_type=MESH
        )

    loads = [
        pltpu.make_async_copy(lat, xb, load_sem.at[0]),
        pltpu.make_async_copy(cot, dy, load_sem.at[1]),
        pltpu.make_async_copy(b_query, bias.at[me, 0:1], load_sem.at[2]),
        pltpu.make_async_copy(b_value, bias.at[me, 1:2], load_sem.at[5]),
        pltpu.make_async_copy(b_up, bias.at[me, 2:3], load_sem.at[6]),
    ]
    for copy in loads:
        copy.start()
    barrier = pltpu.get_barrier_semaphore()
    for target in [to_core, to_y, to_diag, to_x] + [to_z(i) for i in range(1, lines)]:
        pl.semaphore_signal(barrier, inc=1, device_id=target, device_id_type=MESH)
    pl.semaphore_wait(barrier, 3 + lines)

    shards = [
        (w_query, wc.at[0]), (w_key, wc.at[1]), (w_value, wc.at[2]),
        (w_out, wr.at[0]), (w_up, wc.at[3]), (w_down, wr.at[1]),
    ]

    def part(ref, index, count):
        size = ref.shape[0] // count
        return ref.at[aligned(index * size, size)]

    def own_copy(w):
        return pltpu.make_async_copy(shards[w][0], shards[w][1].at[me], own_sem.at[w])

    def core_copy(w, who):
        return remote(shards[w][0], shards[w][1].at[who], gc_s.at[0], gc_r.at[w], to_core)

    def y_copy(w, who):
        mine = 2 * px + qz
        return remote(part(shards[w][0], mine, 4), part(shards[w][1].at[who], mine, 4), gy_s.at[0], gy_r.at[w], to_y)

    def yd_copy(w, who):
        other = 3 - 2 * px - qz
        i = DIRECT.index(w)
        return remote(
            part(shards[w][0], other, 4), part(shards[w][1].at[who], other, 4), gyd_s.at[0], gyd_r.at[i], to_y
        )

    def x_copy(w, which):
        ref = part(shards[w][1].at[t_y], 2 * which + qz, 4)
        return remote(ref, ref, gx_s.at[0], gx_r.at[w], to_x)

    def p_copy(w, which):
        ref = part(shards[w][1].at[t_y], 2 * px + which, 4)
        return remote(ref, ref, gp_s.at[0], gp_r.at[w], to_pair)

    def xx_copy(w, x_part, z_part):
        ref = part(shards[w][1].at[t_y], 2 * (2 * x_part + z_part), 8)
        return remote(ref, ref, gxx_s.at[0], gxx_r.at[w], to_x)

    def pp_copy(w, x_part, z_part):
        ref = part(shards[w][1].at[t_y], 2 * (2 * x_part + z_part) + 1, 8)
        return remote(ref, ref, gpp_s.at[0], gpp_r.at[w], to_pair)

    def far_copy(w, who):
        ref = shards[w][1].at[who]
        return remote(ref, ref, ga_s.at[0], ga_r.at[w], to_core)

    def bias_copy(i, who, target):
        ref = bias.at[who, 0:3]
        return remote(ref, ref, bias_s.at[i], bias_r.at[i], target)

    y_copy(0, me).start()
    for w in range(6):
        core_copy(w, me).start()
        own_copy(w).start()
    for copy in loads[2:]:
        copy.wait()
    for i, target in enumerate((to_core, to_y, to_diag)):
        bias_copy(i, me, target).start()

    def gather_first(w):
        y_copy(w, t_y).wait_recv()
        if w + 2 < 6:
            y_copy(w + 2, me).start()
        x_copy(w, px).start()
        p_copy(w, qz).start()
        if w in DIRECT:
            yd_copy(w, me).start()

    def gather_second(w):
        x_copy(w, 1 - px).wait_recv()
        if w not in DIRECT:
            pp_copy(w, 1 - px, qz).start()
        p_copy(w, 1 - qz).wait_recv()
        if w not in DIRECT:
            xx_copy(w, px, 1 - qz).start()

    def gather_third(w):
        if w in DIRECT:
            yd_copy(w, t_y).wait_recv()
        else:
            xx_copy(w, 1 - px, 1 - qz).wait_recv()
            pp_copy(w, 1 - px, 1 - qz).wait_recv()
        far_copy(w, t_y).start()

    def gather_near(w):
        own_copy(w).wait()
        core_copy(w, t_core).wait_recv()

    def gather_far(w):
        far_copy(w, t_diag).wait_recv()

    loads[0].wait()
    loads[1].wait()
    total = jnp.sum(jnp.where(assign[...] == dp, counts[...], 0).astype(F32), axis=-1, keepdims=True)
    live = (me.astype(F32) < total).astype(F32)
    vec[...] = jnp.zeros_like(vec)
    for who in range(4):
        bias[who, 3:4, :] = jnp.zeros((1, per), F32)

    def add_vec(row, values):
        vec[row : row + 1, :] += jnp.sum(values, axis=0, keepdims=True)

    @pl.loop(0, length // ROWS)
    def _(i):
        rows = aligned(i * ROWS, ROWS)
        scaled, _ = row_stats(xb[rows, :].astype(F32))
        n1[rows, :] = (scaled * pre_gain[...] + pre_shift[...]).astype(BF16)

    y_copy(1, me).start()

    def prepare(first, count):
        @pl.loop(first, first + count)
        def _(i):
            rows = aligned(i * ROWS, ROWS)
            lhs[3, :, rows] = n1[rows, :].astype(F32).T.astype(BF16)
            grad = dy[rows, :].astype(F32) * live
            dy[rows, :] = grad.astype(BF16)
            lhs[0, :, rows] = grad.T.astype(BF16)
            add_vec(5, grad)

    for i, who in enumerate((t_core, t_y, t_diag)):
        bias_copy(i, who, to_core).wait_recv()

    def project(who):
        columns = aligned(who * per, per)

        @pl.loop(0, 3)
        def _(i):
            value = dot(n1[...], wc[i, who]) + bias[who, pl.ds(jnp.where(i == 1, 3, lax.div(i, 2)), 1), :]
            rhs[3 + i, :, columns] = value.astype(BF16)

    def probabilities(rows, columns):
        scores = dot_nt(rhs[3, rows, columns], rhs[4, :, columns]) * (scaling * math.log2(math.e))
        exponent = jnp.exp2(scores - jnp.max(scores, axis=-1, keepdims=True))
        return exponent * (1.0 / jnp.sum(exponent, axis=-1, keepdims=True))

    QROWS = length // 2

    def attend(head):
        columns = aligned(head * HEAD, HEAD)

        @pl.loop(0, 2)
        def _(i):
            rows = aligned(i * QROWS, QROWS)
            probs = probabilities(rows, columns).astype(BF16)
            rhs[2, rows, columns] = dot(probs, rhs[5, :, columns]).astype(BF16)

    tiles = length // ROWS
    for w in range(3):
        gather_near(w)
    project(me)
    gather_first(0)
    project(t_core)
    gather_first(1)
    prepare(0, tiles // 2)
    gather_second(0)
    attend(2 * me)
    gather_first(2)
    attend(2 * me + 1)
    gather_third(0)
    gather_second(1)
    attend(2 * t_core)
    gather_first(3)
    attend(2 * t_core + 1)
    gather_third(1)
    gather_second(2)
    prepare(tiles // 2, tiles // 4)
    gather_first(4)
    prepare(tiles // 2 + tiles // 4, tiles // 4)
    gather_third(2)
    gather_second(3)
    for w in range(3):
        gather_far(w)
    project(t_y)
    gather_first(5)
    gather_third(3)
    project(t_diag)
    gather_second(4)
    attend(2 * t_y)
    attend(2 * t_y + 1)
    gather_third(4)
    gather_second(5)
    attend(2 * t_diag)
    attend(2 * t_diag + 1)
    gather_third(5)

    gather_near(3)
    gather_far(3)

    @pl.loop(0, 4)
    def _(i):
        columns = aligned(i * per, per)
        value = dot(rhs[2], wr[0, :, :, columns].reshape(width, per))
        fa[:, columns] = xb[:, columns].astype(F32) + (value + b_out[:, columns])

    @pl.loop(0, length // ROWS)
    def _(i):
        rows = aligned(i * ROWS, ROWS)
        scaled, _ = row_stats(fa[rows, :])
        normed = scaled * mid_gain[...] + mid_shift[...]
        n2[rows, :] = normed.astype(BF16)
        lhs[1, :, rows] = normed.T.astype(BF16)

    gather_near(4)
    gather_far(4)

    @pl.loop(0, 4)
    def _(i):
        columns = aligned(i * per, per)
        up = dot(n2[...], wc[3, i]) + bias[i, 2:3, :]
        root = math.sqrt(2.0 / math.pi)
        square = up * up
        curve = jnp.tanh(root * up * (1.0 + 0.044715 * square))
        outer = 0.5 * (1.0 + curve)
        rhs[0, :, columns] = (up * outer).astype(BF16)
        slope = root * (1.0 + 3 * 0.044715 * square)
        fb[:, columns] = outer + 0.5 * up * (1.0 - curve * curve) * slope

    def place(k):
        base = lax.div(k, split)
        late = base - 6
        early = late < 0
        which = jnp.where(early, lax.div(base, 2), 3 + lax.rem(late + 6, 3))
        side = jnp.where(early, lax.rem(base, 2), jnp.where(late >= 3, 1, 0))
        return which, side, jnp.minimum(which, 3), lax.rem(k, split) * tall

    def block_of(which, side, who):
        return rhs[which, :, aligned(who * per + side * BLOCK, BLOCK)]

    def c_copy(k):
        return remote(csend.at[k], crecv.at[k], c_s.at[0], c_r.at[lax.rem(k, RING)], to_core)

    def yg_copy(k):
        return remote(ysend.at[k], yrecv.at[k], y_s.at[0], y_r.at[lax.rem(k, RING)], to_y)

    def xg_copy(k):
        return remote(xsend.at[k], xrecv.at[k], x_s.at[0], x_r.at[lax.rem(k, RING)], to_x)

    def z_copy(k, offset):
        peer = lax.rem(rz + offset, lines)
        return remote(
            zsend.at[k, aligned(slot(peer) * piece, piece)], zrecv.at[k, offset - 1], z_s.at[0], z_r.at[lax.rem(k, RING)], to_z(offset)
        )

    def slot(line):
        return lax.rem(line, 2) * (lines // 2) + lax.div(line, 2)

    def z_all(k):
        return remote(zrecv.at[k], zrecv.at[k], z_s.at[0], z_r.at[lax.rem(k, RING)], to_x)

    def az_copy(k, offset):
        peer = lax.rem(lax.div(rz, 2) + offset, lines // 2) * 2 + lax.rem(rz, 2)
        ref = gathered.at[k, aligned(px * half + slot(rz) * piece, piece)]
        return remote(ref, ref, az_s.at[0], az_r.at[lax.rem(k, RING)], {"dp": peer * 2 + px})

    def az_all(k):
        ref = zrecv.at[k, pl.ds(0, lines // 2 - 1)]
        return remote(ref, ref, az_s.at[0], az_r.at[lax.rem(k, RING)], to_x)

    def bz_copy(k, parity):
        ref = gathered.at[k, aligned(px * half + parity * (half // 2), half // 2)]
        return remote(ref, ref, bz_s.at[0], bz_r.at[lax.rem(k, RING)], to_pair)

    def ax_copy(k, which):
        ref = gathered.at[k, aligned(which * half, half)]
        return remote(ref, ref, ax_s.at[0], ax_r.at[lax.rem(k, RING)], to_x)

    def out_copy(k):
        target = grads_out.at[lax.div(k, split), aligned(lax.rem(k, split) * tall, tall)]
        return pltpu.make_async_copy(gathered.at[k], target, out_sem.at[0])

    def stage0(k):
        which, side, left, start = place(k)
        kept = lax.rem(k, lags[3] + 1)
        size = tall // (2 // split)

        @pl.loop(0, 2 // split)
        def _(i):
            rows = aligned(i * size, size)
            block = lhs[left, aligned(start + i * size, size), :]
            for target, first, second in (
                (csend.at[k], 1 - core, 3 - core), (near.at[kept], core, core + 2),
            ):
                pair = jnp.concatenate([block_of(which, side, first), block_of(which, side, second)], axis=1)
                value = dot(block, pair).astype(BF16)
                target[0, rows, :] = value[:, :BLOCK]
                target[1, rows, :] = value[:, BLOCK:]

        c_copy(k).start()

    def stage1(k):
        c_copy(k).wait_recv()
        value = near[lax.rem(k, lags[3] + 1), 1 - yy].astype(F32) + crecv[k, 1 - yy].astype(F32)
        ysend[k] = value.astype(BF16)
        yg_copy(k).start()

    def near_sum(k, index):
        rows = aligned(index * half, half)
        value = near[lax.rem(k, lags[3] + 1), yy, rows, :].astype(F32) + crecv[k, yy, rows, :].astype(F32)
        return value + yrecv[k, rows, :].astype(F32)

    def stage2(k):
        yg_copy(k).wait_recv()
        xsend[k] = near_sum(k, 1 - px).astype(BF16)
        xg_copy(k).start()

    def stage3(k):
        value = near_sum(k, px)
        xg_copy(k).wait_recv()
        zsend[k] = (value + xrecv[k].astype(F32)).astype(BF16)
        for offset in range(1, lines):
            z_copy(k, offset).start()

    def stage4(k):
        z_all(k).wait_recv()
        value = zsend[k, aligned(slot(rz) * piece, piece), :].astype(F32)
        for offset in range(1, lines):
            value = value + zrecv[k, offset - 1].astype(F32)
        gathered[k, aligned(px * half + slot(rz) * piece, piece), :] = value.astype(BF16)
        for offset in range(1, lines // 2):
            az_copy(k, offset).start()

    def stage5(k):
        az_all(k).wait_recv()
        bz_copy(k, lax.rem(rz, 2)).start()

    def stage6(k):
        bz_copy(k, 1 - lax.rem(rz, 2)).wait_recv()
        ax_copy(k, px).start()

    def stage7(k):
        ax_copy(k, 1 - px).wait_recv()
        out_copy(k).start()

    def v_copy(i, target):
        return remote(vec.at[pl.ds(16 * i, 16)], vrecv.at[i], v_s.at[i], v_r.at[i], target)

    def vz_copy(offset):
        ref = vz.at[rz]
        return remote(ref, ref, v_s.at[3], v_r.at[3], to_z(offset))

    def vz_all():
        ref = vz.at[pl.ds(0, lines - 1)]
        return remote(ref, ref, v_s.at[3], v_r.at[3], to_x)

    def piece_out(i):
        columns = aligned(i * per, per)
        value = dot(rhs[0], wr[1, :, :, columns].reshape(width, per))
        value = fa[:, columns] + (value + b_down[:, columns])
        low = (value * live).astype(BF16)
        n2[:, columns] = low

    def piece_up(i):
        columns = aligned(i * per, per)
        value = (dot_nt(dy[...], wr[1, i]) * fb[:, columns]).astype(BF16)
        rhs[1, :, columns] = value
        vec[8:9, columns] = jnp.sum(value.astype(F32), axis=0, keepdims=True)

    def piece_down(i):
        rows = aligned(i * per, per)
        value = dot_nt(rhs[1, :, :per], wc[3, 0, rows, :])
        for who in range(1, 4):
            value = value + dot_nt(rhs[1, :, who * per : (who + 1) * per], wc[3, who, rows, :])
        fb[:, rows] = value

    def piece_mid(i):
        rows = aligned(i * ROWS, ROWS)
        scaled, inverse = row_stats(fa[rows, :])
        up = fb[rows, :]
        add_vec(3, up * scaled)
        add_vec(4, up)
        value = dy[rows, :].astype(F32) + norm_pull(up, scaled, inverse, mid_gain[...])
        fb[rows, :] = value
        low = value.astype(BF16)
        n2[rows, :] = low
        lhs[2, :, rows] = value.T.astype(BF16)
        add_vec(2, low.astype(F32))

    def piece_mixed(i):
        columns = aligned(i * per, per)
        n1[:, columns] = dot_nt(n2[...], wr[0, i]).astype(BF16)

    def piece_head(head):
        columns = aligned(head * HEAD, HEAD)
        queries, keys, values = rhs[3, :, columns], rhs[4, :, columns], rhs[5, :, columns]
        grad_queries = []
        grad_keys = jnp.zeros((length, HEAD), F32)
        grad_values = jnp.zeros((length, HEAD), F32)
        for i in range(2):
            rows = slice(i * QROWS, (i + 1) * QROWS)
            probs = probabilities(rows, columns)
            upstream = n1[rows, columns]
            grad_values = grad_values + dot_tn(probs.astype(BF16), upstream)
            grad_probs = dot_nt(upstream, values)
            inner = jnp.sum(probs * grad_probs, axis=-1, keepdims=True)
            grad_scores = (probs * (grad_probs - inner)).astype(BF16)
            grad_keys = grad_keys + dot_tn(grad_scores, rhs[3, rows, columns])
            grad_queries.append((dot(grad_scores, keys) * scaling).astype(BF16))
        grad_queries = jnp.concatenate(grad_queries, axis=0)
        grad_values = grad_values.astype(BF16)
        rhs[3, :, columns] = grad_queries
        rhs[4, :, columns] = (grad_keys * scaling).astype(BF16)
        rhs[5, :, columns] = grad_values
        vec[6:7, columns] = jnp.sum(grad_queries.astype(F32), axis=0, keepdims=True)
        vec[7:8, columns] = jnp.sum(grad_values.astype(F32), axis=0, keepdims=True)

    def piece_input(i):
        rows = aligned(i * per, per)
        n1_part = jnp.zeros((length, per), F32)
        for m in range(3):
            for who in range(4):
                n1_part = n1_part + dot_nt(rhs[3 + m, :, who * per : (who + 1) * per], wc[m, who, rows, :])
        fa[:, rows] = n1_part

    def piece_last(i):
        rows = aligned(i * ROWS, ROWS)
        scaled, inverse = row_stats(xb[rows, :].astype(F32))
        up = fa[rows, :]
        add_vec(0, up * scaled)
        add_vec(1, up)
        fa[rows, :] = fb[rows, :] + norm_pull(up, scaled, inverse, pre_gain[...])

    def y_store():
        return pltpu.make_async_copy(n2, y_out, load_sem.at[3])

    def gx_store():
        return pltpu.make_async_copy(fa, gx_out, load_sem.at[4])

    def compute(step):
        def during(first, count, size, run):
            @pl.when((step >= first) & (step < first + count))
            def _():
                @pl.loop(0, size)
                def _(i):
                    run((step - first) * size + i)

        @pl.when(step == weave["up"])
        def _():
            gather_near(5)
            gather_far(5)

        during(weave["up"], 2, 2, piece_up)
        during(weave["down"], 2, 2, piece_down)
        during(weave["mid"], 2, length // ROWS // 2, piece_mid)
        during(weave["mixed"], 1, 4, piece_mixed)
        during(weave["even"], 4, 1, lambda i: piece_head(2 * i))
        during(weave["odd"], 4, 1, lambda i: piece_head(2 * i + 1))
        during(weave["out"], 4, 1, piece_out)
        pl.when(step == weave["out"] + 3)(lambda: y_store().start())
        during(weave["input"], 4, 1, piece_input)
        during(weave["last"], 2, length // ROWS // 2, piece_last)

        @pl.when(step == weave["last"] + 1)
        def _():
            gx_store().start()
            v_copy(0, to_core).start()

    stages = [stage0, stage1, stage2, stage3, stage4, stage5, stage6, stage7]

    fine = 2 // split
    after = (weave["last"] + 1) // fine + 1

    @pl.loop(0, chunks + lags[-1])
    def _(tick):
        for lag, stage in zip(lags, stages):
            k = tick - lag

            @pl.when((k >= 0) & (k < chunks))
            def _():
                stage(jnp.clip(k, 0, chunks - 1))

        @pl.loop(0, fine)
        def _(i):
            compute(tick * fine + i)

        for i, target in ((0, to_y), (1, to_x)):
            @pl.when(tick == after + i)
            def _():
                v_copy(i, to_core).wait_recv()
                vec[16 * (i + 1) : 16 * (i + 2), :] = vec[16 * i : 16 * (i + 1), :] + vrecv[i]
                v_copy(i + 1, target).start()

        @pl.when(tick == after + 2)
        def _():
            v_copy(2, to_x).wait_recv()
            vz[rz] = vec[32:48, :] + vrecv[2]
            for offset in range(1, lines):
                vz_copy(offset).start()

        @pl.when(tick == after + 4)
        def _():
            vz_all().wait_recv()
            value = vz[0]
            for i in range(1, lines):
                value = value + vz[i]
            vec_out[...] = value

    for i in range(3):
        bias_copy(i, me, to_core).wait_send()
        v_copy(i, to_core).wait_send()
    vz_all().wait_send()

    def sent(ref, send, recv):
        remote(ref, ref, send.at[0], recv.at[0], to_core).wait_send()

    some = wc.at[0, pl.ds(0, 3)]
    three = wc.at[0, pl.ds(0, 3), pl.ds(0, width // 8)]
    six = wc.at[0, pl.ds(0, 3), pl.ds(0, width // 4)]
    every = wc.at[pl.ds(0, 3), pl.ds(0, 2)]
    for ref, send, recv in (
        (every, gc_s, gc_r), (every, ga_s, ga_r),
        (some.at[:, pl.ds(0, width // 2)], gy_s, gy_r),
        (some.at[:, pl.ds(0, width // 2)], gx_s, gx_r),
        (some.at[:, pl.ds(0, width // 2)], gp_s, gp_r),
        (three, gxx_s, gxx_r), (three, gpp_s, gpp_r), (six, gyd_s, gyd_r),
    ):
        sent(ref, send, recv)
    sent(csend, c_s, c_r)
    sent(ysend, y_s, y_r)
    sent(xsend, x_s, x_r)
    sent(zrecv, z_s, z_r)
    sent(zrecv.at[:, pl.ds(0, lines // 2 - 1)], az_s, az_r)
    sent(xsend.at[:, pl.ds(0, half // 2)], bz_s, bz_r)
    sent(xsend, ax_s, ax_r)
    pltpu.make_async_copy(gathered, gathered, out_sem.at[0]).wait()
    y_store().wait()
    gx_store().wait()


PAIRS = ((6, 9), (7, 10), (8, 11), (2, 3), (4, 5), (0, 1))


def finish_kernel(
    grads, y_in, gx_in, sums,
    y_out, gx_out, g_query, g_key, g_value, g_up, g_out, g_down,
    v0, v1, v2, v3, v4, v5, b0, b1, b2,
    low, high, tall, yb, gb, in_sem, out_sem,
):
    per = high.shape[2]
    me = lax.axis_index("tensor")
    loads = [
        pltpu.make_async_copy(grads.at[k], low.at[m, i], in_sem.at[2 * m + i])
        for m, pair in enumerate(PAIRS)
        for i, k in enumerate(pair)
    ]
    loads += [pltpu.make_async_copy(y_in, yb, in_sem.at[12]), pltpu.make_async_copy(gx_in, gb, in_sem.at[13])]
    stores = [
        pltpu.make_async_copy(high.at[m], out, out_sem.at[m])
        for m, out in enumerate((g_query, g_key, g_value, g_up))
    ]
    stores += [pltpu.make_async_copy(tall.at[m], out, out_sem.at[4 + m]) for m, out in enumerate((g_out, g_down))]
    stores += [pltpu.make_async_copy(yb, y_out, out_sem.at[6]), pltpu.make_async_copy(gb, gx_out, out_sem.at[7])]
    for copy in loads[12:]:
        copy.start()
    for copy in loads[:12]:
        copy.start()
    for out, row in ((v0, 0), (v1, 1), (v2, 2), (v3, 3), (v4, 4), (v5, 5)):
        out[...] = sums[row : row + 1, :]
    for out, row in ((b0, 6), (b1, 7), (b2, 8)):
        out[...] = sums[row : row + 1, aligned(me * per, per)]
    for i in range(2):
        loads[12 + i].wait()
        stores[6 + i].start()
    for m in range(6):
        loads[2 * m].wait()
        loads[2 * m + 1].wait()
        for i in range(2):
            if m < 4:
                high[m, :, i * BLOCK : (i + 1) * BLOCK] = low[m, i].astype(F32)
            else:
                tall[m - 4, i * BLOCK : (i + 1) * BLOCK, :] = low[m, i].astype(F32).T
        stores[m].start()
    for copy in stores:
        copy.wait()


def shards_of(
    lines,
    latents, cotangent, counts, assign, pre_gain, pre_shift, w_query, b_query, w_key, w_value, b_value,
    w_out, b_out, mid_gain, mid_shift, w_up, b_up, w_down, b_down,
):
    _, length, width = latents.shape
    per = w_query.shape[1]
    split = 2 if lines <= 16 else 1
    chunks = CHUNKS * split
    tall = width // split
    half = tall // 2
    line = lambda a: a.reshape(1, -1)
    anywhere = pl.BlockSpec(memory_space=pl.ANY)
    inside = pl.BlockSpec(memory_space=pltpu.VMEM)
    dma = pltpu.SemaphoreType.DMA
    y_out, gx_out, grads, sums = pl.pallas_call(
        partial(step_kernel, lines, split, LAGS[split], WEAVE),
        out_shape=(
            jax.ShapeDtypeStruct((length, width), BF16),
            jax.ShapeDtypeStruct((length, width), F32),
            jax.ShapeDtypeStruct((CHUNKS, width, BLOCK), BF16),
            jax.ShapeDtypeStruct((16, width), F32),
        ),
        in_specs=[anywhere] * 2 + [inside] * 8 + [anywhere] * 9,
        out_specs=(anywhere, anywhere, anywhere, inside),
        scratch_shapes=[
            pltpu.VMEM((4, 4, width, per), BF16),
            pltpu.VMEM((2, 4, per, width), BF16),
            pltpu.VMEM((4, 8, per), F32),
            pltpu.VMEM((length, width), BF16),
            pltpu.VMEM((length, width), BF16),
            pltpu.VMEM((length, width), BF16),
            pltpu.VMEM((length, width), BF16),
            pltpu.VMEM((4, width, length), BF16),
            pltpu.VMEM((6, length, width), BF16),
            pltpu.VMEM((length, width), F32),
            pltpu.VMEM((length, width), F32),
            pltpu.VMEM((48, width), F32),
            pltpu.VMEM((LAGS[split][3] + 1, 2, tall, BLOCK), BF16),
            pltpu.VMEM((chunks, 2, tall, BLOCK), BF16),
            pltpu.VMEM((chunks, 2, tall, BLOCK), BF16),
            pltpu.VMEM((chunks, tall, BLOCK), BF16),
            pltpu.VMEM((chunks, tall, BLOCK), BF16),
            pltpu.VMEM((chunks, half, BLOCK), BF16),
            pltpu.VMEM((chunks, half, BLOCK), BF16),
            pltpu.VMEM((chunks, half, BLOCK), BF16),
            pltpu.VMEM((chunks, lines - 1, half // lines, BLOCK), BF16),
            pltpu.VMEM((chunks, tall, BLOCK), BF16),
            pltpu.VMEM((3, 16, width), F32),
            pltpu.VMEM((lines, 16, width), F32),
            dma((7,)), dma((6,)), dma((1,)),
        ]
        + [dma((1,)), dma((6,))] * 2
        + [dma((1,)), dma((3,))]
        + [dma((1,)), dma((6,))] * 5
        + [dma((3,))] * 2
        + [dma((1,)), dma((RING,))] * 7
        + [dma((4,))] * 2,
        compiler_params=pltpu.CompilerParams(
            collective_id=0, has_side_effects=True, vmem_limit_bytes=67043328
        ),
    )(
        latents.reshape(length, width), cotangent.reshape(length, width), line(counts), line(assign),
        line(pre_gain), line(pre_shift), line(b_out), line(mid_gain), line(mid_shift), line(b_down),
        line(b_query), line(b_value), line(b_up),
        w_query, w_key, w_value, w_out, w_up, w_down,
    )

    full = jax.ShapeDtypeStruct((1, width), F32)
    own = jax.ShapeDtypeStruct((1, per), F32)
    wide = jax.ShapeDtypeStruct((width, per), F32)
    flat = jax.ShapeDtypeStruct((per, width), F32)
    results = pl.pallas_call(
        finish_kernel,
        out_shape=(
            jax.ShapeDtypeStruct((length, width), BF16),
            jax.ShapeDtypeStruct((length, width), F32),
            *[wide] * 4, *[flat] * 2, *[full] * 6, *[own] * 3,
        ),
        in_specs=[anywhere] * 3 + [inside],
        out_specs=(*[anywhere] * 8, *[inside] * 9),
        scratch_shapes=[
            pltpu.VMEM((6, 2, width, BLOCK), BF16),
            pltpu.VMEM((4, width, per), F32),
            pltpu.VMEM((2, per, width), F32),
            pltpu.VMEM((length, width), BF16),
            pltpu.VMEM((length, width), F32),
            dma((14,)), dma((8,)),
        ],
        compiler_params=pltpu.CompilerParams(vmem_limit_bytes=67043328),
    )(grads, y_out, gx_out, sums)
    y_out, gx_out, g_query, g_key, g_value, g_up, g_out, g_down = results[:8]
    v0, v1, v2, v3, v4, v5, b0, b1, b2 = [a.reshape(-1) for a in results[8:]]
    return (
        y_out.reshape(latents.shape), gx_out.reshape(latents.shape),
        v0, v1, g_query, b0, g_key, g_value, b1, g_out, v2, v3, v4, g_up, b2, g_down, v5,
    )


def solution(mesh):
    assert mesh.shape["tensor"] == 4
    return jax.shard_map(
        partial(shards_of, mesh.shape["dp"] // 2),
        mesh=mesh,
        in_specs=(
            P(("dp", "tensor"), None, None),
            P(("dp", "tensor"), None, None),
            P(),
            P(),
            P(),
            P(),
            P(None, "tensor"),
            P("tensor"),
            P(None, "tensor"),
            P(None, "tensor"),
            P("tensor"),
            P("tensor", None),
            P(),
            P(),
            P(),
            P(None, "tensor"),
            P("tensor"),
            P("tensor", None),
            P(),
        ),
        out_specs=(
            P(("dp", "tensor"), None, None),
            P(("dp", "tensor"), None, None),
            P(),
            P(),
            P(None, "tensor"),
            P("tensor"),
            P(None, "tensor"),
            P(None, "tensor"),
            P("tensor"),
            P("tensor", None),
            P(),
            P(),
            P(),
            P(None, "tensor"),
            P("tensor"),
            P("tensor", None),
            P(),
        ),
        check_vma=False,
    )
```

```python
from functools import partial
import math

import jax
import jax.numpy as jnp
from jax import lax
from jax.experimental import pallas as pl
from jax.experimental.pallas import tpu as pltpu
from jax.sharding import PartitionSpec as P

HEAD = 128
EPS = 1e-05
CHUNKS = 12
BLOCK = 128
ROWS = 128
RING = 8
DIRECT = (2, 3, 4)
LAGS = {1: (0, 1, 2, 3, 4, 5, 6, 7), 2: (0, 1, 3, 4, 6, 8, 10, 12)}
WEAVE = dict(up=1, down=3, mid=5, mixed=7, even=8, odd=12, out=10, input=16, last=20)
F32 = jnp.float32
BF16 = jnp.bfloat16
MESH = pl.DeviceIdType.MESH


def dot(left, right):
    return lax.dot_general(left, right, (((1,), (0,)), ((), ())), preferred_element_type=F32)


def dot_nt(left, right):
    return lax.dot_general(left, right, (((1,), (1,)), ((), ())), preferred_element_type=F32)


def dot_tn(left, right):
    return lax.dot_general(left, right, (((0,), (0,)), ((), ())), preferred_element_type=F32)


def aligned(start, size):
    return pl.ds(pl.multiple_of(start, size), size)


def row_stats(values):
    center = jnp.mean(values, axis=-1, keepdims=True)
    centered = values - center
    inverse = lax.rsqrt(jnp.mean(centered * centered, axis=-1, keepdims=True) + EPS)
    return centered * inverse, inverse


def norm_pull(upstream, scaled, inverse, gain):
    weighted = upstream * gain
    first = jnp.mean(weighted, axis=-1, keepdims=True)
    second = jnp.mean(weighted * scaled, axis=-1, keepdims=True)
    return inverse * (weighted - first - scaled * second)


def step_kernel(
    lines, split, lags, weave,
    lat, cot, counts, assign, pre_gain, pre_shift, b_out, mid_gain, mid_shift, b_down, b_query, b_value, b_up,
    w_query, w_key, w_value, w_out, w_up, w_down,
    y_out, gx_out, grads_out, vec_out,
    wc, wr, bias, xb, dy, n1, n2, lhs, rhs, fa, fb, vec,
    near, csend, crecv, ysend, yrecv, xsend, xrecv, zsend, zrecv, gathered, vrecv, vz,
    load_sem, own_sem, out_sem,
    gc_s, gc_r, gy_s, gy_r, gyd_s, gyd_r, gx_s, gx_r, gp_s, gp_r, gxx_s, gxx_r, gpp_s, gpp_r, ga_s, ga_r, bias_s, bias_r,
    c_s, c_r, y_s, y_r, x_s, x_r, z_s, z_r, az_s, az_r, bz_s, bz_r, ax_s, ax_r, v_s, v_r,
):
    length, width = xb.shape
    per = wc.shape[3]
    chunks = CHUNKS * split
    tall = width // split
    half = tall // 2
    piece = half // lines
    scaling = 1.0 / math.sqrt(HEAD)
    dp = lax.axis_index("dp")
    me = lax.axis_index("tensor")
    px, rz = lax.rem(dp, 2), lax.div(dp, 2)
    core, yy = lax.rem(me, 2), lax.div(me, 2)
    t_core, t_y, t_diag = me + 1 - 2 * core, me + 2 - 4 * yy, 3 - me
    to_core, to_y, to_diag = {"tensor": t_core}, {"tensor": t_y}, {"tensor": t_diag}
    to_x = {"dp": dp + 1 - 2 * px}
    qz = lax.rem(rz, 2)
    to_pair = {"dp": (rz + 1 - 2 * qz) * 2 + px}

    def to_z(offset):
        return {"dp": lax.rem(rz + offset, lines) * 2 + px}

    def remote(src, dst, send, recv, target):
        return pltpu.make_async_remote_copy(
            src_ref=src, dst_ref=dst, send_sem=send, recv_sem=recv, device_id=target, device_id_type=MESH
        )

    loads = [
        pltpu.make_async_copy(lat, xb, load_sem.at[0]),
        pltpu.make_async_copy(cot, dy, load_sem.at[1]),
        pltpu.make_async_copy(b_query, bias.at[me, 0:1], load_sem.at[2]),
        pltpu.make_async_copy(b_value, bias.at[me, 1:2], load_sem.at[5]),
        pltpu.make_async_copy(b_up, bias.at[me, 2:3], load_sem.at[6]),
    ]
    for copy in loads:
        copy.start()
    barrier = pltpu.get_barrier_semaphore()
    for target in [to_core, to_y, to_diag, to_x] + [to_z(i) for i in range(1, lines)]:
        pl.semaphore_signal(barrier, inc=1, device_id=target, device_id_type=MESH)
    pl.semaphore_wait(barrier, 3 + lines)

    shards = [
        (w_query, wc.at[0]), (w_key, wc.at[1]), (w_value, wc.at[2]),
        (w_out, wr.at[0]), (w_up, wc.at[3]), (w_down, wr.at[1]),
    ]

    def part(ref, index, count):
        size = ref.shape[0] // count
        return ref.at[aligned(index * size, size)]

    def own_copy(w):
        return pltpu.make_async_copy(shards[w][0], shards[w][1].at[me], own_sem.at[w])

    def core_copy(w, who):
        return remote(shards[w][0], shards[w][1].at[who], gc_s.at[0], gc_r.at[w], to_core)

    def y_copy(w, who):
        mine = 2 * px + qz
        return remote(part(shards[w][0], mine, 4), part(shards[w][1].at[who], mine, 4), gy_s.at[0], gy_r.at[w], to_y)

    def yd_copy(w, who):
        other = 3 - 2 * px - qz
        i = DIRECT.index(w)
        return remote(
            part(shards[w][0], other, 4), part(shards[w][1].at[who], other, 4), gyd_s.at[0], gyd_r.at[i], to_y
        )

    def x_copy(w, which):
        ref = part(shards[w][1].at[t_y], 2 * which + qz, 4)
        return remote(ref, ref, gx_s.at[0], gx_r.at[w], to_x)

    def p_copy(w, which):
        ref = part(shards[w][1].at[t_y], 2 * px + which, 4)
        return remote(ref, ref, gp_s.at[0], gp_r.at[w], to_pair)

    def xx_copy(w, x_part, z_part):
        ref = part(shards[w][1].at[t_y], 2 * (2 * x_part + z_part), 8)
        return remote(ref, ref, gxx_s.at[0], gxx_r.at[w], to_x)

    def pp_copy(w, x_part, z_part):
        ref = part(shards[w][1].at[t_y], 2 * (2 * x_part + z_part) + 1, 8)
        return remote(ref, ref, gpp_s.at[0], gpp_r.at[w], to_pair)

    def far_copy(w, who):
        ref = shards[w][1].at[who]
        return remote(ref, ref, ga_s.at[0], ga_r.at[w], to_core)

    def bias_copy(i, who, target):
        ref = bias.at[who, 0:3]
        return remote(ref, ref, bias_s.at[i], bias_r.at[i], target)

    y_copy(0, me).start()
    for w in range(6):
        core_copy(w, me).start()
        own_copy(w).start()
    for copy in loads[2:]:
        copy.wait()
    for i, target in enumerate((to_core, to_y, to_diag)):
        bias_copy(i, me, target).start()

    def gather_first(w):
        y_copy(w, t_y).wait_recv()
        if w + 2 < 6:
            y_copy(w + 2, me).start()
        x_copy(w, px).start()
        p_copy(w, qz).start()
        if w in DIRECT:
            yd_copy(w, me).start()

    def gather_second(w):
        x_copy(w, 1 - px).wait_recv()
        if w not in DIRECT:
            pp_copy(w, 1 - px, qz).start()
        p_copy(w, 1 - qz).wait_recv()
        if w not in DIRECT:
            xx_copy(w, px, 1 - qz).start()

    def gather_third(w):
        if w in DIRECT:
            yd_copy(w, t_y).wait_recv()
        else:
            xx_copy(w, 1 - px, 1 - qz).wait_recv()
            pp_copy(w, 1 - px, 1 - qz).wait_recv()
        far_copy(w, t_y).start()

    def gather_near(w):
        own_copy(w).wait()
        core_copy(w, t_core).wait_recv()

    def gather_far(w):
        far_copy(w, t_diag).wait_recv()

    loads[0].wait()
    loads[1].wait()
    total = jnp.sum(jnp.where(assign[...] == dp, counts[...], 0).astype(F32), axis=-1, keepdims=True)
    live = (me.astype(F32) < total).astype(F32)
    vec[...] = jnp.zeros_like(vec)
    for who in range(4):
        bias[who, 3:4, :] = jnp.zeros((1, per), F32)

    def add_vec(row, values):
        vec[row : row + 1, :] += jnp.sum(values, axis=0, keepdims=True)

    @pl.loop(0, length // ROWS)
    def _(i):
        rows = aligned(i * ROWS, ROWS)
        scaled, _ = row_stats(xb[rows, :].astype(F32))
        n1[rows, :] = (scaled * pre_gain[...] + pre_shift[...]).astype(BF16)

    y_copy(1, me).start()

    def prepare(first, count):
        @pl.loop(first, first + count)
        def _(i):
            rows = aligned(i * ROWS, ROWS)
            lhs[3, :, rows] = n1[rows, :].astype(F32).T.astype(BF16)
            grad = dy[rows, :].astype(F32) * live
            dy[rows, :] = grad.astype(BF16)
            lhs[0, :, rows] = grad.T.astype(BF16)
            add_vec(5, grad)

    for i, who in enumerate((t_core, t_y, t_diag)):
        bias_copy(i, who, to_core).wait_recv()

    def project(who):
        columns = aligned(who * per, per)

        @pl.loop(0, 3)
        def _(i):
            value = dot(n1[...], wc[i, who]) + bias[who, pl.ds(jnp.where(i == 1, 3, lax.div(i, 2)), 1), :]
            rhs[3 + i, :, columns] = value.astype(BF16)

    def probabilities(rows, columns):
        scores = dot_nt(rhs[3, rows, columns], rhs[4, :, columns]) * (scaling * math.log2(math.e))
        exponent = jnp.exp2(scores - jnp.max(scores, axis=-1, keepdims=True))
        return exponent * (1.0 / jnp.sum(exponent, axis=-1, keepdims=True))

    QROWS = length // 2

    def attend(head):
        columns = aligned(head * HEAD, HEAD)

        @pl.loop(0, 2)
        def _(i):
            rows = aligned(i * QROWS, QROWS)
            probs = probabilities(rows, columns).astype(BF16)
            rhs[2, rows, columns] = dot(probs, rhs[5, :, columns]).astype(BF16)

    tiles = length // ROWS
    for w in range(3):
        gather_near(w)
    gather_first(0)
    project(me)
    project(t_core)
    gather_first(1)
    prepare(0, tiles // 2)
    gather_second(0)
    attend(2 * me)
    gather_first(2)
    attend(2 * me + 1)
    gather_third(0)
    gather_second(1)
    attend(2 * t_core)
    gather_first(3)
    attend(2 * t_core + 1)
    gather_third(1)
    gather_second(2)
    prepare(tiles // 2, tiles // 4)
    gather_first(4)
    prepare(tiles // 2 + tiles // 4, tiles // 4)
    gather_third(2)
    gather_second(3)
    for w in range(3):
        gather_far(w)
    project(t_y)
    gather_first(5)
    gather_third(3)
    project(t_diag)
    gather_second(4)
    attend(2 * t_y)
    attend(2 * t_y + 1)
    gather_third(4)
    gather_second(5)
    attend(2 * t_diag)
    attend(2 * t_diag + 1)
    gather_third(5)

    gather_near(3)
    gather_far(3)

    @pl.loop(0, 4)
    def _(i):
        columns = aligned(i * per, per)
        value = dot(rhs[2], wr[0, :, :, columns].reshape(width, per))
        fa[:, columns] = xb[:, columns].astype(F32) + (value + b_out[:, columns])

    @pl.loop(0, length // ROWS)
    def _(i):
        rows = aligned(i * ROWS, ROWS)
        scaled, _ = row_stats(fa[rows, :])
        normed = scaled * mid_gain[...] + mid_shift[...]
        n2[rows, :] = normed.astype(BF16)
        lhs[1, :, rows] = normed.T.astype(BF16)

    gather_near(4)
    gather_far(4)

    @pl.loop(0, 4)
    def _(i):
        columns = aligned(i * per, per)
        up = dot(n2[...], wc[3, i]) + bias[i, 2:3, :]
        root = math.sqrt(2.0 / math.pi)
        square = up * up
        curve = jnp.tanh(root * up * (1.0 + 0.044715 * square))
        outer = 0.5 * (1.0 + curve)
        rhs[0, :, columns] = (up * outer).astype(BF16)
        slope = root * (1.0 + 3 * 0.044715 * square)
        fb[:, columns] = outer + 0.5 * up * (1.0 - curve * curve) * slope

    def place(k):
        base = lax.div(k, split)
        late = base - 6
        early = late < 0
        which = jnp.where(early, lax.div(base, 2), 3 + lax.rem(late + 6, 3))
        side = jnp.where(early, lax.rem(base, 2), jnp.where(late >= 3, 1, 0))
        return which, side, jnp.minimum(which, 3), lax.rem(k, split) * tall

    def block_of(which, side, who):
        return rhs[which, :, aligned(who * per + side * BLOCK, BLOCK)]

    def c_copy(k):
        return remote(csend.at[k], crecv.at[k], c_s.at[0], c_r.at[lax.rem(k, RING)], to_core)

    def yg_copy(k):
        return remote(ysend.at[k], yrecv.at[k], y_s.at[0], y_r.at[lax.rem(k, RING)], to_y)

    def xg_copy(k):
        return remote(xsend.at[k], xrecv.at[k], x_s.at[0], x_r.at[lax.rem(k, RING)], to_x)

    def z_copy(k, offset):
        peer = lax.rem(rz + offset, lines)
        return remote(
            zsend.at[k, aligned(slot(peer) * piece, piece)], zrecv.at[k, offset - 1], z_s.at[0], z_r.at[lax.rem(k, RING)], to_z(offset)
        )

    def slot(line):
        return lax.rem(line, 2) * (lines // 2) + lax.div(line, 2)

    def z_all(k):
        return remote(zrecv.at[k], zrecv.at[k], z_s.at[0], z_r.at[lax.rem(k, RING)], to_x)

    def az_copy(k, offset):
        peer = lax.rem(lax.div(rz, 2) + offset, lines // 2) * 2 + lax.rem(rz, 2)
        ref = gathered.at[k, aligned(px * half + slot(rz) * piece, piece)]
        return remote(ref, ref, az_s.at[0], az_r.at[lax.rem(k, RING)], {"dp": peer * 2 + px})

    def az_all(k):
        ref = zrecv.at[k, pl.ds(0, lines // 2 - 1)]
        return remote(ref, ref, az_s.at[0], az_r.at[lax.rem(k, RING)], to_x)

    def bz_copy(k, parity):
        ref = gathered.at[k, aligned(px * half + parity * (half // 2), half // 2)]
        return remote(ref, ref, bz_s.at[0], bz_r.at[lax.rem(k, RING)], to_pair)

    def ax_copy(k, which):
        ref = gathered.at[k, aligned(which * half, half)]
        return remote(ref, ref, ax_s.at[0], ax_r.at[lax.rem(k, RING)], to_x)

    def out_copy(k):
        target = grads_out.at[lax.div(k, split), aligned(lax.rem(k, split) * tall, tall)]
        return pltpu.make_async_copy(gathered.at[k], target, out_sem.at[0])

    def stage0(k):
        which, side, left, start = place(k)
        kept = lax.rem(k, lags[3] + 1)
        size = tall // (2 // split)

        @pl.loop(0, 2 // split)
        def _(i):
            rows = aligned(i * size, size)
            block = lhs[left, aligned(start + i * size, size), :]
            for target, first, second in (
                (csend.at[k], 1 - core, 3 - core), (near.at[kept], core, core + 2),
            ):
                pair = jnp.concatenate([block_of(which, side, first), block_of(which, side, second)], axis=1)
                value = dot(block, pair).astype(BF16)
                target[0, rows, :] = value[:, :BLOCK]
                target[1, rows, :] = value[:, BLOCK:]

        c_copy(k).start()

    def stage1(k):
        c_copy(k).wait_recv()
        value = near[lax.rem(k, lags[3] + 1), 1 - yy].astype(F32) + crecv[k, 1 - yy].astype(F32)
        ysend[k] = value.astype(BF16)
        yg_copy(k).start()

    def near_sum(k, index):
        rows = aligned(index * half, half)
        value = near[lax.rem(k, lags[3] + 1), yy, rows, :].astype(F32) + crecv[k, yy, rows, :].astype(F32)
        return value + yrecv[k, rows, :].astype(F32)

    def stage2(k):
        yg_copy(k).wait_recv()
        xsend[k] = near_sum(k, 1 - px).astype(BF16)
        xg_copy(k).start()

    def stage3(k):
        value = near_sum(k, px)
        xg_copy(k).wait_recv()
        zsend[k] = (value + xrecv[k].astype(F32)).astype(BF16)
        for offset in range(1, lines):
            z_copy(k, offset).start()

    def stage4(k):
        z_all(k).wait_recv()
        value = zsend[k, aligned(slot(rz) * piece, piece), :].astype(F32)
        for offset in range(1, lines):
            value = value + zrecv[k, offset - 1].astype(F32)
        gathered[k, aligned(px * half + slot(rz) * piece, piece), :] = value.astype(BF16)
        for offset in range(1, lines // 2):
            az_copy(k, offset).start()

    def stage5(k):
        az_all(k).wait_recv()
        bz_copy(k, lax.rem(rz, 2)).start()

    def stage6(k):
        bz_copy(k, 1 - lax.rem(rz, 2)).wait_recv()
        ax_copy(k, px).start()

    def stage7(k):
        ax_copy(k, 1 - px).wait_recv()
        out_copy(k).start()

    def v_copy(i, target):
        return remote(vec.at[pl.ds(16 * i, 16)], vrecv.at[i], v_s.at[i], v_r.at[i], target)

    def vz_copy(offset):
        ref = vz.at[rz]
        return remote(ref, ref, v_s.at[3], v_r.at[3], to_z(offset))

    def vz_all():
        ref = vz.at[pl.ds(0, lines - 1)]
        return remote(ref, ref, v_s.at[3], v_r.at[3], to_x)

    def piece_out(i):
        columns = aligned(i * per, per)
        value = dot(rhs[0], wr[1, :, :, columns].reshape(width, per))
        value = fa[:, columns] + (value + b_down[:, columns])
        low = (value * live).astype(BF16)
        n2[:, columns] = low

    def piece_up(i):
        columns = aligned(i * per, per)
        value = (dot_nt(dy[...], wr[1, i]) * fb[:, columns]).astype(BF16)
        rhs[1, :, columns] = value
        vec[8:9, columns] = jnp.sum(value.astype(F32), axis=0, keepdims=True)

    def piece_down(i):
        rows = aligned(i * per, per)
        value = dot_nt(rhs[1, :, :per], wc[3, 0, rows, :])
        for who in range(1, 4):
            value = value + dot_nt(rhs[1, :, who * per : (who + 1) * per], wc[3, who, rows, :])
        fb[:, rows] = value

    def piece_mid(i):
        rows = aligned(i * ROWS, ROWS)
        scaled, inverse = row_stats(fa[rows, :])
        up = fb[rows, :]
        add_vec(3, up * scaled)
        add_vec(4, up)
        value = dy[rows, :].astype(F32) + norm_pull(up, scaled, inverse, mid_gain[...])
        fb[rows, :] = value
        low = value.astype(BF16)
        n2[rows, :] = low
        lhs[2, :, rows] = value.T.astype(BF16)
        add_vec(2, low.astype(F32))

    def piece_mixed(i):
        columns = aligned(i * per, per)
        n1[:, columns] = dot_nt(n2[...], wr[0, i]).astype(BF16)

    def piece_head(head):
        columns = aligned(head * HEAD, HEAD)
        queries, keys, values = rhs[3, :, columns], rhs[4, :, columns], rhs[5, :, columns]
        grad_queries = []
        grad_keys = jnp.zeros((length, HEAD), F32)
        grad_values = jnp.zeros((length, HEAD), F32)
        for i in range(2):
            rows = slice(i * QROWS, (i + 1) * QROWS)
            probs = probabilities(rows, columns)
            upstream = n1[rows, columns]
            grad_values = grad_values + dot_tn(probs.astype(BF16), upstream)
            grad_probs = dot_nt(upstream, values)
            inner = jnp.sum(probs * grad_probs, axis=-1, keepdims=True)
            grad_scores = (probs * (grad_probs - inner)).astype(BF16)
            grad_keys = grad_keys + dot_tn(grad_scores, rhs[3, rows, columns])
            grad_queries.append((dot(grad_scores, keys) * scaling).astype(BF16))
        grad_queries = jnp.concatenate(grad_queries, axis=0)
        grad_values = grad_values.astype(BF16)
        rhs[3, :, columns] = grad_queries
        rhs[4, :, columns] = (grad_keys * scaling).astype(BF16)
        rhs[5, :, columns] = grad_values
        vec[6:7, columns] = jnp.sum(grad_queries.astype(F32), axis=0, keepdims=True)
        vec[7:8, columns] = jnp.sum(grad_values.astype(F32), axis=0, keepdims=True)

    def piece_input(i):
        rows = aligned(i * per, per)
        n1_part = jnp.zeros((length, per), F32)
        for m in range(3):
            for who in range(4):
                n1_part = n1_part + dot_nt(rhs[3 + m, :, who * per : (who + 1) * per], wc[m, who, rows, :])
        fa[:, rows] = n1_part

    def piece_last(i):
        rows = aligned(i * ROWS, ROWS)
        scaled, inverse = row_stats(xb[rows, :].astype(F32))
        up = fa[rows, :]
        add_vec(0, up * scaled)
        add_vec(1, up)
        fa[rows, :] = fb[rows, :] + norm_pull(up, scaled, inverse, pre_gain[...])

    def y_store():
        return pltpu.make_async_copy(n2, y_out, load_sem.at[3])

    def gx_store():
        return pltpu.make_async_copy(fa, gx_out, load_sem.at[4])

    def compute(step):
        def during(first, count, size, run):
            @pl.when((step >= first) & (step < first + count))
            def _():
                @pl.loop(0, size)
                def _(i):
                    run((step - first) * size + i)

        @pl.when(step == weave["up"])
        def _():
            gather_near(5)
            gather_far(5)

        during(weave["up"], 2, 2, piece_up)
        during(weave["down"], 2, 2, piece_down)
        during(weave["mid"], 2, length // ROWS // 2, piece_mid)
        during(weave["mixed"], 1, 4, piece_mixed)
        during(weave["even"], 4, 1, lambda i: piece_head(2 * i))
        during(weave["odd"], 4, 1, lambda i: piece_head(2 * i + 1))
        during(weave["out"], 4, 1, piece_out)
        pl.when(step == weave["out"] + 3)(lambda: y_store().start())
        during(weave["input"], 4, 1, piece_input)
        during(weave["last"], 2, length // ROWS // 2, piece_last)

        @pl.when(step == weave["last"] + 1)
        def _():
            gx_store().start()
            v_copy(0, to_core).start()

    stages = [stage0, stage1, stage2, stage3, stage4, stage5, stage6, stage7]

    fine = 2 // split
    after = (weave["last"] + 1) // fine + 1

    @pl.loop(0, chunks + lags[-1])
    def _(tick):
        for lag, stage in zip(lags, stages):
            k = tick - lag

            @pl.when((k >= 0) & (k < chunks))
            def _():
                stage(jnp.clip(k, 0, chunks - 1))

        @pl.loop(0, fine)
        def _(i):
            compute(tick * fine + i)

        for i, target in ((0, to_y), (1, to_x)):
            @pl.when(tick == after + i)
            def _():
                v_copy(i, to_core).wait_recv()
                vec[16 * (i + 1) : 16 * (i + 2), :] = vec[16 * i : 16 * (i + 1), :] + vrecv[i]
                v_copy(i + 1, target).start()

        @pl.when(tick == after + 2)
        def _():
            v_copy(2, to_x).wait_recv()
            vz[rz] = vec[32:48, :] + vrecv[2]
            for offset in range(1, lines):
                vz_copy(offset).start()

        @pl.when(tick == after + 4)
        def _():
            vz_all().wait_recv()
            value = vz[0]
            for i in range(1, lines):
                value = value + vz[i]
            vec_out[...] = value

    for i in range(3):
        bias_copy(i, me, to_core).wait_send()
        v_copy(i, to_core).wait_send()
    vz_all().wait_send()

    def sent(ref, send, recv):
        remote(ref, ref, send.at[0], recv.at[0], to_core).wait_send()

    some = wc.at[0, pl.ds(0, 3)]
    three = wc.at[0, pl.ds(0, 3), pl.ds(0, width // 8)]
    six = wc.at[0, pl.ds(0, 3), pl.ds(0, width // 4)]
    every = wc.at[pl.ds(0, 3), pl.ds(0, 2)]
    for ref, send, recv in (
        (every, gc_s, gc_r), (every, ga_s, ga_r),
        (some.at[:, pl.ds(0, width // 2)], gy_s, gy_r),
        (some.at[:, pl.ds(0, width // 2)], gx_s, gx_r),
        (some.at[:, pl.ds(0, width // 2)], gp_s, gp_r),
        (three, gxx_s, gxx_r), (three, gpp_s, gpp_r), (six, gyd_s, gyd_r),
    ):
        sent(ref, send, recv)
    sent(csend, c_s, c_r)
    sent(ysend, y_s, y_r)
    sent(xsend, x_s, x_r)
    sent(zrecv, z_s, z_r)
    sent(zrecv.at[:, pl.ds(0, lines // 2 - 1)], az_s, az_r)
    sent(xsend.at[:, pl.ds(0, half // 2)], bz_s, bz_r)
    sent(xsend, ax_s, ax_r)
    pltpu.make_async_copy(gathered, gathered, out_sem.at[0]).wait()
    y_store().wait()
    gx_store().wait()


PAIRS = ((6, 9), (7, 10), (8, 11), (2, 3), (4, 5), (0, 1))


def finish_kernel(
    grads, y_in, gx_in, sums,
    y_out, gx_out, g_query, g_key, g_value, g_up, g_out, g_down,
    v0, v1, v2, v3, v4, v5, b0, b1, b2,
    low, high, tall, yb, gb, in_sem, out_sem,
):
    per = high.shape[2]
    me = lax.axis_index("tensor")
    loads = [
        pltpu.make_async_copy(grads.at[k], low.at[m, i], in_sem.at[2 * m + i])
        for m, pair in enumerate(PAIRS)
        for i, k in enumerate(pair)
    ]
    loads += [pltpu.make_async_copy(y_in, yb, in_sem.at[12]), pltpu.make_async_copy(gx_in, gb, in_sem.at[13])]
    stores = [
        pltpu.make_async_copy(high.at[m], out, out_sem.at[m])
        for m, out in enumerate((g_query, g_key, g_value, g_up))
    ]
    stores += [pltpu.make_async_copy(tall.at[m], out, out_sem.at[4 + m]) for m, out in enumerate((g_out, g_down))]
    stores += [pltpu.make_async_copy(yb, y_out, out_sem.at[6]), pltpu.make_async_copy(gb, gx_out, out_sem.at[7])]
    for copy in loads[12:]:
        copy.start()
    for copy in loads[:12]:
        copy.start()
    for out, row in ((v0, 0), (v1, 1), (v2, 2), (v3, 3), (v4, 4), (v5, 5)):
        out[...] = sums[row : row + 1, :]
    for out, row in ((b0, 6), (b1, 7), (b2, 8)):
        out[...] = sums[row : row + 1, aligned(me * per, per)]
    for i in range(2):
        loads[12 + i].wait()
        stores[6 + i].start()
    for m in range(6):
        loads[2 * m].wait()
        loads[2 * m + 1].wait()
        for i in range(2):
            if m < 4:
                high[m, :, i * BLOCK : (i + 1) * BLOCK] = low[m, i].astype(F32)
            else:
                tall[m - 4, i * BLOCK : (i + 1) * BLOCK, :] = low[m, i].astype(F32).T
        stores[m].start()
    for copy in stores:
        copy.wait()


def shards_of(
    lines,
    latents, cotangent, counts, assign, pre_gain, pre_shift, w_query, b_query, w_key, w_value, b_value,
    w_out, b_out, mid_gain, mid_shift, w_up, b_up, w_down, b_down,
):
    _, length, width = latents.shape
    per = w_query.shape[1]
    split = 2 if lines <= 16 else 1
    chunks = CHUNKS * split
    tall = width // split
    half = tall // 2
    line = lambda a: a.reshape(1, -1)
    anywhere = pl.BlockSpec(memory_space=pl.ANY)
    inside = pl.BlockSpec(memory_space=pltpu.VMEM)
    dma = pltpu.SemaphoreType.DMA
    y_out, gx_out, grads, sums = pl.pallas_call(
        partial(step_kernel, lines, split, LAGS[split], WEAVE),
        out_shape=(
            jax.ShapeDtypeStruct((length, width), BF16),
            jax.ShapeDtypeStruct((length, width), F32),
            jax.ShapeDtypeStruct((CHUNKS, width, BLOCK), BF16),
            jax.ShapeDtypeStruct((16, width), F32),
        ),
        in_specs=[anywhere] * 2 + [inside] * 8 + [anywhere] * 9,
        out_specs=(anywhere, anywhere, anywhere, inside),
        scratch_shapes=[
            pltpu.VMEM((4, 4, width, per), BF16),
            pltpu.VMEM((2, 4, per, width), BF16),
            pltpu.VMEM((4, 8, per), F32),
            pltpu.VMEM((length, width), BF16),
            pltpu.VMEM((length, width), BF16),
            pltpu.VMEM((length, width), BF16),
            pltpu.VMEM((length, width), BF16),
            pltpu.VMEM((4, width, length), BF16),
            pltpu.VMEM((6, length, width), BF16),
            pltpu.VMEM((length, width), F32),
            pltpu.VMEM((length, width), F32),
            pltpu.VMEM((48, width), F32),
            pltpu.VMEM((LAGS[split][3] + 1, 2, tall, BLOCK), BF16),
            pltpu.VMEM((chunks, 2, tall, BLOCK), BF16),
            pltpu.VMEM((chunks, 2, tall, BLOCK), BF16),
            pltpu.VMEM((chunks, tall, BLOCK), BF16),
            pltpu.VMEM((chunks, tall, BLOCK), BF16),
            pltpu.VMEM((chunks, half, BLOCK), BF16),
            pltpu.VMEM((chunks, half, BLOCK), BF16),
            pltpu.VMEM((chunks, half, BLOCK), BF16),
            pltpu.VMEM((chunks, lines - 1, half // lines, BLOCK), BF16),
            pltpu.VMEM((chunks, tall, BLOCK), BF16),
            pltpu.VMEM((3, 16, width), F32),
            pltpu.VMEM((lines, 16, width), F32),
            dma((7,)), dma((6,)), dma((1,)),
        ]
        + [dma((1,)), dma((6,))] * 2
        + [dma((1,)), dma((3,))]
        + [dma((1,)), dma((6,))] * 5
        + [dma((3,))] * 2
        + [dma((1,)), dma((RING,))] * 7
        + [dma((4,))] * 2,
        compiler_params=pltpu.CompilerParams(
            collective_id=0, has_side_effects=True, vmem_limit_bytes=67043328
        ),
    )(
        latents.reshape(length, width), cotangent.reshape(length, width), line(counts), line(assign),
        line(pre_gain), line(pre_shift), line(b_out), line(mid_gain), line(mid_shift), line(b_down),
        line(b_query), line(b_value), line(b_up),
        w_query, w_key, w_value, w_out, w_up, w_down,
    )

    full = jax.ShapeDtypeStruct((1, width), F32)
    own = jax.ShapeDtypeStruct((1, per), F32)
    wide = jax.ShapeDtypeStruct((width, per), F32)
    flat = jax.ShapeDtypeStruct((per, width), F32)
    results = pl.pallas_call(
        finish_kernel,
        out_shape=(
            jax.ShapeDtypeStruct((length, width), BF16),
            jax.ShapeDtypeStruct((length, width), F32),
            *[wide] * 4, *[flat] * 2, *[full] * 6, *[own] * 3,
        ),
        in_specs=[anywhere] * 3 + [inside],
        out_specs=(*[anywhere] * 8, *[inside] * 9),
        scratch_shapes=[
            pltpu.VMEM((6, 2, width, BLOCK), BF16),
            pltpu.VMEM((4, width, per), F32),
            pltpu.VMEM((2, per, width), F32),
            pltpu.VMEM((length, width), BF16),
            pltpu.VMEM((length, width), F32),
            dma((14,)), dma((8,)),
        ],
        compiler_params=pltpu.CompilerParams(vmem_limit_bytes=67043328),
    )(grads, y_out, gx_out, sums)
    y_out, gx_out, g_query, g_key, g_value, g_up, g_out, g_down = results[:8]
    v0, v1, v2, v3, v4, v5, b0, b1, b2 = [a.reshape(-1) for a in results[8:]]
    return (
        y_out.reshape(latents.shape), gx_out.reshape(latents.shape),
        v0, v1, g_query, b0, g_key, g_value, b1, g_out, v2, v3, v4, g_up, b2, g_down, v5,
    )


def solution(mesh):
    assert mesh.shape["tensor"] == 4
    return jax.shard_map(
        partial(shards_of, mesh.shape["dp"] // 2),
        mesh=mesh,
        in_specs=(
            P(("dp", "tensor"), None, None),
            P(("dp", "tensor"), None, None),
            P(),
            P(),
            P(),
            P(),
            P(None, "tensor"),
            P("tensor"),
            P(None, "tensor"),
            P(None, "tensor"),
            P("tensor"),
            P("tensor", None),
            P(),
            P(),
            P(),
            P(None, "tensor"),
            P("tensor"),
            P("tensor", None),
            P(),
        ),
        out_specs=(
            P(("dp", "tensor"), None, None),
            P(("dp", "tensor"), None, None),
            P(),
            P(),
            P(None, "tensor"),
            P("tensor"),
            P(None, "tensor"),
            P(None, "tensor"),
            P("tensor"),
            P("tensor", None),
            P(),
            P(),
            P(),
            P(None, "tensor"),
            P("tensor"),
            P("tensor", None),
            P(),
        ),
        check_vma=False,
    )
```
